32 devices in a mesh: grp: 4 (over z), gx: 8 (over y, x, core).
Axes of the slice: x: 2, y: 2, z: 4, core: 2. Of those that a mesh axis runs over, the one named last changes fastest.
Arguments:
- component_density: float32 [53, 256, 1024], P(None, 'gx', 'grp'), may hold values from 0.05 to 2
- scaled_thermal_state: float32 [256, 1024], P('gx', 'grp'), may hold values from 0.5 to 1.5
- leading_direction_flow: float32 [256, 1024], P('gx', 'grp'), may hold values from -1 to 1
- trailing_direction_flow: float32 [256, 1024], P('gx', 'grp'), may hold values from -1 to 1
- spreading_coefficient: float32 [54], replicated, may hold values from 0.02 to 0.2
- colliding_pair: int32 [325, 2], replicated, may hold values from 0 to 52
- natural_exponent_scaler: float32 [325], replicated, may hold values from -3 to -1
- arrhenius_energy: float32 [325], replicated, may hold values from 0 to 2
- stoichiometric_output: float32 [325, 53], replicated, may hold values from 0.004 to 0.075
- formation_warming: float32 [53], replicated, may hold values from -1.8 to 1.8
- explicit_increments: int32 [2048], P(('grp', 'gx')), may hold values from 1 to 4, as said below
Outputs:
- species_out: float32 [53, 256, 1024], P(None, 'gx', 'grp')
- temperature_out: float32 [256, 1024], P('gx', 'grp')
The draws below stay inside these ranges and needn't reach their ends.
Inputs may be any that keep to these rules, and one draw needn't show every extreme that they name: `explicit_increments`: substep counts of the tiles, in the order of the tiles described in the reference program.
All inputs are finite; a program needn't handle non-finite values.
Results may differ from the reference program's by a relative error of at most 0.0003.
Values sent between devices are 32-bit elements; how exact they have to be, the bound alone decides.
A program may use at most 64 MiB of HBM per device.

```python
import math
import jax
import jax.numpy as jnp
from jax import lax

SPEC = 53
RXN = 325
CX = 32
CY = 256
TILE = 128
MINSUB = 1
MAXSUB = 4
GRID_LENGTH_LEAD = 256
GRID_LENGTH_TRAIL = 1024
TD = 64
TILES = 2048
N_GRP = 4
N_GX = 8


def draw_explicit_increments(key, part):
    device_count = TILES // TD
    hot_key, drawn_key, busy_key, place_key = jax.random.split(key, 4)
    heated = jax.random.randint(hot_key, (device_count, 1), 0, 8) == 0
    drawn = jax.random.randint(drawn_key, (device_count, TD), MINSUB, MINSUB + 2)
    busy = jax.random.randint(busy_key, (device_count, TD), MAXSUB - 1, MAXSUB + 1)
    tallies = jnp.where(heated, busy, drawn).reshape(TILES)
    spots = jax.random.randint(place_key, (1,), 0, TILES)
    tallies = tallies.at[spots[0]].set(MAXSUB)
    other_spot = (spots[0] + TD) % TILES
    tallies = tallies.at[other_spot].set(MINSUB)
    return tallies.astype(jnp.int32)


def touch_ends(values, stream_key, smallest, high):
    longest = values.shape.index(max(values.shape))
    spots = []
    for shift in (0, 1):
        where = [jax.random.randint(jax.random.fold_in(stream_key, axis), (), 0, length) for axis, length in enumerate(values.shape)]
        where[longest] = (where[longest] + shift) % values.shape[longest]
        spots.append(tuple(where))
    return values.at[spots[0]].set(smallest).at[spots[1]].set(high)


def levels(own_key, dims, pieces, low, largest):
    loudness, own = 1.0, jax.random.fold_in(own_key, 6)
    for axis_at, blocks in pieces:
        heights = jnp.exp(jax.random.uniform(jax.random.fold_in(own, axis_at), (blocks,), jnp.float32, low / len(pieces), largest / len(pieces)))
        loudness = loudness * jnp.repeat(heights, dims[axis_at] // blocks).reshape([-1 if axis == axis_at else 1 for axis in range(len(dims))])
    return loudness


def normal_values(stream_key, shape, scale, limit, held_as=jnp.bfloat16):
    array = scale * jax.random.normal(stream_key, shape, jnp.float32)
    return jnp.clip(array, min=-limit, max=limit).astype(held_as)


def setup_inputs(seed: int = 0) -> dict:
    splits = jax.random.split(jax.random.key(seed), 12)
    return {
        "component_density": jnp.clip(jnp.exp(math.log(2.0) - 3.6888794 * jax.random.uniform(splits[0], (SPEC, GRID_LENGTH_LEAD, GRID_LENGTH_TRAIL), jnp.float32) ** levels(splits[0], (SPEC, GRID_LENGTH_LEAD, GRID_LENGTH_TRAIL), ((1, 8), (2, 4)), -0.2, 0.2)), 0.05, 2.0),
        "scaled_thermal_state": jnp.clip(0.5 + 1.0 * jax.random.uniform(splits[1], (GRID_LENGTH_LEAD, GRID_LENGTH_TRAIL), jnp.float32) ** levels(splits[1], (GRID_LENGTH_LEAD, GRID_LENGTH_TRAIL), ((0, 8), (1, 4)), -0.2, 0.2), 0.5, 1.5),
        "leading_direction_flow": jnp.clip(jax.random.uniform(splits[2], (GRID_LENGTH_LEAD, GRID_LENGTH_TRAIL), jnp.float32, -1.0, 1.0) * levels(splits[2], (GRID_LENGTH_LEAD, GRID_LENGTH_TRAIL), ((0, 8), (1, 4)), -0.4, 0.0), -1.0, 1.0),
        "trailing_direction_flow": jnp.clip(jax.random.uniform(splits[3], (GRID_LENGTH_LEAD, GRID_LENGTH_TRAIL), jnp.float32, -1.0, 1.0) * levels(splits[3], (GRID_LENGTH_LEAD, GRID_LENGTH_TRAIL), ((0, 8), (1, 4)), -0.4, 0.0), -1.0, 1.0),
        "spreading_coefficient": jnp.clip(jnp.exp(jax.random.uniform(splits[4], (SPEC + 1,), jnp.float32, math.log(0.02), math.log(0.2))), 0.02, 0.2),
        "colliding_pair": touch_ends(jax.random.randint(splits[5], (RXN, 2), 0, SPEC), jax.random.fold_in(splits[5], 1), 0, SPEC - 1).astype(jnp.int32),
        "natural_exponent_scaler": jnp.clip(jax.random.uniform(splits[6], (RXN,), jnp.float32, -3.0, -1.0), -3.0, -1.0),
        "arrhenius_energy": jnp.clip(jax.random.uniform(splits[7], (RXN,), jnp.float32, 0.0, 2.0), 0.0, 2.0),
        "stoichiometric_output": jnp.clip(jnp.exp(jax.random.uniform(splits[8], (RXN, SPEC), jnp.float32, math.log(0.004), math.log(0.075))), 0.004, 0.075),
        "formation_warming": normal_values(splits[9], (SPEC,), 0.3, 1.8, jnp.float32),
        "explicit_increments": draw_explicit_increments(jax.random.fold_in(splits[11], 71), 0),
    }


transport_step = 0.4
chemistry_span = 0.5
sixth_first = (0.75, -0.15, 1.0 / 60.0)
sixth_second = (1.5, -0.15, 1.0 / 90.0)
sixth_center = -49.0 / 18.0


def tendency(extended, speeds, spreading_coefficient):
    height = extended.shape[1] - 6
    breadth = extended.shape[2] - 6

    def along_first(values, offset):
        return values[:, 3 + offset:3 + offset + height, 3:3 + breadth]

    def along_second(values, offset):
        return values[:, 3:3 + height, 3 + offset:3 + offset + breadth]

    east_flux = speeds[0:1] * extended
    north_flux = speeds[1:2] * extended
    gradient = jnp.zeros((extended.shape[0], height, breadth), jnp.float32)
    laplacian = 2.0 * sixth_center * along_first(extended, 0)
    for offset in range(1, 4):
        gradient = gradient + sixth_first[offset - 1] * (along_first(east_flux, offset) - along_first(east_flux, -offset) + along_second(north_flux, offset) - along_second(north_flux, -offset))
        laplacian = laplacian + sixth_second[offset - 1] * (along_first(extended, offset) + along_first(extended, -offset) + along_second(extended, offset) + along_second(extended, -offset))
    return spreading_coefficient[:, None, None] * laplacian - gradient


def build_tables(colliding_pair, stoichiometric_output):
    species_ids = jnp.arange(stoichiometric_output.shape[1], dtype=jnp.int32)[:, None]
    first_table = (species_ids == colliding_pair[None, :, 0]).astype(jnp.float32)
    second_table = (species_ids == colliding_pair[None, :, 1]).astype(jnp.float32)
    return stoichiometric_output.T, jnp.concatenate([first_table, second_table], 1)


def substep_once(combined_state_array, step_sizes, mechanism):
    gain_table, loss_table, colliding_pair, natural_exponent_scaler, arrhenius_energy, formation_warming = mechanism
    amounts = combined_state_array[:-1]
    warmth = combined_state_array[-1]
    rate_constant = jnp.exp(natural_exponent_scaler[:, None] + arrhenius_energy[:, None] * jnp.tanh(warmth)[None, :])
    first_partner = jnp.take(amounts, colliding_pair[:, 0], axis=0)
    second_partner = jnp.take(amounts, colliding_pair[:, 1], axis=0)
    progress = rate_constant * first_partner * second_partner
    gained = jnp.dot(gain_table, progress, precision=lax.Precision.HIGHEST, preferred_element_type=jnp.float32)
    partners = jnp.concatenate([rate_constant * second_partner, rate_constant * first_partner], 0)
    destroyed = jnp.dot(loss_table, partners, precision=lax.Precision.HIGHEST, preferred_element_type=jnp.float32)
    updated = (amounts + step_sizes[None, :] * gained) / (1.0 + step_sizes[None, :] * destroyed)
    warmer = warmth + jnp.dot(formation_warming, updated - amounts, precision=lax.Precision.HIGHEST, preferred_element_type=jnp.float32)
    return jnp.concatenate([updated, warmer[None, :]], 0)


def substep_loop(combined_state_array, counts, turn_count, mechanism):
    step_sizes = chemistry_span / counts.astype(jnp.float32)

    def advance(substep, current):
        advanced = substep_once(current, step_sizes, mechanism)
        return jnp.where((substep < counts)[None, :], advanced, current)

    return lax.fori_loop(0, turn_count, advance, combined_state_array)


def periodic(values):
    return jnp.pad(values, ((0, 0), (3, 3), (3, 3)), mode="wrap")


def reference(component_density, scaled_thermal_state, leading_direction_flow, trailing_direction_flow, spreading_coefficient, colliding_pair, natural_exponent_scaler, arrhenius_energy, stoichiometric_output, formation_warming, explicit_increments):
    combined_state_array = jnp.concatenate([component_density, scaled_thermal_state[None]], 0)
    speed_wide = periodic(jnp.stack([leading_direction_flow, trailing_direction_flow]))
    section_one = combined_state_array + transport_step * tendency(periodic(combined_state_array), speed_wide, spreading_coefficient)
    section_two = 0.75 * combined_state_array + 0.25 * (section_one + transport_step * tendency(periodic(section_one), speed_wide, spreading_coefficient))
    advected = combined_state_array / 3.0 + (2.0 / 3.0) * (section_two + transport_step * tendency(periodic(section_two), speed_wide, spreading_coefficient))
    clipped = jnp.concatenate([jnp.maximum(advected[:-1], 0.0), advected[-1:]], 0)
    layers = SPEC + 1
    blocks = clipped.reshape(layers, N_GX, CX, N_GRP, CY).transpose(3, 1, 0, 2, 4).reshape(N_GRP * N_GX, layers, CX * CY)
    cell_counts = jnp.repeat(explicit_increments.reshape(N_GRP * N_GX, -1), TILE, axis=1)
    gain_table, loss_table = build_tables(colliding_pair, stoichiometric_output)
    mechanism = (gain_table, loss_table, colliding_pair, natural_exponent_scaler, arrhenius_energy, formation_warming)

    def per_device(device_pair):
        device_block, device_counts = device_pair
        return substep_loop(device_block, device_counts, MAXSUB, mechanism)

    reacted = lax.map(per_device, (blocks, cell_counts))
    restored = reacted.reshape(N_GRP, N_GX, layers, CX, CY).transpose(2, 1, 3, 0, 4).reshape(layers, GRID_LENGTH_LEAD, GRID_LENGTH_TRAIL)
    return restored[:SPEC], restored[SPEC]
```

```python
import functools
import math

import jax
import jax.numpy as jnp
import numpy as np
from jax import lax
from jax.experimental import pallas as pl
from jax.experimental.pallas import tpu as pltpu
from jax.sharding import PartitionSpec as P

TILE = 128
HALO = 9
FIRST_SCALE = 60.0
SECOND_SCALE = 180.0
transport_step = 0.4
chemistry_span = 0.5
sixth_first = (0.75, -0.15, 1.0 / 60.0)
sixth_second = (1.5, -0.15, 1.0 / 90.0)
sixth_center = -49.0 / 18.0


def up8(n):
    return -(-n // 8) * 8


def halo_kernel(sizes, main, first_cols, last_cols, top, bottom, left, right, send, recv):
    n_grp, n_gx = sizes
    g, x = lax.axis_index("grp"), lax.axis_index("gx")
    rows = main.shape[0]
    place = lambda dg, dx: (lax.rem(g + dg + n_grp, n_grp), lax.rem(x + dx + n_gx, n_gx))
    barrier = pltpu.get_barrier_semaphore()
    around = [(dg, dx) for dg in (-1, 0, 1) for dx in (-1, 0, 1) if (dg, dx) != (0, 0)]
    for dg, dx in around:
        pl.semaphore_signal(barrier, inc=1, device_id=place(dg, dx),
                            device_id_type=pl.DeviceIdType.MESH)
    pl.semaphore_wait(barrier, len(around))
    early, late = pl.ds(0, HALO), pl.ds(rows - HALO, HALO)
    above, beside, below = pl.ds(0, HALO), pl.ds(HALO, rows), pl.ds(HALO + rows, HALO)
    plan = [
        (main.at[late], top, 0, 1),
        (main.at[early], bottom, 0, -1),
        (last_cols, left.at[beside], 1, 0),
        (first_cols, right.at[beside], -1, 0),
        (last_cols.at[late], left.at[above], 1, 1),
        (last_cols.at[early], left.at[below], 1, -1),
        (first_cols.at[late], right.at[above], -1, 1),
        (first_cols.at[early], right.at[below], -1, -1),
    ]
    copies = []
    for n, (src, dst, dg, dx) in enumerate(plan):
        copy = pltpu.make_async_remote_copy(
            src_ref=src, dst_ref=dst, send_sem=send.at[n], recv_sem=recv.at[n],
            device_id=place(dg, dx), device_id_type=pl.DeviceIdType.MESH)
        copy.start()
        copies.append(copy)
    for copy in copies:
        copy.wait()


def exchange(main, first_cols, last_cols):
    rows, layers, cols = main.shape
    sizes = (lax.axis_size("grp"), lax.axis_size("gx"))
    anywhere = pl.BlockSpec(memory_space=pltpu.VMEM)
    strip = jax.ShapeDtypeStruct((HALO, layers, cols), jnp.float32)
    edge = jax.ShapeDtypeStruct((rows + 2 * HALO,) + first_cols.shape[1:], jnp.float32)
    return pl.pallas_call(
        functools.partial(halo_kernel, sizes),
        in_specs=[anywhere] * 3,
        out_specs=[anywhere] * 4,
        out_shape=[strip, strip, edge, edge],
        scratch_shapes=[pltpu.SemaphoreType.DMA((8,)), pltpu.SemaphoreType.DMA((8,))],
        compiler_params=pltpu.CompilerParams(collective_id=0, has_side_effects=True),
        name="halo",
    )(main, first_cols, last_cols)


def halves(value):
    high = value.astype(jnp.bfloat16)
    return high, (value - high.astype(jnp.float32)).astype(jnp.bfloat16)


def transport_kernel(fields, main, top, bottom, side, diff, band, uv_main, uv_top, uv_bottom, uv_side,
                     out, start, one, two, east, north, pieces, across):
    rows, _, cols = main.shape
    wide = rows + 2 * HALO
    gap = side.shape[2]
    width = cols + gap
    tile = pl.program_id(0)
    u_at, v_at = fields % 8, (fields + 1) % 8

    def fill(dst, m, t, b, s, sub):
        def put(r, ref, at):
            if sub is None:
                dst[r, :, :cols] = ref[at]
            else:
                dst[r, :, :cols] = jnp.broadcast_to(ref[at, sub:sub + 1, :], (8, cols))

        def mid(r, c):
            put(HALO + r, m, r)
            return c

        lax.fori_loop(0, rows, mid, 0, unroll=4)
        for r in range(HALO):
            put(r, t, r)
            put(HALO + rows + r, b, r)

        def edge(r, c):
            if sub is None:
                dst[r, :, cols:] = s[r]
            else:
                dst[r, :, cols:] = jnp.broadcast_to(s[r, sub:sub + 1, :], (8, gap))
            return c

        lax.fori_loop(0, wide, edge, 0, unroll=5)

    @pl.when(tile == 0)
    def _():
        fill(east, uv_main, uv_top, uv_bottom, uv_side, u_at)
        fill(north, uv_main, uv_top, uv_bottom, uv_side, v_at)

    fill(start, main, top, bottom, side, None)
    d = diff[...] * transport_step
    d_wide = jnp.concatenate([d] * (width // 128), axis=1)

    def columns(src, low, high):
        scale = d_wide * (1.0 / SECOND_SCALE)

        def split(j, c):
            fs, gs = [], []
            for q in range(2):
                i = low + 2 * j + q
                f = src[i]
                fs.append(scale * f)
                gs.append((-transport_step / FIRST_SCALE) * (north[i] * f))
            f_high, f_low = halves(jnp.concatenate(fs, 0))
            g_high, g_low = halves(jnp.concatenate(gs, 0))
            at = pl.ds(pl.multiple_of(j * 16, 16), 16)
            pieces[at, 0:width] = f_high
            pieces[at, width:2 * width] = f_low
            pieces[at, 2 * width:3 * width] = g_high
            pieces[at, 3 * width:4 * width] = g_low
            return c

        lax.fori_loop(0, (high - low) // 2, split, 0, unroll=2 if (high - low) % 4 == 0 else 1)
        count = (high - low) * 8
        across[0:count] = jnp.dot(pieces[0:count], band[...], preferred_element_type=jnp.float32)

    def change(src, i, low, n):
        lap = sixth_center * src[i, :, :n]
        grad = None
        for k in range(1, 4):
            ahead, behind = src[i + k, :, :n], src[i - k, :, :n]
            lap = lap + sixth_second[k - 1] * (ahead + behind)
            slope = (sixth_first[k - 1] * transport_step) * (
                east[i + k, :, :n] * ahead - east[i - k, :, :n] * behind)
            grad = slope if grad is None else grad + slope
        col = across[pl.ds(pl.multiple_of((i - low) * 8, 8), 8), :n]
        return col + (d_wide[:, :n] * lap - grad)

    columns(start, 3, wide - 3)

    def first(i, c):
        one[i] = start[i] + change(start, i, 3, width)
        return c

    lax.fori_loop(3, wide - 3, first, 0, unroll=math.gcd(wide - 6, 4))
    columns(one, 6, wide - 6)

    def second(i, c):
        two[i] = 0.75 * start[i] + 0.25 * (one[i] + change(one, i, 6, width))
        return c

    lax.fori_loop(6, wide - 6, second, 0, unroll=math.gcd(wide - 12, 4))
    columns(two, 9, wide - 9)
    ids = tile * 8 + lax.broadcasted_iota(jnp.int32, (8, cols), 0)
    is_species = ids < fields - 1

    def third(i, c):
        value = start[i, :, :cols] * (1.0 / 3.0) + (2.0 / 3.0) * (
            two[i, :, :cols] + change(two, i, 9, cols))
        out[i - HALO] = jnp.where(is_species, jnp.maximum(value, 0.0), value)
        return c

    lax.fori_loop(9, wide - 9, third, 0, unroll=math.gcd(rows, 4))


def band_matrix(width):
    here = np.arange(width)
    lag = (here[:, None] - here[None, :]) % width
    second = np.where(lag == 0, round(sixth_center * SECOND_SCALE), 0)
    first = np.zeros((width, width))
    for k in range(1, 4):
        ahead, behind = lag == k, lag == width - k
        second = np.where(ahead | behind, round(sixth_second[k - 1] * SECOND_SCALE), second)
        weight = round(sixth_first[k - 1] * FIRST_SCALE)
        first = np.where(ahead, weight, np.where(behind, -weight, first))
    return jnp.asarray(np.concatenate([second, second, first, first], 0), jnp.bfloat16)


def transport(main, top, bottom, side, vectors, diff_at, fields):
    rows, layers, cols = main.shape
    wide = rows + 2 * HALO
    gap = side.shape[2]
    width = cols + gap
    uv_tile = fields // 8
    band = band_matrix(width)
    by = lambda r, n: pl.BlockSpec((r, 8, n), lambda t: (0, t, 0))
    uv = lambda r, n: pl.BlockSpec((r, 8, n), lambda t: (0, uv_tile, 0))
    return pl.pallas_call(
        functools.partial(transport_kernel, fields),
        grid=(layers // 8,),
        in_specs=[by(rows, cols), by(HALO, cols), by(HALO, cols), by(wide, gap),
                  pl.BlockSpec((8, 128), lambda t: (diff_at + t, 0)),
                  pl.BlockSpec(band.shape, lambda t: (0, 0)),
                  uv(rows, cols), uv(HALO, cols), uv(HALO, cols), uv(wide, gap)],
        out_specs=by(rows, cols),
        out_shape=jax.ShapeDtypeStruct(main.shape, jnp.float32),
        scratch_shapes=[pltpu.VMEM((wide, 8, width), jnp.float32) for _ in range(5)]
        + [pltpu.VMEM(((wide - 6) * 8, 4 * width), jnp.bfloat16),
           pltpu.VMEM(((wide - 6) * 8, width), jnp.float32)],
        name="transport",
    )(main, top, bottom, side, vectors, band, main, top, bottom, side)


GROUP = 16
PITCH = GROUP + 1
LANES = 128


def chemistry_kernel(reactions, species, order, counts, pair, rates, warming, state, gain, out, warm_out,
                     held, gained, progress, table, steps, staged, sems, *losses):
    rows, layers, cols = state.shape
    per_row = cols // TILE
    tiles = rows * per_row
    warm_row = species
    span = progress.shape[0] // GROUP
    depth = span // 8 * 8
    half = table.shape[0] // 2
    blocks = layers // 8

    progress[...] = jnp.zeros_like(progress)
    table[...] = jnp.zeros_like(table)
    high, low = halves(gain[...])
    table[0:species, 0:reactions] = high
    table[half:half + species, 0:reactions] = low
    for loss in losses:
        loss[...] = jnp.zeros_like(loss)

    def at(field):
        return pl.ds(field * PITCH, GROUP)

    def handle(g, c):
        ids = [order[g * GROUP + t] for t in range(GROUP)]
        numbers = [counts[t] for t in ids]
        places = [(t // per_row, pl.ds(pl.multiple_of((t % per_row) * TILE, TILE), TILE)) for t in ids]
        turn_count = functools.reduce(jnp.maximum, numbers)
        for t in range(GROUP):
            r, lanes = places[t]
            steps[t:t + 1, :] = jnp.full((1, LANES), numbers[t].astype(jnp.float32))
            for f in range(blocks):
                held[pl.ds(f * 8 * PITCH + t, 8, stride=PITCH)] = state[r, f * 8:(f + 1) * 8, lanes]

        def advance(s, c):
            heat = jnp.tanh(held[at(warm_row)])
            for r in range(reactions):
                first = pl.ds(pair[r], GROUP)
                second = pl.ds(pair[reactions + r], GROUP)
                a = jnp.broadcast_to(rates[r:r + 1, :], (GROUP, LANES))
                e = jnp.broadcast_to(rates[reactions + r:reactions + r + 1, :], (GROUP, LANES))
                weight = jnp.broadcast_to(rates[2 * reactions + r:2 * reactions + r + 1, :], (GROUP, LANES))
                rate = jnp.exp2(a + e * heat)
                ca, cb = held[first], held[second]
                qa, qb = rate * ca, rate * cb
                progress[pl.ds(r, GROUP, stride=span)] = qa * (weight * cb)
                n = 2 * (r % (len(losses) // 2))
                losses[n][first] += qb
                losses[n + 1][second] += qa
            for q in range(GROUP // 2):
                p = jnp.concatenate([progress[pl.ds((2 * q + t) * span, depth)] for t in range(2)], 1)
                both = jnp.dot(table[...], p.astype(jnp.bfloat16), preferred_element_type=jnp.float32)
                total = both[:half] + both[half:]
                for t in range(2):
                    for f in range(blocks):
                        gained[pl.ds(f * 8 * PITCH + 2 * q + t, 8, stride=PITCH)] = (
                            total[f * 8:(f + 1) * 8, t * TILE:(t + 1) * TILE])
            number = steps[...]
            h = chemistry_span / number
            active = s.astype(jnp.float32) < number
            change = jnp.zeros((GROUP, LANES), jnp.float32)
            for j in range(species):
                x = held[at(j)]
                destroyed = functools.reduce(jnp.add, [loss[at(j)] for loss in losses])
                for loss in losses:
                    loss[at(j)] = jnp.zeros((GROUP, LANES), jnp.float32)
                updated = (x + h * gained[at(j)]) / (1.0 + h * destroyed)
                change = change + warming[j] * (updated - x)
                held[at(j)] = jnp.where(active, updated, x)
            w = held[at(warm_row)]
            held[at(warm_row)] = jnp.where(active, w + change, w)
            return c

        lax.fori_loop(0, turn_count, advance, 0)
        for t in range(GROUP):
            for f in range(0, warm_row + 1, 8):
                n = min(8, warm_row + 1 - f)
                staged[pl.ds(((ids[t] % per_row) * (warm_row + 1) + f) * rows + ids[t] // per_row, n, stride=rows)] = (
                    held[pl.ds(f * PITCH + t, n, stride=PITCH)])
        return c

    lax.fori_loop(0, tiles // GROUP, handle, 0)
    height = (warm_row + 1) * rows
    copies = []
    for n in range(per_row):
        lanes = pl.ds(n * TILE, TILE)
        copies.append(pltpu.make_async_copy(
            staged.at[pl.ds(n * height, warm_row * rows)], out.at[:, lanes], sems.at[0, n]))
        copies.append(pltpu.make_async_copy(
            staged.at[pl.ds(n * height + warm_row * rows, rows)], warm_out.at[:, lanes], sems.at[1, n]))
    for copy in copies:
        copy.start()
    for copy in copies:
        copy.wait()


LOSSES = 6


def chemistry(state, order, counts, pair, rates, warming, gain):
    rows, layers, cols = state.shape
    species, reactions = gain.shape
    depth = -(-reactions // 16) * 16
    smem = pl.BlockSpec(memory_space=pltpu.SMEM)
    vmem = pl.BlockSpec(memory_space=pltpu.VMEM)
    block = pltpu.VMEM((layers * PITCH, LANES), jnp.float32)
    return pl.pallas_call(
        functools.partial(chemistry_kernel, reactions, species),
        in_specs=[smem, smem, smem, vmem, smem, vmem, vmem],
        out_specs=[pl.BlockSpec(memory_space=pl.ANY)] * 2,
        out_shape=[jax.ShapeDtypeStruct((species * rows, cols), jnp.float32),
                   jax.ShapeDtypeStruct((rows, cols), jnp.float32)],
        scratch_shapes=[block, block,
                        pltpu.VMEM((GROUP * (depth + 1), LANES), jnp.float32),
                        pltpu.VMEM((2 * -(-layers // 16) * 16, depth), jnp.bfloat16),
                        pltpu.VMEM((GROUP, LANES), jnp.float32),
                        pltpu.VMEM((cols // TILE * (species + 1) * rows, TILE), jnp.float32),
                        pltpu.SemaphoreType.DMA((2, cols // TILE))]
        + [block] * LOSSES,
        name="chemistry",
    )(order, counts, pair, rates, warming, state, gain)


def spread_weights(reactions):
    golden = (math.sqrt(5.0) - 1.0) / 2.0
    return jnp.asarray(np.exp2((np.arange(reactions) * golden) % 1.0), jnp.float32)


def by_count(counts):
    tiles = counts.shape[0]
    ids = jnp.arange(tiles, dtype=jnp.int32)
    key = counts * tiles + ids
    rank = jnp.sum((key[None, :] < key[:, None]).astype(jnp.int32), 1)
    return jnp.sum(jnp.where(rank[:, None] == ids[None, :], ids[:, None], 0), 0)


def body(component_density, scaled_thermal_state, leading_direction_flow, trailing_direction_flow,
         spreading_coefficient, colliding_pair, natural_exponent_scaler, arrhenius_energy,
         stoichiometric_output, formation_warming, explicit_increments):
    species, rows, cols = component_density.shape
    fields = species + 1
    layers = up8(fields + 2)
    bundle = jnp.concatenate(
        [component_density, scaled_thermal_state[None], leading_direction_flow[None],
         trailing_direction_flow[None]], 0)
    bundle = jnp.pad(bundle, ((0, layers - fields - 2), (0, 0), (0, 0)))
    main = jnp.transpose(bundle, (1, 0, 2))

    first_cols = jnp.transpose(main[:, :, :HALO], (0, 2, 1))
    last_cols = jnp.transpose(main[:, :, cols - HALO:], (0, 2, 1))
    top, bottom, left, right = exchange(main, first_cols, last_cols)
    gap = jnp.zeros((rows + 2 * HALO, 128 - 2 * HALO, layers), jnp.float32)
    side = jnp.transpose(jnp.concatenate([right, gap, left], 1), (0, 2, 1))
    spread = jnp.broadcast_to(jnp.pad(spreading_coefficient, (0, layers - fields))[:, None], (layers, 128))
    clipped = transport(main, top, bottom, side, spread, 0, fields)
    scale = 1.0 / math.log(2.0)
    weight = spread_weights(arrhenius_energy.shape[0])
    rates = jnp.concatenate([natural_exponent_scaler * scale, arrhenius_energy * scale, weight])
    rates = jnp.broadcast_to(rates[:, None], (rates.shape[0], LANES))
    pair = jnp.concatenate([colliding_pair[:, 0], colliding_pair[:, 1]]) * PITCH
    reacted, warm = chemistry(clipped, by_count(explicit_increments), explicit_increments, pair, rates,
                              formation_warming, stoichiometric_output.T / weight)
    return reacted.reshape(species, rows, cols), warm


def solution(mesh):
    return jax.shard_map(
        body,
        mesh=mesh,
        in_specs=(
            P(None, "gx", "grp"),
            P("gx", "grp"),
            P("gx", "grp"),
            P("gx", "grp"),
            P(),
            P(),
            P(),
            P(),
            P(),
            P(),
            P(("grp", "gx")),
        ),
        out_specs=(P(None, "gx", "grp"), P("gx", "grp")),
        check_vma=False,
    )
```

```python
import functools
import math

import jax
import jax.numpy as jnp
import numpy as np
from jax import lax
from jax.experimental import pallas as pl
from jax.experimental.pallas import tpu as pltpu
from jax.sharding import PartitionSpec as P

TILE = 128
FIRST_SCALE = 60.0
SECOND_SCALE = 180.0
transport_step = 0.4
chemistry_span = 0.5
sixth_first = (0.75, -0.15, 1.0 / 60.0)
sixth_second = (1.5, -0.15, 1.0 / 90.0)
sixth_center = -49.0 / 18.0


def up8(n):
    return -(-n // 8) * 8


REACH = 3
SLOT = 4
LANES = 128


def halves(value):
    high = value.astype(jnp.bfloat16)
    return high, (value - high.astype(jnp.float32)).astype(jnp.bfloat16)


def advect_kernel(fields, sizes, density, warm, leading, trailing, spread, band, out,
                  start, one, two, east, north, pieces, across, packed, landed, flows, send, recv):
    n_grp, n_gx = sizes
    g, x = lax.axis_index("grp"), lax.axis_index("gx")
    rows, cols = warm.shape
    parts = cols // LANES
    tiles = start.shape[0] // parts
    species = fields - 1
    last = fields // 8
    up, down = (g, lax.rem(x + n_gx - 1, n_gx)), (g, lax.rem(x + 1, n_gx))
    left, right = (lax.rem(g + n_grp - 1, n_grp), x), (lax.rem(g + 1, n_grp), x)
    barrier = pltpu.get_barrier_semaphore()
    for place in (up, down, left, right):
        pl.semaphore_signal(barrier, inc=1, device_id=place, device_id_type=pl.DeviceIdType.MESH)

    lane = lax.broadcasted_iota(jnp.int32, (8, LANES), 1)
    row_of = lane // SLOT
    slot = lane % SLOT

    def at(row, count=1):
        return pl.ds(pl.multiple_of(row * 8, 8), count * 8)

    def spread_out(read, t, sub):
        for q in range(rows // 8):
            for h in range(parts):
                start[t * parts + h, pl.ds((REACH + q * 8) * 8 + sub, 8, stride=8), :] = read(q, h)

    def of_density(f):
        return lambda q, h: density[pl.ds(pl.multiple_of(f * rows + q * 8, 8), 8), h * LANES:(h + 1) * LANES]

    def of_plane(ref):
        return lambda q, h: ref[q * 8:(q + 1) * 8, h * LANES:(h + 1) * LANES]

    def copies(s, t):
        held = (start, one, two)[s]
        both = pl.ds(t * parts, parts)
        plan = [
            (held.at[both, pl.ds(REACH * 8, REACH * 8)], held.at[both, pl.ds((REACH + rows) * 8, REACH * 8)], up),
            (held.at[both, pl.ds(rows * 8, REACH * 8)], held.at[both, pl.ds(0, REACH * 8)], down),
            (packed.at[s, t, 0], landed.at[s, t, 1], left),
            (packed.at[s, t, 1], landed.at[s, t, 0], right),
        ]
        return [pltpu.make_async_remote_copy(
            src_ref=src, dst_ref=dst, send_sem=send.at[s, t, n], recv_sem=recv.at[s, t, n],
            device_id=place, device_id_type=pl.DeviceIdType.MESH) for n, (src, dst, place) in enumerate(plan)]

    def pack(s, t):
        held = (start, one, two)[s]
        first = jnp.zeros((8, LANES), jnp.float32)
        final = jnp.zeros((8, LANES), jnp.float32)
        for i in range(rows):
            mine = row_of == i
            first = jnp.where(mine, pltpu.roll(held[t * parts, at(REACH + i), :], (SLOT * i) % LANES, 1), first)
            final = jnp.where(mine, pltpu.roll(held[t * parts + parts - 1, at(REACH + i), :],
                                               (SLOT * i + REACH) % LANES, 1), final)
        packed[s, t, 0] = first
        packed[s, t, 1] = final
        for copy in copies(s, t):
            copy.start()

    for f in range(last * 8, species):
        spread_out(of_density(f), last, f % 8)
    for n, ref in enumerate((warm, leading, trailing)):
        spread_out(of_plane(ref), last, (species + n) % 8)
    pl.semaphore_wait(barrier, 4)
    pack(0, last)

    def prepare(t, c):
        for sub in range(8):
            spread_out(of_density(t * 8 + sub), t, sub)
        pack(0, t)
        return c

    lax.fori_loop(0, last, prepare, 0)

    for i in range(rows):
        for h in range(parts):
            lanes = slice(h * LANES, (h + 1) * LANES)
            east[h, at(REACH + i), :] = jnp.broadcast_to(leading[i:i + 1, lanes], (8, LANES))
            north[h, at(i), :] = jnp.broadcast_to(trailing[i:i + 1, lanes], (8, LANES))

    def arrive(s, t):
        for copy in copies(s, t):
            copy.wait_recv()

    arrive(0, last)
    u_sub, v_sub = fields % 8, (fields + 1) % 8
    for r in (*range(REACH), *range(REACH + rows, 2 * REACH + rows)):
        for h in range(parts):
            east[h, at(r), :] = jnp.broadcast_to(
                start[last * parts + h, pl.ds(r * 8 + u_sub, 1), :], (8, LANES))
    for side in range(2):
        flow = jnp.broadcast_to(landed[0, last, side, pl.ds(v_sub, 1), :], (8, LANES))
        for k in range(1, REACH + 1):
            inside = (slot >= REACH - k) & (slot < REACH) if side == 0 else slot < k
            weight = (1.0 if side == 0 else -1.0) * transport_step * sixth_first[k - 1]
            flows[side * REACH + k - 1] = jnp.where(inside, weight * flow, 0.0)

    def stage(s):
        held, fresh = (start, one, two)[s], (one, two, None)[s]

        def tile(n, c):
            t = lax.rem(n + last, tiles)

            @pl.when(n > 0 if s == 0 else n >= 0)
            def _():
                arrive(s, t)

            d = spread[at(t), :] * transport_step
            scale = d * (1.0 / SECOND_SCALE)

            def split(j, c):
                for h in range(parts):
                    fs, gs = [], []
                    for q in range(2):
                        i = 2 * j + q
                        f = held[t * parts + h, at(REACH + i), :]
                        fs.append(scale * f)
                        gs.append((-transport_step / FIRST_SCALE) * (north[h, at(i), :] * f))
                    f_high, f_low = halves(jnp.concatenate(fs, 0))
                    g_high, g_low = halves(jnp.concatenate(gs, 0))
                    place = pl.ds(pl.multiple_of(j * 16, 16), 16)
                    for m, piece in enumerate((f_high, f_low, g_high, g_low)):
                        pieces[place, m * cols + h * LANES:m * cols + (h + 1) * LANES] = piece
                return c

            lax.fori_loop(0, rows // 2, split, 0, unroll=4)
            across[...] = jnp.dot(pieces[...], band[...], preferred_element_type=jnp.float32)

            borders = []
            for side in range(2):
                halo = landed[s, t, side]
                total = None
                for k in range(1, REACH + 1):
                    inside = (slot >= REACH - k) & (slot < REACH) if side == 0 else slot < k
                    part = (jnp.where(inside, sixth_second[k - 1] * d, 0.0) + flows[side * REACH + k - 1]) * halo
                    if k < REACH:
                        part = pltpu.roll(part, (k - REACH) % LANES if side == 0 else REACH - k, 1)
                    total = part if total is None else total + part
                borders.append(total)
            ids = t * 8 + lax.broadcasted_iota(jnp.int32, (8, LANES), 0)

            def update(b, c):
                for h in range(parts):
                    lanes = slice(h * LANES, (h + 1) * LANES)
                    f = [held[t * parts + h, at(b * 8 + m), :] for m in range(8 + 2 * REACH)]
                    gs = [east[h, at(b * 8 + m), :] * f[m] for m in range(8 + 2 * REACH)]
                    for r in range(8):
                        i = b * 8 + r
                        m = r + REACH
                        lap = sixth_center * f[m]
                        grad = None
                        for k in range(1, REACH + 1):
                            lap = lap + sixth_second[k - 1] * (f[m + k] + f[m - k])
                            slope = (sixth_first[k - 1] * transport_step) * (gs[m + k] - gs[m - k])
                            grad = slope if grad is None else grad + slope
                        change = across[at(i), lanes] + (d * lap - grad)
                        if h == 0:
                            change = change + jnp.where(
                                lane < REACH, pltpu.roll(borders[0], lax.rem(LANES - SLOT * i, LANES), 1), 0.0)
                        if h == parts - 1:
                            change = change + jnp.where(
                                lane >= LANES - REACH,
                                pltpu.roll(borders[1], lax.rem(2 * LANES - REACH - SLOT * i, LANES), 1), 0.0)
                        if s == 0:
                            fresh[t * parts + h, at(REACH + i), :] = f[m] + change
                        elif s == 1:
                            fresh[t * parts + h, at(REACH + i), :] = (
                                0.75 * start[t * parts + h, at(REACH + i), :] + 0.25 * (f[m] + change))
                        else:
                            value = start[t * parts + h, at(REACH + i), :] * (1.0 / 3.0) + (2.0 / 3.0) * (f[m] + change)
                            out[t * parts + h, at(i), :] = jnp.where(ids < species, jnp.maximum(value, 0.0), value)
                return c

            lax.fori_loop(0, rows // 8, update, 0)
            if s < 2:
                pack(s + 1, t)
            return c

        lax.fori_loop(0, tiles, tile, 0)

    for s in range(3):
        stage(s)

    def finish(t, c):
        for s in range(3):
            for copy in copies(s, t):
                copy.wait_send()
        return c

    lax.fori_loop(0, tiles, finish, 0)


def band_matrix(width):
    here = np.arange(width)
    lag = here[:, None] - here[None, :]
    second = np.where(lag == 0, round(sixth_center * SECOND_SCALE), 0)
    first = np.zeros((width, width))
    for k in range(1, REACH + 1):
        ahead, behind = lag == k, lag == -k
        second = np.where(ahead | behind, round(sixth_second[k - 1] * SECOND_SCALE), second)
        weight = round(sixth_first[k - 1] * FIRST_SCALE)
        first = np.where(ahead, weight, np.where(behind, -weight, first))
    return jnp.asarray(np.concatenate([second, second, first, first], 0), jnp.bfloat16)


def advect(density, warm, leading, trailing, spread):
    species, rows, cols = density.shape
    fields = species + 1
    tiles = (fields + 2) // 8
    if (fields + 2) % 8 or rows * SLOT > LANES or cols % LANES or rows % 8:
        raise ValueError("unsupported sizes")
    parts = cols // LANES
    sizes = (lax.axis_size("grp"), lax.axis_size("gx"))
    vmem = pl.BlockSpec(memory_space=pltpu.VMEM)
    wide = pltpu.VMEM((tiles * parts, (rows + 2 * REACH) * 8, LANES), jnp.float32)
    band = band_matrix(cols)
    return pl.pallas_call(
        functools.partial(advect_kernel, fields, sizes),
        in_specs=[vmem] * 6,
        out_specs=vmem,
        out_shape=jax.ShapeDtypeStruct((tiles * parts, rows * 8, LANES), jnp.float32),
        scratch_shapes=[wide, wide, wide,
                        pltpu.VMEM((parts, (rows + 2 * REACH) * 8, LANES), jnp.float32),
                        pltpu.VMEM((parts, rows * 8, LANES), jnp.float32),
                        pltpu.VMEM((rows * 8, 4 * cols), jnp.bfloat16),
                        pltpu.VMEM((rows * 8, cols), jnp.float32),
                        pltpu.VMEM((3, tiles, 2, 8, LANES), jnp.float32),
                        pltpu.VMEM((3, tiles, 2, 8, LANES), jnp.float32),
                        pltpu.VMEM((2 * REACH, 8, LANES), jnp.float32),
                        pltpu.SemaphoreType.DMA((3, tiles, 4)),
                        pltpu.SemaphoreType.DMA((3, tiles, 4))],
        compiler_params=pltpu.CompilerParams(collective_id=0, has_side_effects=True),
        name="advect",
    )(density.reshape(species * rows, cols), warm, leading, trailing, spread, band)


GROUP = 16
PITCH = GROUP + 1


def chemistry_kernel(reactions, species, order, counts, pair, rates, warming, state, gain, out, warm_out,
                     held, gained, progress, table, steps, staged, sems, *losses):
    rows, cols = warm_out.shape
    layers = state.shape[0] * LANES // cols * 8
    per_row = cols // TILE
    tiles = rows * per_row
    warm_row = species
    span = progress.shape[0] // GROUP
    depth = span // 8 * 8
    half = table.shape[0] // 2
    blocks = layers // 8

    progress[...] = jnp.zeros_like(progress)
    table[...] = jnp.zeros_like(table)
    high, low = halves(gain[...])
    table[0:species, 0:reactions] = high
    table[half:half + species, 0:reactions] = low
    for loss in losses:
        loss[...] = jnp.zeros_like(loss)

    def at(field):
        return pl.ds(field * PITCH, GROUP)

    def handle(g, c):
        ids = [order[g * GROUP + t] for t in range(GROUP)]
        numbers = [counts[t] for t in ids]
        places = [(t % per_row, pl.ds(pl.multiple_of(t // per_row * 8, 8), 8)) for t in ids]
        turn_count = functools.reduce(jnp.maximum, numbers)
        for t in range(GROUP):
            part, at_row = places[t]
            steps[t:t + 1, :] = jnp.full((1, LANES), numbers[t].astype(jnp.float32))
            for f in range(blocks):
                held[pl.ds(f * 8 * PITCH + t, 8, stride=PITCH)] = state[f * per_row + part, at_row, :]

        def advance(s, c):
            heat = jnp.tanh(held[at(warm_row)])
            for r in range(reactions):
                first = pl.ds(pair[r], GROUP)
                second = pl.ds(pair[reactions + r], GROUP)
                a = jnp.broadcast_to(rates[r:r + 1, :], (GROUP, LANES))
                e = jnp.broadcast_to(rates[reactions + r:reactions + r + 1, :], (GROUP, LANES))
                weight = jnp.broadcast_to(rates[2 * reactions + r:2 * reactions + r + 1, :], (GROUP, LANES))
                rate = jnp.exp2(a + e * heat)
                ca, cb = held[first], held[second]
                qa, qb = rate * ca, rate * cb
                progress[pl.ds(r, GROUP, stride=span)] = qa * (weight * cb)
                n = 2 * (r % (len(losses) // 2))
                losses[n][first] += qb
                losses[n + 1][second] += qa
            for q in range(GROUP // 2):
                p = jnp.concatenate([progress[pl.ds((2 * q + t) * span, depth)] for t in range(2)], 1)
                both = jnp.dot(table[...], p.astype(jnp.bfloat16), preferred_element_type=jnp.float32)
                total = both[:half] + both[half:]
                for t in range(2):
                    for f in range(blocks):
                        gained[pl.ds(f * 8 * PITCH + 2 * q + t, 8, stride=PITCH)] = (
                            total[f * 8:(f + 1) * 8, t * TILE:(t + 1) * TILE])
            number = steps[...]
            h = chemistry_span / number
            active = s.astype(jnp.float32) < number
            change = jnp.zeros((GROUP, LANES), jnp.float32)
            for j in range(species):
                x = held[at(j)]
                destroyed = functools.reduce(jnp.add, [loss[at(j)] for loss in losses])
                for loss in losses:
                    loss[at(j)] = jnp.zeros((GROUP, LANES), jnp.float32)
                updated = (x + h * gained[at(j)]) / (1.0 + h * destroyed)
                change = change + warming[j] * (updated - x)
                held[at(j)] = jnp.where(active, updated, x)
            w = held[at(warm_row)]
            held[at(warm_row)] = jnp.where(active, w + change, w)
            return c

        lax.fori_loop(0, turn_count, advance, 0)
        for t in range(GROUP):
            for f in range(0, warm_row + 1, 8):
                n = min(8, warm_row + 1 - f)
                staged[pl.ds(((ids[t] % per_row) * (warm_row + 1) + f) * rows + ids[t] // per_row, n, stride=rows)] = (
                    held[pl.ds(f * PITCH + t, n, stride=PITCH)])
        return c

    lax.fori_loop(0, tiles // GROUP, handle, 0)
    height = (warm_row + 1) * rows
    copies = []
    for n in range(per_row):
        lanes = pl.ds(n * TILE, TILE)
        copies.append(pltpu.make_async_copy(
            staged.at[pl.ds(n * height, warm_row * rows)], out.at[:, lanes], sems.at[0, n]))
        copies.append(pltpu.make_async_copy(
            staged.at[pl.ds(n * height + warm_row * rows, rows)], warm_out.at[:, lanes], sems.at[1, n]))
    for copy in copies:
        copy.start()
    for copy in copies:
        copy.wait()


LOSSES = 6


def chemistry(state, order, counts, pair, rates, warming, gain, rows, cols):
    species, reactions = gain.shape
    layers = state.shape[0] * LANES // cols * 8
    depth = -(-reactions // 16) * 16
    smem = pl.BlockSpec(memory_space=pltpu.SMEM)
    vmem = pl.BlockSpec(memory_space=pltpu.VMEM)
    block = pltpu.VMEM((layers * PITCH, LANES), jnp.float32)
    return pl.pallas_call(
        functools.partial(chemistry_kernel, reactions, species),
        in_specs=[smem, smem, smem, vmem, smem, vmem, vmem],
        out_specs=[pl.BlockSpec(memory_space=pl.ANY)] * 2,
        out_shape=[jax.ShapeDtypeStruct((species * rows, cols), jnp.float32),
                   jax.ShapeDtypeStruct((rows, cols), jnp.float32)],
        scratch_shapes=[block, block,
                        pltpu.VMEM((GROUP * (depth + 1), LANES), jnp.float32),
                        pltpu.VMEM((2 * -(-layers // 16) * 16, depth), jnp.bfloat16),
                        pltpu.VMEM((GROUP, LANES), jnp.float32),
                        pltpu.VMEM((cols // TILE * (species + 1) * rows, TILE), jnp.float32),
                        pltpu.SemaphoreType.DMA((2, cols // TILE))]
        + [block] * LOSSES,
        name="chemistry",
    )(order, counts, pair, rates, warming, state, gain)


def spread_weights(reactions):
    golden = (math.sqrt(5.0) - 1.0) / 2.0
    return jnp.asarray(np.exp2((np.arange(reactions) * golden) % 1.0), jnp.float32)


def by_count(counts):
    tiles = counts.shape[0]
    ids = jnp.arange(tiles, dtype=jnp.int32)
    key = counts * tiles + ids
    rank = jnp.sum((key[None, :] < key[:, None]).astype(jnp.int32), 1)
    return jnp.sum(jnp.where(rank[:, None] == ids[None, :], ids[:, None], 0), 0)


def body(component_density, scaled_thermal_state, leading_direction_flow, trailing_direction_flow,
         spreading_coefficient, colliding_pair, natural_exponent_scaler, arrhenius_energy,
         stoichiometric_output, formation_warming, explicit_increments):
    species, rows, cols = component_density.shape
    layers = up8(species + 3)
    spread = jnp.broadcast_to(jnp.pad(spreading_coefficient, (0, layers - species - 1))[:, None], (layers, LANES))
    clipped = advect(component_density, scaled_thermal_state, leading_direction_flow, trailing_direction_flow, spread)
    scale = 1.0 / math.log(2.0)
    weight = spread_weights(arrhenius_energy.shape[0])
    rates = jnp.concatenate([natural_exponent_scaler * scale, arrhenius_energy * scale, weight])
    rates = jnp.broadcast_to(rates[:, None], (rates.shape[0], LANES))
    pair = jnp.concatenate([colliding_pair[:, 0], colliding_pair[:, 1]]) * PITCH
    reacted, warm = chemistry(clipped, by_count(explicit_increments), explicit_increments, pair, rates,
                              formation_warming, stoichiometric_output.T / weight, rows, cols)
    return reacted.reshape(species, rows, cols), warm


def solution(mesh):
    return jax.shard_map(
        body,
        mesh=mesh,
        in_specs=(
            P(None, "gx", "grp"),
            P("gx", "grp"),
            P("gx", "grp"),
            P("gx", "grp"),
            P(),
            P(),
            P(),
            P(),
            P(),
            P(),
            P(("grp", "gx")),
        ),
        out_specs=(P(None, "gx", "grp"), P("gx", "grp")),
        check_vma=False,
    )
```

```python
import functools
import math

import jax
import jax.numpy as jnp
import numpy as np
from jax import lax
from jax.experimental import pallas as pl
from jax.experimental.pallas import tpu as pltpu
from jax.sharding import PartitionSpec as P

TILE = 128
FIRST_SCALE = 60.0
SECOND_SCALE = 180.0
transport_step = 0.4
chemistry_span = 0.5
sixth_first = (0.75, -0.15, 1.0 / 60.0)
sixth_second = (1.5, -0.15, 1.0 / 90.0)
sixth_center = -49.0 / 18.0


def up8(n):
    return -(-n // 8) * 8


REACH = 3
SLOT = 4
LANES = 128


def halves(value):
    high = value.astype(jnp.bfloat16)
    return high, (value - high.astype(jnp.float32)).astype(jnp.bfloat16)


def advect_kernel(fields, sizes, density, warm, leading, trailing, spread, band, out,
                  start, one, two, east, north, pieces, across, packed, landed, flows, send, recv):
    n_grp, n_gx = sizes
    g, x = lax.axis_index("grp"), lax.axis_index("gx")
    rows, cols = warm.shape
    parts = cols // LANES
    tiles = start.shape[0] // parts
    species = fields - 1
    last = fields // 8
    up, down = (g, lax.rem(x + n_gx - 1, n_gx)), (g, lax.rem(x + 1, n_gx))
    left, right = (lax.rem(g + n_grp - 1, n_grp), x), (lax.rem(g + 1, n_grp), x)
    barrier = pltpu.get_barrier_semaphore()
    for place in (up, down, left, right):
        pl.semaphore_signal(barrier, inc=1, device_id=place, device_id_type=pl.DeviceIdType.MESH)

    lane = lax.broadcasted_iota(jnp.int32, (8, LANES), 1)
    row_of = lane // SLOT
    slot = lane % SLOT

    def at(row):
        return pl.ds(row * 8 if isinstance(row, int) else pl.multiple_of(row * 8, 8), 8)

    def spread_out(read, t, sub):
        for q in range(rows // 8):
            for h in range(parts):
                start[t * parts + h, pl.ds((REACH + q * 8) * 8 + sub, 8, stride=8), :] = read(q, h)

    def of_density(f):
        return lambda q, h: density[pl.ds(pl.multiple_of(f * rows + q * 8, 8), 8), h * LANES:(h + 1) * LANES]

    def of_plane(ref):
        return lambda q, h: ref[q * 8:(q + 1) * 8, h * LANES:(h + 1) * LANES]

    def copies(s, t):
        held = (start, one, two)[s]
        both = pl.ds(t * parts, parts)
        plan = [
            (held.at[both, pl.ds(REACH * 8, REACH * 8)], held.at[both, pl.ds((REACH + rows) * 8, REACH * 8)], up),
            (held.at[both, pl.ds(rows * 8, REACH * 8)], held.at[both, pl.ds(0, REACH * 8)], down),
            (packed.at[s, t, 0], landed.at[s, t, 1], left),
            (packed.at[s, t, 1], landed.at[s, t, 0], right),
        ]
        return [pltpu.make_async_remote_copy(
            src_ref=src, dst_ref=dst, send_sem=send.at[s, t, n], recv_sem=recv.at[s, t, n],
            device_id=place, device_id_type=pl.DeviceIdType.MESH) for n, (src, dst, place) in enumerate(plan)]

    def pack(s, t):
        held = (start, one, two)[s]
        first = jnp.zeros((8, LANES), jnp.float32)
        final = jnp.zeros((8, LANES), jnp.float32)
        for i in range(rows):
            mine = row_of == i
            first = jnp.where(mine, pltpu.roll(held[t * parts, at(REACH + i), :], (SLOT * i) % LANES, 1), first)
            final = jnp.where(mine, pltpu.roll(held[t * parts + parts - 1, at(REACH + i), :],
                                               (SLOT * i + REACH) % LANES, 1), final)
        packed[s, t, 0] = first
        packed[s, t, 1] = final
        for copy in copies(s, t):
            copy.start()

    for f in range(last * 8, species):
        spread_out(of_density(f), last, f % 8)
    for n, ref in enumerate((warm, leading, trailing)):
        spread_out(of_plane(ref), last, (species + n) % 8)
    pl.semaphore_wait(barrier, 4)
    pack(0, last)

    def prepare(t, c):
        for sub in range(8):
            spread_out(of_density(t * 8 + sub), t, sub)
        pack(0, t)
        return c

    lax.fori_loop(0, last, prepare, 0)

    pull, push = transport_step * sixth_first[0], -transport_step / FIRST_SCALE
    for i in range(rows):
        for h in range(parts):
            lanes = slice(h * LANES, (h + 1) * LANES)
            east[h, at(REACH + i), :] = jnp.broadcast_to(pull * leading[i:i + 1, lanes], (8, LANES))
            north[h, at(i), :] = jnp.broadcast_to(push * trailing[i:i + 1, lanes], (8, LANES))

    def arrive(s, t):
        for copy in copies(s, t):
            copy.wait_recv()

    arrive(0, last)
    u_sub, v_sub = fields % 8, (fields + 1) % 8
    for r in (*range(REACH), *range(REACH + rows, 2 * REACH + rows)):
        for h in range(parts):
            east[h, at(r), :] = jnp.broadcast_to(
                pull * start[last * parts + h, pl.ds(r * 8 + u_sub, 1), :], (8, LANES))
    for side in range(2):
        flow = jnp.broadcast_to(landed[0, last, side, pl.ds(v_sub, 1), :], (8, LANES))
        for k in range(1, REACH + 1):
            inside = (slot >= REACH - k) & (slot < REACH) if side == 0 else slot < k
            weight = (1.0 if side == 0 else -1.0) * transport_step * sixth_first[k - 1]
            flows[side * REACH + k - 1] = jnp.where(inside, weight * flow, 0.0)

    def split(held, t):
        scale = spread[at(t), :] * (transport_step / SECOND_SCALE)
        for j in range(rows // 2):
            for h in range(parts):
                fs, gs = [], []
                for q in range(2):
                    i = 2 * j + q
                    f = held[t * parts + h, at(REACH + i), :]
                    fs.append(scale * f)
                    gs.append(north[h, at(i), :] * f)
                f_high, f_low = halves(jnp.concatenate(fs, 0))
                g_high, g_low = halves(jnp.concatenate(gs, 0))
                place = pl.ds(j * 16, 16)
                for m, piece in enumerate((f_high, f_low, g_high, g_low)):
                    pieces[place, m * cols + h * LANES:m * cols + (h + 1) * LANES] = piece

    def stage(s):
        held, fresh = (start, one, two)[s], (one, two, None)[s]

        def tile(n, c):
            t = lax.rem(n + last, tiles)

            @pl.when(n > 0 if s == 0 else n >= 0)
            def _():
                arrive(s, t)

            d = spread[at(t), :] * transport_step
            across[...] = jnp.dot(pieces[...], band[...], preferred_element_type=jnp.float32)
            split(held, lax.rem(t + 1, tiles))

            borders = []
            for side in range(2):
                halo = landed[s, t, side]
                total = None
                for k in range(1, REACH + 1):
                    inside = (slot >= REACH - k) & (slot < REACH) if side == 0 else slot < k
                    part = (jnp.where(inside, sixth_second[k - 1] * d, 0.0) + flows[side * REACH + k - 1]) * halo
                    if k < REACH:
                        part = pltpu.roll(part, (k - REACH) % LANES if side == 0 else REACH - k, 1)
                    total = part if total is None else total + part
                borders.append(total)
            ids = t * 8 + lax.broadcasted_iota(jnp.int32, (8, LANES), 0)
            reach = sixth_second[0] * d

            for b in range(rows // 8):
                for h in range(parts):
                    lanes = slice(h * LANES, (h + 1) * LANES)
                    f = [held[t * parts + h, at(b * 8 + m), :] for m in range(8 + 2 * REACH)]
                    gs = [east[h, at(b * 8 + m), :] * f[m] for m in range(8 + 2 * REACH)]
                    for r in range(8):
                        i = b * 8 + r
                        m = r + REACH
                        lap = (sixth_center / sixth_second[0]) * f[m] + (f[m + 1] + f[m - 1])
                        grad = gs[m + 1] - gs[m - 1]
                        for k in range(2, REACH + 1):
                            lap = lap + (sixth_second[k - 1] / sixth_second[0]) * (f[m + k] + f[m - k])
                            grad = grad + (sixth_first[k - 1] / sixth_first[0]) * (gs[m + k] - gs[m - k])
                        change = across[at(i), lanes] + (reach * lap - grad)
                        if h == 0:
                            change = change + jnp.where(
                                lane < REACH, pltpu.roll(borders[0], (LANES - SLOT * i) % LANES, 1), 0.0)
                        if h == parts - 1:
                            change = change + jnp.where(
                                lane >= LANES - REACH,
                                pltpu.roll(borders[1], (2 * LANES - REACH - SLOT * i) % LANES, 1), 0.0)
                        if s == 0:
                            fresh[t * parts + h, at(REACH + i), :] = f[m] + change
                        elif s == 1:
                            fresh[t * parts + h, at(REACH + i), :] = (
                                0.75 * start[t * parts + h, at(REACH + i), :] + 0.25 * (f[m] + change))
                        else:
                            value = start[t * parts + h, at(REACH + i), :] * (1.0 / 3.0) + (2.0 / 3.0) * (f[m] + change)
                            out[t * parts + h, at(i), :] = jnp.where(ids < species, jnp.maximum(value, 0.0), value)
            if s < 2:
                pack(s + 1, t)
            return c

        split(held, last)
        lax.fori_loop(0, tiles, tile, 0)

    for s in range(3):
        stage(s)

    def finish(t, c):
        for s in range(3):
            for copy in copies(s, t):
                copy.wait_send()
        return c

    lax.fori_loop(0, tiles, finish, 0)


def band_matrix(width):
    here = np.arange(width)
    lag = here[:, None] - here[None, :]
    second = np.where(lag == 0, round(sixth_center * SECOND_SCALE), 0)
    first = np.zeros((width, width))
    for k in range(1, REACH + 1):
        ahead, behind = lag == k, lag == -k
        second = np.where(ahead | behind, round(sixth_second[k - 1] * SECOND_SCALE), second)
        weight = round(sixth_first[k - 1] * FIRST_SCALE)
        first = np.where(ahead, weight, np.where(behind, -weight, first))
    return jnp.asarray(np.concatenate([second, second, first, first], 0), jnp.bfloat16)


def advect(density, warm, leading, trailing, spread):
    species, rows, cols = density.shape
    fields = species + 1
    tiles = (fields + 2) // 8
    if (fields + 2) % 8 or rows * SLOT > LANES or cols % LANES or rows % 8:
        raise ValueError("unsupported sizes")
    parts = cols // LANES
    sizes = (lax.axis_size("grp"), lax.axis_size("gx"))
    vmem = pl.BlockSpec(memory_space=pltpu.VMEM)
    wide = pltpu.VMEM((tiles * parts, (rows + 2 * REACH) * 8, LANES), jnp.float32)
    band = band_matrix(cols)
    return pl.pallas_call(
        functools.partial(advect_kernel, fields, sizes),
        in_specs=[vmem] * 6,
        out_specs=vmem,
        out_shape=jax.ShapeDtypeStruct((tiles * parts, rows * 8, LANES), jnp.float32),
        scratch_shapes=[wide, wide, wide,
                        pltpu.VMEM((parts, (rows + 2 * REACH) * 8, LANES), jnp.float32),
                        pltpu.VMEM((parts, rows * 8, LANES), jnp.float32),
                        pltpu.VMEM((rows * 8, 4 * cols), jnp.bfloat16),
                        pltpu.VMEM((rows * 8, cols), jnp.float32),
                        pltpu.VMEM((3, tiles, 2, 8, LANES), jnp.float32),
                        pltpu.VMEM((3, tiles, 2, 8, LANES), jnp.float32),
                        pltpu.VMEM((2 * REACH, 8, LANES), jnp.float32),
                        pltpu.SemaphoreType.DMA((3, tiles, 4)),
                        pltpu.SemaphoreType.DMA((3, tiles, 4))],
        compiler_params=pltpu.CompilerParams(collective_id=0, has_side_effects=True),
        name="advect",
    )(density.reshape(species * rows, cols), warm, leading, trailing, spread, band)


GROUP = 16
PITCH = GROUP + 1


def chemistry_kernel(reactions, species, order, counts, pair, rates, warming, state, gain, out, warm_out,
                     held, gained, progress, table, steps, staged, sems, *losses):
    rows, cols = warm_out.shape
    layers = state.shape[0] * LANES // cols * 8
    per_row = cols // TILE
    tiles = rows * per_row
    warm_row = species
    span = progress.shape[0] // GROUP
    depth = span // 8 * 8
    half = table.shape[0] // 2
    blocks = layers // 8

    progress[...] = jnp.zeros_like(progress)
    table[...] = jnp.zeros_like(table)
    high, low = halves(gain[...])
    table[0:species, 0:reactions] = high
    table[half:half + species, 0:reactions] = low
    for loss in losses:
        loss[...] = jnp.zeros_like(loss)

    def at(field):
        return pl.ds(field * PITCH, GROUP)

    def handle(g, c):
        ids = [order[g * GROUP + t] for t in range(GROUP)]
        numbers = [counts[t] for t in ids]
        places = [(t % per_row, pl.ds(pl.multiple_of(t // per_row * 8, 8), 8)) for t in ids]
        turn_count = functools.reduce(jnp.maximum, numbers)
        for t in range(GROUP):
            part, at_row = places[t]
            steps[t:t + 1, :] = jnp.full((1, LANES), numbers[t].astype(jnp.float32))
            for f in range(blocks):
                held[pl.ds(f * 8 * PITCH + t, 8, stride=PITCH)] = state[f * per_row + part, at_row, :]

        def advance(s, c):
            heat = jnp.tanh(held[at(warm_row)])
            for r in range(reactions):
                first = pl.ds(pair[r], GROUP)
                second = pl.ds(pair[reactions + r], GROUP)
                a = jnp.broadcast_to(rates[r:r + 1, :], (GROUP, LANES))
                e = jnp.broadcast_to(rates[reactions + r:reactions + r + 1, :], (GROUP, LANES))
                weight = jnp.broadcast_to(rates[2 * reactions + r:2 * reactions + r + 1, :], (GROUP, LANES))
                rate = jnp.exp2(a + e * heat)
                ca, cb = held[first], held[second]
                qa, qb = rate * ca, rate * cb
                progress[pl.ds(r, GROUP, stride=span)] = qa * (weight * cb)
                n = 2 * (r % (len(losses) // 2))
                losses[n][first] += qb
                losses[n + 1][second] += qa
            for q in range(GROUP // 2):
                p = jnp.concatenate([progress[pl.ds((2 * q + t) * span, depth)] for t in range(2)], 1)
                both = jnp.dot(table[...], p.astype(jnp.bfloat16), preferred_element_type=jnp.float32)
                total = both[:half] + both[half:]
                for t in range(2):
                    for f in range(blocks):
                        gained[pl.ds(f * 8 * PITCH + 2 * q + t, 8, stride=PITCH)] = (
                            total[f * 8:(f + 1) * 8, t * TILE:(t + 1) * TILE])
            number = steps[...]
            h = chemistry_span / number
            active = s.astype(jnp.float32) < number
            change = jnp.zeros((GROUP, LANES), jnp.float32)
            for j in range(species):
                x = held[at(j)]
                destroyed = functools.reduce(jnp.add, [loss[at(j)] for loss in losses])
                for loss in losses:
                    loss[at(j)] = jnp.zeros((GROUP, LANES), jnp.float32)
                updated = (x + h * gained[at(j)]) / (1.0 + h * destroyed)
                change = change + warming[j] * (updated - x)
                held[at(j)] = jnp.where(active, updated, x)
            w = held[at(warm_row)]
            held[at(warm_row)] = jnp.where(active, w + change, w)
            return c

        lax.fori_loop(0, turn_count, advance, 0)
        for t in range(GROUP):
            for f in range(0, warm_row + 1, 8):
                n = min(8, warm_row + 1 - f)
                staged[pl.ds(((ids[t] % per_row) * (warm_row + 1) + f) * rows + ids[t] // per_row, n, stride=rows)] = (
                    held[pl.ds(f * PITCH + t, n, stride=PITCH)])
        return c

    lax.fori_loop(0, tiles // GROUP, handle, 0)
    height = (warm_row + 1) * rows
    copies = []
    for n in range(per_row):
        lanes = pl.ds(n * TILE, TILE)
        copies.append(pltpu.make_async_copy(
            staged.at[pl.ds(n * height, warm_row * rows)], out.at[:, lanes], sems.at[0, n]))
        copies.append(pltpu.make_async_copy(
            staged.at[pl.ds(n * height + warm_row * rows, rows)], warm_out.at[:, lanes], sems.at[1, n]))
    for copy in copies:
        copy.start()
    for copy in copies:
        copy.wait()


LOSSES = 6


def chemistry(state, order, counts, pair, rates, warming, gain, rows, cols):
    species, reactions = gain.shape
    layers = state.shape[0] * LANES // cols * 8
    depth = -(-reactions // 16) * 16
    smem = pl.BlockSpec(memory_space=pltpu.SMEM)
    vmem = pl.BlockSpec(memory_space=pltpu.VMEM)
    block = pltpu.VMEM((layers * PITCH, LANES), jnp.float32)
    return pl.pallas_call(
        functools.partial(chemistry_kernel, reactions, species),
        in_specs=[smem, smem, smem, vmem, smem, vmem, vmem],
        out_specs=[pl.BlockSpec(memory_space=pl.ANY)] * 2,
        out_shape=[jax.ShapeDtypeStruct((species * rows, cols), jnp.float32),
                   jax.ShapeDtypeStruct((rows, cols), jnp.float32)],
        scratch_shapes=[block, block,
                        pltpu.VMEM((GROUP * (depth + 1), LANES), jnp.float32),
                        pltpu.VMEM((2 * -(-layers // 16) * 16, depth), jnp.bfloat16),
                        pltpu.VMEM((GROUP, LANES), jnp.float32),
                        pltpu.VMEM((cols // TILE * (species + 1) * rows, TILE), jnp.float32),
                        pltpu.SemaphoreType.DMA((2, cols // TILE))]
        + [block] * LOSSES,
        name="chemistry",
    )(order, counts, pair, rates, warming, state, gain)


def spread_weights(reactions):
    golden = (math.sqrt(5.0) - 1.0) / 2.0
    return jnp.asarray(np.exp2((np.arange(reactions) * golden) % 1.0), jnp.float32)


def by_count(counts):
    tiles = counts.shape[0]
    ids = jnp.arange(tiles, dtype=jnp.int32)
    key = counts * tiles + ids
    rank = jnp.sum((key[None, :] < key[:, None]).astype(jnp.int32), 1)
    return jnp.sum(jnp.where(rank[:, None] == ids[None, :], ids[:, None], 0), 0)


def body(component_density, scaled_thermal_state, leading_direction_flow, trailing_direction_flow,
         spreading_coefficient, colliding_pair, natural_exponent_scaler, arrhenius_energy,
         stoichiometric_output, formation_warming, explicit_increments):
    species, rows, cols = component_density.shape
    layers = up8(species + 3)
    spread = jnp.broadcast_to(jnp.pad(spreading_coefficient, (0, layers - species - 1))[:, None], (layers, LANES))
    clipped = advect(component_density, scaled_thermal_state, leading_direction_flow, trailing_direction_flow, spread)
    scale = 1.0 / math.log(2.0)
    weight = spread_weights(arrhenius_energy.shape[0])
    rates = jnp.concatenate([natural_exponent_scaler * scale, arrhenius_energy * scale, weight])
    rates = jnp.broadcast_to(rates[:, None], (rates.shape[0], LANES))
    pair = jnp.concatenate([colliding_pair[:, 0], colliding_pair[:, 1]]) * PITCH
    reacted, warm = chemistry(clipped, by_count(explicit_increments), explicit_increments, pair, rates,
                              formation_warming, stoichiometric_output.T / weight, rows, cols)
    return reacted.reshape(species, rows, cols), warm


def solution(mesh):
    return jax.shard_map(
        body,
        mesh=mesh,
        in_specs=(
            P(None, "gx", "grp"),
            P("gx", "grp"),
            P("gx", "grp"),
            P("gx", "grp"),
            P(),
            P(),
            P(),
            P(),
            P(),
            P(),
            P(("grp", "gx")),
        ),
        out_specs=(P(None, "gx", "grp"), P("gx", "grp")),
        check_vma=False,
    )
```

```python
import functools
import math

import jax
import jax.numpy as jnp
import numpy as np
from jax import lax
from jax.experimental import pallas as pl
from jax.experimental.pallas import tpu as pltpu
from jax.sharding import PartitionSpec as P

TILE = 128
FIRST_SCALE = 60.0
SECOND_SCALE = 180.0
transport_step = 0.4
chemistry_span = 0.5
sixth_first = (0.75, -0.15, 1.0 / 60.0)
sixth_second = (1.5, -0.15, 1.0 / 90.0)
sixth_center = -49.0 / 18.0


def up(n, m):
    return -(-n // m) * m


def spread_weights(reactions):
    golden = (math.sqrt(5.0) - 1.0) / 2.0
    return np.exp2((np.arange(reactions) * golden) % 1.0).astype(np.float32)


REACH = 3
SLOT = 4
LANES = 128
NEVER = -16384.0
TRIPS = 3


def halves(value):
    high = value.astype(jnp.bfloat16)
    return high, (value - high.astype(jnp.float32)).astype(jnp.bfloat16)


def prepare_tables(pair, scaler, energy, produced, weight, counts, rates, table, offsets, order, lines):
    reactions = pair.shape[1]
    length = rates.shape[0] // 3
    species = produced.shape[0]
    half = table.shape[0] // 2
    scale = 1.0 / math.log(2.0)
    wide = lines.shape[1]
    lines[...] = jnp.zeros_like(lines)
    lines[0:1, :] = jnp.full((1, wide), NEVER)
    lines[0:1, 0:reactions] = scaler[...] * scale
    lines[1:2, 0:reactions] = energy[...] * scale
    lines[2:3, 0:reactions] = weight[...]
    for n in range(3):
        for r in range(0, length, LANES):
            count = min(LANES, length - r)
            row = jnp.broadcast_to(lines[n:n + 1, r:r + LANES], (LANES, LANES))
            rates[n * length + r:n * length + r + count, :] = row.T[:count]
    table[...] = jnp.zeros_like(table)
    high, low = halves(produced[...] / weight[...])
    table[0:species, 0:reactions] = high
    table[half:half + species, 0:reactions] = low
    offsets[...] = jnp.zeros_like(offsets)
    for n in range(2):
        offsets[:, n * wide:n * wide + reactions] = pair[n:n + 1, :] * PITCH
    tiles = counts.shape[1]
    lines[3:4, 0:tiles] = counts[...].astype(jnp.float32) * tiles
    key = lines[3:4, 0:LANES] + lax.broadcasted_iota(jnp.int32, (1, LANES), 1).astype(jnp.float32)
    down = lax.broadcasted_iota(jnp.int32, (LANES, LANES), 0).astype(jnp.float32)
    along = lax.broadcasted_iota(jnp.int32, (LANES, LANES), 1)
    across = jnp.broadcast_to(key, (LANES, LANES))
    before = jnp.where((across < across.T) & (along < tiles), 1.0, 0.0)
    rank = jnp.sum(before, axis=1, keepdims=True)
    here = jnp.where((rank == along.astype(jnp.float32)) & (down < tiles), down, 0.0)
    order[...] = jnp.sum(here, axis=0, keepdims=True).astype(jnp.int32)


def advect_kernel(fields, sizes, density, warm, leading, trailing, diffusion, band, pair, scaler, energy, produced,
                  weight, counts, out, rates, table, offsets, order,
                  lines, spread, start, one, two, east, north, pieces, across, packed, landed, flows, send, recv):
    n_grp, n_gx = sizes
    g, x = lax.axis_index("grp"), lax.axis_index("gx")
    rows, cols = warm.shape
    parts = cols // LANES
    tiles = start.shape[0] // parts
    species = fields - 1
    last = fields // 8
    up, down = (g, lax.rem(x + n_gx - 1, n_gx)), (g, lax.rem(x + 1, n_gx))
    left, right = (lax.rem(g + n_grp - 1, n_grp), x), (lax.rem(g + 1, n_grp), x)
    barrier = pltpu.get_barrier_semaphore()
    for place in (up, down, left, right):
        pl.semaphore_signal(barrier, inc=1, device_id=place, device_id_type=pl.DeviceIdType.MESH)

    lane = lax.broadcasted_iota(jnp.int32, (8, LANES), 1)
    row_of = lane // SLOT
    slot = lane % SLOT

    def at(row):
        return pl.ds(row * 8 if isinstance(row, int) else pl.multiple_of(row * 8, 8), 8)

    def spread_out(read, t, sub):
        for q in range(rows // 8):
            for h in range(parts):
                start[t * parts + h, pl.ds((REACH + q * 8) * 8 + sub, 8, stride=8), :] = read(q, h)

    def of_density(f):
        return lambda q, h: density[pl.ds(pl.multiple_of(f * rows + q * 8, 8), 8), h * LANES:(h + 1) * LANES]

    def of_plane(ref):
        return lambda q, h: ref[q * 8:(q + 1) * 8, h * LANES:(h + 1) * LANES]

    def copies(s, t):
        held = (start, one, two)[s]
        both = pl.ds(t * parts, parts)
        plan = [
            (held.at[both, pl.ds(REACH * 8, REACH * 8)], held.at[both, pl.ds((REACH + rows) * 8, REACH * 8)], up),
            (held.at[both, pl.ds(rows * 8, REACH * 8)], held.at[both, pl.ds(0, REACH * 8)], down),
            (packed.at[s, t, 0], landed.at[s, t, 1], left),
            (packed.at[s, t, 1], landed.at[s, t, 0], right),
        ]
        return [pltpu.make_async_remote_copy(
            src_ref=src, dst_ref=dst, send_sem=send.at[s, t, n], recv_sem=recv.at[s, t, n],
            device_id=place, device_id_type=pl.DeviceIdType.MESH) for n, (src, dst, place) in enumerate(plan)]

    def pack(s, t):
        held = (start, one, two)[s]
        first = jnp.zeros((8, LANES), jnp.float32)
        final = jnp.zeros((8, LANES), jnp.float32)
        for i in range(rows):
            mine = row_of == i
            first = jnp.where(mine, pltpu.roll(held[t * parts, at(REACH + i), :], (SLOT * i) % LANES, 1), first)
            final = jnp.where(mine, pltpu.roll(held[t * parts + parts - 1, at(REACH + i), :],
                                               (SLOT * i + REACH) % LANES, 1), final)
        packed[s, t, 0] = first
        packed[s, t, 1] = final
        for copy in copies(s, t):
            copy.start()

    for f in range(tiles * 8):
        spread[f:f + 1, :] = jnp.full((1, LANES), diffusion[f] if f < fields else 0.0)
    for f in range(last * 8, species):
        spread_out(of_density(f), last, f % 8)
    for n, ref in enumerate((warm, leading, trailing)):
        spread_out(of_plane(ref), last, (species + n) % 8)
    pl.semaphore_wait(barrier, 4)
    pack(0, last)

    def prepare(t, c):
        for sub in range(8):
            spread_out(of_density(t * 8 + sub), t, sub)
        pack(0, t)
        return c

    lax.fori_loop(0, last, prepare, 0)

    pull, push = transport_step * sixth_first[0], -transport_step / FIRST_SCALE
    for i in range(rows):
        for h in range(parts):
            lanes = slice(h * LANES, (h + 1) * LANES)
            east[h, at(REACH + i), :] = jnp.broadcast_to(pull * leading[i:i + 1, lanes], (8, LANES))
            north[h, at(i), :] = jnp.broadcast_to(push * trailing[i:i + 1, lanes], (8, LANES))

    def arrive(s, t):
        for copy in copies(s, t):
            copy.wait_recv()

    prepare_tables(pair, scaler, energy, produced, weight, counts, rates, table, offsets, order, lines)
    arrive(0, last)
    u_sub, v_sub = fields % 8, (fields + 1) % 8
    for r in (*range(REACH), *range(REACH + rows, 2 * REACH + rows)):
        for h in range(parts):
            east[h, at(r), :] = jnp.broadcast_to(
                pull * start[last * parts + h, pl.ds(r * 8 + u_sub, 1), :], (8, LANES))
    for side in range(2):
        flow = jnp.broadcast_to(landed[0, last, side, pl.ds(v_sub, 1), :], (8, LANES))
        for k in range(1, REACH + 1):
            inside = (slot >= REACH - k) & (slot < REACH) if side == 0 else slot < k
            weight = (1.0 if side == 0 else -1.0) * transport_step * sixth_first[k - 1]
            flows[side * REACH + k - 1] = jnp.where(inside, weight * flow, 0.0)

    def split(held, t):
        scale = spread[at(t), :] * (transport_step / SECOND_SCALE)
        for j in range(rows // 2):
            for h in range(parts):
                fs, gs = [], []
                for q in range(2):
                    i = 2 * j + q
                    f = held[t * parts + h, at(REACH + i), :]
                    fs.append(scale * f)
                    gs.append(north[h, at(i), :] * f)
                f_high, f_low = halves(jnp.concatenate(fs, 0))
                g_high, g_low = halves(jnp.concatenate(gs, 0))
                place = pl.ds(j * 16, 16)
                for m, piece in enumerate((f_high, f_low, g_high, g_low)):
                    pieces[place, m * cols + h * LANES:m * cols + (h + 1) * LANES] = piece

    def stage(s):
        held, fresh = (start, one, two)[s], (one, two, None)[s]

        def tile(n, c):
            t = lax.rem(n + last, tiles)

            @pl.when(n > 0 if s == 0 else n >= 0)
            def _():
                arrive(s, t)

            d = spread[at(t), :] * transport_step
            across[...] = jnp.dot(pieces[...], band[...], preferred_element_type=jnp.float32)
            split(held, lax.rem(t + 1, tiles))

            borders = []
            for side in range(2):
                halo = landed[s, t, side]
                total = None
                for k in range(1, REACH + 1):
                    inside = (slot >= REACH - k) & (slot < REACH) if side == 0 else slot < k
                    part = (jnp.where(inside, sixth_second[k - 1] * d, 0.0) + flows[side * REACH + k - 1]) * halo
                    if k < REACH:
                        part = pltpu.roll(part, (k - REACH) % LANES if side == 0 else REACH - k, 1)
                    total = part if total is None else total + part
                borders.append(total)
            ids = t * 8 + lax.broadcasted_iota(jnp.int32, (8, LANES), 0)
            reach = sixth_second[0] * d

            for b in range(rows // 8):
                for h in range(parts):
                    lanes = slice(h * LANES, (h + 1) * LANES)
                    f = [held[t * parts + h, at(b * 8 + m), :] for m in range(8 + 2 * REACH)]
                    gs = [east[h, at(b * 8 + m), :] * f[m] for m in range(8 + 2 * REACH)]
                    for r in range(8):
                        i = b * 8 + r
                        m = r + REACH
                        lap = (sixth_center / sixth_second[0]) * f[m] + (f[m + 1] + f[m - 1])
                        grad = gs[m + 1] - gs[m - 1]
                        for k in range(2, REACH + 1):
                            lap = lap + (sixth_second[k - 1] / sixth_second[0]) * (f[m + k] + f[m - k])
                            grad = grad + (sixth_first[k - 1] / sixth_first[0]) * (gs[m + k] - gs[m - k])
                        change = across[at(i), lanes] + (reach * lap - grad)
                        if h == 0:
                            change = change + jnp.where(
                                lane < REACH, pltpu.roll(borders[0], (LANES - SLOT * i) % LANES, 1), 0.0)
                        if h == parts - 1:
                            change = change + jnp.where(
                                lane >= LANES - REACH,
                                pltpu.roll(borders[1], (2 * LANES - REACH - SLOT * i) % LANES, 1), 0.0)
                        if s == 0:
                            fresh[t * parts + h, at(REACH + i), :] = f[m] + change
                        elif s == 1:
                            fresh[t * parts + h, at(REACH + i), :] = (
                                0.75 * start[t * parts + h, at(REACH + i), :] + 0.25 * (f[m] + change))
                        else:
                            value = start[t * parts + h, at(REACH + i), :] * (1.0 / 3.0) + (2.0 / 3.0) * (f[m] + change)
                            out[t * parts + h, at(i), :] = jnp.where(ids < species, jnp.maximum(value, 0.0), value)
            if s < 2:
                pack(s + 1, t)
            return c

        split(held, last)
        lax.fori_loop(0, tiles, tile, 0)

    for s in range(3):
        stage(s)

    def finish(t, c):
        for s in range(3):
            for copy in copies(s, t):
                copy.wait_send()
        return c

    lax.fori_loop(0, tiles, finish, 0)


def band_matrix(width):
    here = np.arange(width)
    lag = here[:, None] - here[None, :]
    second = np.where(lag == 0, round(sixth_center * SECOND_SCALE), 0)
    first = np.zeros((width, width))
    for k in range(1, REACH + 1):
        ahead, behind = lag == k, lag == -k
        second = np.where(ahead | behind, round(sixth_second[k - 1] * SECOND_SCALE), second)
        weight = round(sixth_first[k - 1] * FIRST_SCALE)
        first = np.where(ahead, weight, np.where(behind, -weight, first))
    return jnp.asarray(np.concatenate([second, second, first, first], 0), jnp.bfloat16)


def advect(density, warm, leading, trailing, diffusion, pair, scaler, energy, produced, counts):
    species, rows, cols = density.shape
    fields = species + 1
    tiles = (fields + 2) // 8
    if (fields + 2) % 8 or rows * SLOT > LANES or cols % LANES or rows % 8:
        raise ValueError("unsupported sizes")
    parts = cols // LANES
    sizes = (lax.axis_size("grp"), lax.axis_size("gx"))
    vmem = pl.BlockSpec(memory_space=pltpu.VMEM)
    wide = pltpu.VMEM((tiles * parts, (rows + 2 * REACH) * 8, LANES), jnp.float32)
    band = band_matrix(cols)
    reactions = pair.shape[1]
    if counts.shape[1] > LANES or species > 64:
        raise ValueError("unsupported sizes")
    length = up(up(reactions, TRIPS), 8)
    weight = spread_weights(reactions)[None]
    smem = pl.BlockSpec(memory_space=pltpu.SMEM)
    return pl.pallas_call(
        functools.partial(advect_kernel, fields, sizes),
        in_specs=[vmem] * 4 + [smem] + [vmem] * 7,
        out_specs=[vmem] * 5,
        out_shape=[jax.ShapeDtypeStruct((tiles * parts, rows * 8, LANES), jnp.float32),
                   jax.ShapeDtypeStruct((3 * length, LANES), jnp.float32),
                   jax.ShapeDtypeStruct((2 * up(species, 8), up(length, 16)), jnp.bfloat16),
                   jax.ShapeDtypeStruct((1, 2 * up(length, LANES)), jnp.int32),
                   jax.ShapeDtypeStruct((1, LANES), jnp.int32)],
        scratch_shapes=[pltpu.VMEM((8, up(length, LANES)), jnp.float32),
                        pltpu.VMEM((tiles * 8, LANES), jnp.float32), wide, wide, wide,
                        pltpu.VMEM((parts, (rows + 2 * REACH) * 8, LANES), jnp.float32),
                        pltpu.VMEM((parts, rows * 8, LANES), jnp.float32),
                        pltpu.VMEM((rows * 8, 4 * cols), jnp.bfloat16),
                        pltpu.VMEM((rows * 8, cols), jnp.float32),
                        pltpu.VMEM((3, tiles, 2, 8, LANES), jnp.float32),
                        pltpu.VMEM((3, tiles, 2, 8, LANES), jnp.float32),
                        pltpu.VMEM((2 * REACH, 8, LANES), jnp.float32),
                        pltpu.SemaphoreType.DMA((3, tiles, 4)),
                        pltpu.SemaphoreType.DMA((3, tiles, 4))],
        compiler_params=pltpu.CompilerParams(collective_id=0, has_side_effects=True),
        name="advect",
    )(density.reshape(species * rows, cols), warm, leading, trailing, diffusion, band, pair, scaler, energy, produced,
      weight, counts)


GROUP = 16
PITCH = GROUP + 1
SPAN = 9


def chemistry_kernel(species, chunk, order, counts, pair, warming, rates, table, state, out, warm_out,
                     held, low_gained, high_gained, progress, steps, staged, sems, *losses):
    rows, cols = warm_out.shape
    layers = state.shape[0] * LANES // cols * 8
    per_row = cols // TILE
    tiles = rows * per_row
    warm_row = species
    length = rates.shape[0] // 3
    reactions = length // chunk * chunk
    span = progress.shape[0] // GROUP
    depth = table.shape[1]
    half = table.shape[0] // 2
    blocks = layers // 8
    lines = staged.reshape(staged.shape[0] * staged.shape[1], LANES)
    line_span = staged.shape[1]
    gained = (low_gained, high_gained)

    for t in range(GROUP):
        progress[pl.ds(t * span + reactions, depth - reactions)] = jnp.zeros((depth - reactions, LANES), jnp.float32)
    for loss in losses:
        loss[...] = jnp.zeros_like(loss)

    def at(field):
        return pl.ds(field * PITCH, GROUP)

    def handle(g, c):
        ids = [order[0, g * GROUP + t] for t in range(GROUP)]
        numbers = [counts[t] for t in ids]
        places = [(t % per_row, pl.ds(pl.multiple_of(t // per_row * 8, 8), 8)) for t in ids]
        turn_count = functools.reduce(jnp.maximum, numbers)
        for t in range(GROUP):
            part, at_row = places[t]
            steps[t:t + 1, :] = jnp.full((1, LANES), numbers[t].astype(jnp.float32))
            for f in range(blocks):
                held[pl.ds(f * 8 * PITCH + t, 8, stride=PITCH)] = state[f * per_row + part, at_row, :]

        def advance(s, c):
            heat = jnp.tanh(held[at(warm_row)])

            def react(k, c):
                for j in range(chunk):
                    r = k * chunk + j
                    first = pl.ds(pair[0, r], GROUP)
                    second = pl.ds(pair[0, pair.shape[1] // 2 + r], GROUP)
                    a, e, weight = [jnp.broadcast_to(rates[pl.ds(n * length + r, 1), :], (GROUP, LANES)) for n in range(3)]
                    rate = jnp.exp2(a + e * heat)
                    ca, cb = held[first], held[second]
                    qa, qb = rate * ca, rate * cb
                    progress[pl.ds(r, GROUP, stride=span)] = qa * (weight * cb)
                    n = 2 * (j % (len(losses) // 2))
                    losses[n][first] += qb
                    losses[n + 1][second] += qa
                return c

            lax.fori_loop(0, reactions // chunk, react, 0)
            for n, fill in enumerate(gained):
                for q in range(4 * n, 4 * n + 4):
                    p = jnp.concatenate([progress[pl.ds((2 * q + t) * span, depth)] for t in range(2)], 1)
                    both = jnp.dot(table[...], p.astype(jnp.bfloat16), preferred_element_type=jnp.float32)
                    total = both[:half] + both[half:]
                    for t in range(2):
                        for f in range(half // 8):
                            fill[pl.ds(f * 8 * SPAN + 2 * (q - 4 * n) + t, 8, stride=SPAN)] = (
                                total[f * 8:(f + 1) * 8, t * TILE:(t + 1) * TILE])
                number = steps[8 * n:8 * n + 8, :]
                pace = number * (1.0 / chemistry_span)
                active = s.astype(jnp.float32) < number
                change = jnp.zeros((8, LANES), jnp.float32)
                for j in range(species):
                    place = pl.ds(j * PITCH + 8 * n, 8)
                    x = held[place]
                    destroyed = functools.reduce(jnp.add, [loss[place] for loss in losses])
                    for loss in losses:
                        loss[place] = jnp.zeros((8, LANES), jnp.float32)
                    updated = (pace * x + fill[pl.ds(j * SPAN, 8)]) / (pace + destroyed)
                    change = change + warming[j] * (updated - x)
                    held[place] = jnp.where(active, updated, x)
                place = pl.ds(warm_row * PITCH + 8 * n, 8)
                w = held[place]
                held[place] = jnp.where(active, w + change, w)
            return c

        lax.fori_loop(0, turn_count, advance, 0)
        for t in range(GROUP):
            line = (ids[t] % per_row) * ((warm_row + 1) * line_span) + ids[t] // per_row
            for f in range(0, warm_row + 1, 8):
                n = min(8, warm_row + 1 - f)
                lines[pl.ds(line + f * line_span, n, stride=line_span)] = held[pl.ds(f * PITCH + t, n, stride=PITCH)]
        return c

    lax.fori_loop(0, tiles // GROUP, handle, 0)
    wide = out.reshape(species, rows, cols)
    copies = []
    for n in range(per_row):
        lanes = pl.ds(n * TILE, TILE)
        first = n * (warm_row + 1)
        copies.append(pltpu.make_async_copy(
            staged.at[pl.ds(first, species), pl.ds(0, rows)], wide.at[:, :, lanes], sems.at[0, n]))
        copies.append(pltpu.make_async_copy(
            staged.at[first + species, pl.ds(0, rows)], warm_out.at[:, lanes], sems.at[1, n]))
    for copy in copies:
        copy.start()
    for copy in copies:
        copy.wait()


LOSSES = 4


def chemistry(state, order, counts, pair, warming, rates, table, species, rows, cols):
    layers = state.shape[0] * LANES // cols * 8
    smem = pl.BlockSpec(memory_space=pltpu.SMEM)
    vmem = pl.BlockSpec(memory_space=pltpu.VMEM)
    block = pltpu.VMEM((layers * PITCH, LANES), jnp.float32)
    part = pltpu.VMEM((layers * SPAN, LANES), jnp.float32)
    return pl.pallas_call(
        functools.partial(chemistry_kernel, species, rates.shape[0] // 3 // TRIPS),
        in_specs=[smem, smem, smem, smem, vmem, vmem, vmem],
        out_specs=[pl.BlockSpec(memory_space=pl.ANY)] * 2,
        out_shape=[jax.ShapeDtypeStruct((species * rows, cols), jnp.float32),
                   jax.ShapeDtypeStruct((rows, cols), jnp.float32)],
        scratch_shapes=[block, part, part,
                        pltpu.VMEM((GROUP * (table.shape[1] + 1), LANES), jnp.float32),
                        pltpu.VMEM((GROUP, LANES), jnp.float32),
                        pltpu.VMEM((cols // TILE * (species + 1), rows + 8, TILE), jnp.float32),
                        pltpu.SemaphoreType.DMA((2, cols // TILE))]
        + [block] * LOSSES,
        name="chemistry",
    )(order, counts, pair, warming, rates, table, state)


def body(component_density, scaled_thermal_state, leading_direction_flow, trailing_direction_flow,
         spreading_coefficient, colliding_pair, natural_exponent_scaler, arrhenius_energy,
         stoichiometric_output, formation_warming, explicit_increments):
    species, rows, cols = component_density.shape
    clipped, rates, table, pair, order = advect(
        component_density, scaled_thermal_state, leading_direction_flow, trailing_direction_flow, spreading_coefficient,
        colliding_pair.T, natural_exponent_scaler[None], arrhenius_energy[None], stoichiometric_output.T,
        explicit_increments[None])
    reacted, warm = chemistry(clipped, order, explicit_increments, pair, formation_warming, rates, table,
                              species, rows, cols)
    return reacted.reshape(species, rows, cols), warm


def solution(mesh):
    return jax.shard_map(
        body,
        mesh=mesh,
        in_specs=(
            P(None, "gx", "grp"),
            P("gx", "grp"),
            P("gx", "grp"),
            P("gx", "grp"),
            P(),
            P(),
            P(),
            P(),
            P(),
            P(),
            P(("grp", "gx")),
        ),
        out_specs=(P(None, "gx", "grp"), P("gx", "grp")),
        check_vma=False,
    )
```

```python
import functools
import math

import jax
import jax.numpy as jnp
import numpy as np
from jax import lax
from jax.experimental import pallas as pl
from jax.experimental.pallas import tpu as pltpu
from jax.sharding import PartitionSpec as P

TILE = 128
FIRST_SCALE = 60.0
SECOND_SCALE = 180.0
transport_step = 0.4
chemistry_span = 0.5
sixth_first = (0.75, -0.15, 1.0 / 60.0)
sixth_second = (1.5, -0.15, 1.0 / 90.0)
sixth_center = -49.0 / 18.0


def up(n, m):
    return -(-n // m) * m


def spread_weights(reactions):
    golden = (math.sqrt(5.0) - 1.0) / 2.0
    return np.exp2((np.arange(reactions) * golden) % 1.0).astype(np.float32)


REACH = 3
SLOT = 4
LANES = 128
NEVER = -16384.0
TRIPS = 3
ROOM = 32 << 20


def halves(value):
    high = value.astype(jnp.bfloat16)
    return high, (value - high.astype(jnp.float32)).astype(jnp.bfloat16)


def prepare_tables(pair, scaler, energy, produced, weight, counts, rates, table, offsets, order, lines):
    reactions = pair.shape[1]
    length = rates.shape[0] // 3
    species = produced.shape[0]
    half = table.shape[0] // 2
    scale = 1.0 / math.log(2.0)
    wide = lines.shape[1]
    lines[...] = jnp.zeros_like(lines)
    lines[0:1, :] = jnp.full((1, wide), NEVER)
    lines[0, 0:reactions] = scaler[...] * scale
    lines[1, 0:reactions] = energy[...] * scale
    lines[2:3, 0:reactions] = weight[...]
    for n in range(3):
        for r in range(0, length, LANES):
            count = min(LANES, length - r)
            row = jnp.broadcast_to(lines[n:n + 1, r:r + LANES], (LANES, LANES))
            rates[n * length + r:n * length + r + count, :] = row.T[:count]
    table[...] = jnp.zeros_like(table)
    high, low = halves(produced[...] / weight[...])
    table[0:species, 0:reactions] = high
    table[half:half + species, 0:reactions] = low
    offsets[...] = jnp.zeros_like(offsets)
    for n in range(2):
        offsets[:, n * wide:n * wide + reactions] = pair[n:n + 1, :] * PITCH
    tiles = counts.shape[1]
    lines[3:4, 0:tiles] = counts[...].astype(jnp.float32) * tiles
    key = lines[3:4, 0:LANES] + lax.broadcasted_iota(jnp.int32, (1, LANES), 1).astype(jnp.float32)
    down = lax.broadcasted_iota(jnp.int32, (LANES, LANES), 0).astype(jnp.float32)
    along = lax.broadcasted_iota(jnp.int32, (LANES, LANES), 1)
    across = jnp.broadcast_to(key, (LANES, LANES))
    before = jnp.where((across < across.T) & (along < tiles), 1.0, 0.0)
    rank = jnp.sum(before, axis=1, keepdims=True)
    here = jnp.where((rank == along.astype(jnp.float32)) & (down < tiles), down, 0.0)
    order[...] = jnp.sum(here, axis=0, keepdims=True).astype(jnp.int32)


def advect_kernel(fields, sizes, density, warm, leading, trailing, diffusion, band, pair, scaler, energy, produced,
                  weight, counts, out, rates, table, offsets, order,
                  lines, spread, start, one, two, east, north, pieces, across, packed, landed, flows, send, recv):
    n_grp, n_gx = sizes
    g, x = lax.axis_index("grp"), lax.axis_index("gx")
    rows, cols = warm.shape
    parts = cols // LANES
    tiles = start.shape[0] // parts
    species = fields - 1
    last = fields // 8
    up, down = (g, lax.rem(x + n_gx - 1, n_gx)), (g, lax.rem(x + 1, n_gx))
    left, right = (lax.rem(g + n_grp - 1, n_grp), x), (lax.rem(g + 1, n_grp), x)
    barrier = pltpu.get_barrier_semaphore()
    for place in (up, down, left, right):
        pl.semaphore_signal(barrier, inc=1, device_id=place, device_id_type=pl.DeviceIdType.MESH)

    lane = lax.broadcasted_iota(jnp.int32, (8, LANES), 1)
    slot = lane % SLOT
    home = LANES - SLOT * rows

    def at(row):
        return pl.ds(row * 8 if isinstance(row, int) else pl.multiple_of(row * 8, 8), 8)

    def spread_out(read, t, sub):
        for q in range(rows // 8):
            for h in range(parts):
                start[t * parts + h, pl.ds((REACH + q * 8) * 8 + sub, 8, stride=8), :] = read(q, h)

    def of_density(f):
        return lambda q, h: density[pl.ds(pl.multiple_of(f * rows + q * 8, 8), 8), h * LANES:(h + 1) * LANES]

    def of_plane(ref):
        return lambda q, h: ref[q * 8:(q + 1) * 8, h * LANES:(h + 1) * LANES]

    def copies(s, t):
        held = (start, one, two)[s]
        both = pl.ds(t * parts, parts)
        plan = [
            (held.at[both, pl.ds(REACH * 8, REACH * 8)], held.at[both, pl.ds((REACH + rows) * 8, REACH * 8)], up),
            (held.at[both, pl.ds(rows * 8, REACH * 8)], held.at[both, pl.ds(0, REACH * 8)], down),
            (packed.at[s, t, 0], landed.at[s, t, 1], left),
            (packed.at[s, t, 1], landed.at[s, t, 0], right),
        ]
        return [pltpu.make_async_remote_copy(
            src_ref=src, dst_ref=dst, send_sem=send.at[s, t, n], recv_sem=recv.at[s, t, n],
            device_id=place, device_id_type=pl.DeviceIdType.MESH) for n, (src, dst, place) in enumerate(plan)]

    def pack(s, t):
        held = (start, one, two)[s]
        def merge(low, count, part, join):
            if count == 1:
                return held[t * parts + part, at(REACH + low), :]
            here = count // 2
            return join(merge(low, here, part, join), here, merge(low + here, count - here, part, join), count - here)

        def from_left(a, n, b, m):
            return jnp.where(lane < SLOT * n, a, pltpu.roll(b, SLOT * n, 1))

        def from_right(a, n, b, m):
            return jnp.where(lane >= LANES - SLOT * m, b, pltpu.roll(a, LANES - SLOT * m, 1))

        first = merge(0, rows, 0, from_left)
        final = merge(0, rows, parts - 1, from_right)
        packed[s, t, 0] = first
        packed[s, t, 1] = final
        for copy in copies(s, t):
            copy.start()

    for f in range(tiles * 8):
        spread[f:f + 1, :] = jnp.full((1, LANES), diffusion[f] if f < fields else 0.0)
    for f in range(last * 8, species):
        spread_out(of_density(f), last, f % 8)
    for n, ref in enumerate((warm, leading, trailing)):
        spread_out(of_plane(ref), last, (species + n) % 8)
    pl.semaphore_wait(barrier, 4)
    pack(0, last)

    def prepare(t, c):
        for sub in range(8):
            spread_out(of_density(t * 8 + sub), t, sub)
        pack(0, t)
        return c

    lax.fori_loop(0, last, prepare, 0)

    pull, push = transport_step * sixth_first[0], -transport_step / FIRST_SCALE
    for i in range(rows):
        for h in range(parts):
            lanes = slice(h * LANES, (h + 1) * LANES)
            east[h, at(REACH + i), :] = jnp.broadcast_to(pull * leading[i:i + 1, lanes], (8, LANES))
            north[h, at(i), :] = jnp.broadcast_to(push * trailing[i:i + 1, lanes], (8, LANES))

    def arrive(s, t):
        for copy in copies(s, t):
            copy.wait_recv()

    prepare_tables(pair, scaler, energy, produced, weight, counts, rates, table, offsets, order, lines)
    arrive(0, last)
    u_sub, v_sub = fields % 8, (fields + 1) % 8
    for r in (*range(REACH), *range(REACH + rows, 2 * REACH + rows)):
        for h in range(parts):
            east[h, at(r), :] = jnp.broadcast_to(
                pull * start[last * parts + h, pl.ds(r * 8 + u_sub, 1), :], (8, LANES))
    for side in range(2):
        flow = jnp.broadcast_to(landed[0, last, side, pl.ds(v_sub, 1), :], (8, LANES))
        for k in range(1, REACH + 1):
            inside = slot >= SLOT - k if side == 0 else slot < k
            weight = (1.0 if side == 0 else -1.0) * transport_step * sixth_first[k - 1]
            flows[side * REACH + k - 1] = jnp.where(inside, weight * flow, 0.0)

    def split(held, t):
        scale = spread[at(t), :] * (transport_step / SECOND_SCALE)
        for i in range(rows):
            fs = [held[t * parts + h, at(REACH + i), :] for h in range(parts)]
            f_high, f_low = halves(jnp.concatenate([scale * f for f in fs], 1))
            g_high, g_low = halves(jnp.concatenate([north[h, at(i), :] * f for h, f in enumerate(fs)], 1))
            for m, piece in enumerate((f_high, f_low, g_high, g_low)):
                pieces[at(i), m * cols:(m + 1) * cols] = piece

    def stage(s):
        held, fresh = (start, one, two)[s], (one, two, None)[s]

        def tile(n, c):
            t = lax.rem(n + last, tiles)

            @pl.when(n > 0 if s == 0 else n >= 0)
            def _():
                arrive(s, t)

            d = spread[at(t), :] * transport_step
            across[...] = jnp.dot(pieces[...], band[...], preferred_element_type=jnp.float32)
            split(held, lax.rem(t + 1, tiles))

            borders = []
            for side in range(2):
                halo = landed[s, t, side]
                total = None
                for k in range(1, REACH + 1):
                    inside = slot >= SLOT - k if side == 0 else slot < k
                    part = (jnp.where(inside, sixth_second[k - 1] * d, 0.0) + flows[side * REACH + k - 1]) * halo
                    if k < REACH:
                        part = pltpu.roll(part, (k - REACH) % LANES if side == 0 else REACH - k, 1)
                    total = part if total is None else total + part
                borders.append(total)
            ids = t * 8 + lax.broadcasted_iota(jnp.int32, (8, LANES), 0)
            reach = sixth_second[0] * d

            for b in range(rows // 8):
                for h in range(parts):
                    lanes = slice(h * LANES, (h + 1) * LANES)
                    f = [held[t * parts + h, at(b * 8 + m), :] for m in range(8 + 2 * REACH)]
                    gs = [east[h, at(b * 8 + m), :] * f[m] for m in range(8 + 2 * REACH)]
                    for r in range(8):
                        i = b * 8 + r
                        m = r + REACH
                        lap = (sixth_center / sixth_second[0]) * f[m] + (f[m + 1] + f[m - 1])
                        grad = gs[m + 1] - gs[m - 1]
                        for k in range(2, REACH + 1):
                            lap = lap + (sixth_second[k - 1] / sixth_second[0]) * (f[m + k] + f[m - k])
                            grad = grad + (sixth_first[k - 1] / sixth_first[0]) * (gs[m + k] - gs[m - k])
                        change = across[at(i), lanes] + (reach * lap - grad)
                        if h == 0:
                            change = change + jnp.where(
                                lane < REACH, pltpu.roll(borders[0], (LANES - home - SLOT * i - 1) % LANES, 1), 0.0)
                        if h == parts - 1:
                            change = change + jnp.where(
                                lane >= LANES - REACH,
                                pltpu.roll(borders[1], (2 * LANES - REACH - SLOT * i) % LANES, 1), 0.0)
                        if s == 0:
                            fresh[t * parts + h, at(REACH + i), :] = f[m] + change
                        elif s == 1:
                            fresh[t * parts + h, at(REACH + i), :] = (
                                0.75 * start[t * parts + h, at(REACH + i), :] + 0.25 * (f[m] + change))
                        else:
                            value = start[t * parts + h, at(REACH + i), :] * (1.0 / 3.0) + (2.0 / 3.0) * (f[m] + change)
                            out[t * parts + h, at(i), :] = jnp.where(ids < species, jnp.maximum(value, 0.0), value)
            if s < 2:
                pack(s + 1, t)
            return c

        split(held, last)
        lax.fori_loop(0, tiles, tile, 0)

    for s in range(3):
        stage(s)

    def finish(t, c):
        for s in range(3):
            for copy in copies(s, t):
                copy.wait_send()
        return c

    lax.fori_loop(0, tiles, finish, 0)


def band_matrix(width):
    here = np.arange(width)
    lag = here[:, None] - here[None, :]
    second = np.where(lag == 0, round(sixth_center * SECOND_SCALE), 0)
    first = np.zeros((width, width))
    for k in range(1, REACH + 1):
        ahead, behind = lag == k, lag == -k
        second = np.where(ahead | behind, round(sixth_second[k - 1] * SECOND_SCALE), second)
        weight = round(sixth_first[k - 1] * FIRST_SCALE)
        first = np.where(ahead, weight, np.where(behind, -weight, first))
    return jnp.asarray(np.concatenate([second, second, first, first], 0), jnp.bfloat16)


def advect(density, warm, leading, trailing, diffusion, pair, scaler, energy, produced, counts):
    species, rows, cols = density.shape
    fields = species + 1
    tiles = (fields + 2) // 8
    if (fields + 2) % 8 or rows * SLOT > LANES or cols % LANES or rows % 8:
        raise ValueError("unsupported sizes")
    parts = cols // LANES
    sizes = (lax.axis_size("grp"), lax.axis_size("gx"))
    vmem = pl.BlockSpec(memory_space=pltpu.VMEM)
    wide = pltpu.VMEM((tiles * parts, (rows + 2 * REACH) * 8, LANES), jnp.float32)
    band = band_matrix(cols)
    reactions = pair.shape[1]
    if counts.shape[1] > LANES or species > 64:
        raise ValueError("unsupported sizes")
    length = up(up(reactions, TRIPS), 8)
    weight = spread_weights(reactions)[None]
    smem = pl.BlockSpec(memory_space=pltpu.SMEM)
    return pl.pallas_call(
        functools.partial(advect_kernel, fields, sizes),
        in_specs=[vmem] * 4 + [smem] + [vmem] * 7,
        out_specs=[vmem] * 5,
        out_shape=[jax.ShapeDtypeStruct((tiles * parts, rows * 8, LANES), jnp.float32),
                   jax.ShapeDtypeStruct((3 * length, LANES), jnp.float32),
                   jax.ShapeDtypeStruct((2 * up(species, 8), up(length, 16)), jnp.bfloat16),
                   jax.ShapeDtypeStruct((1, 2 * up(length, LANES)), jnp.int32),
                   jax.ShapeDtypeStruct((1, LANES), jnp.int32)],
        scratch_shapes=[pltpu.VMEM((8, up(length, LANES)), jnp.float32),
                        pltpu.VMEM((tiles * 8, LANES), jnp.float32), wide, wide, wide,
                        pltpu.VMEM((parts, (rows + 2 * REACH) * 8, LANES), jnp.float32),
                        pltpu.VMEM((parts, rows * 8, LANES), jnp.float32),
                        pltpu.VMEM((rows * 8, 4 * cols), jnp.bfloat16),
                        pltpu.VMEM((rows * 8, cols), jnp.float32),
                        pltpu.VMEM((3, tiles, 2, 8, LANES), jnp.float32),
                        pltpu.VMEM((3, tiles, 2, 8, LANES), jnp.float32),
                        pltpu.VMEM((2 * REACH, 8, LANES), jnp.float32),
                        pltpu.SemaphoreType.DMA((3, tiles, 4)),
                        pltpu.SemaphoreType.DMA((3, tiles, 4))],
        compiler_params=pltpu.CompilerParams(collective_id=0, has_side_effects=True, vmem_limit_bytes=ROOM),
        name="advect",
    )(density.reshape(species * rows, cols), warm, leading, trailing, diffusion, band, pair, scaler, energy, produced,
      weight, counts)


GROUP = 16
PITCH = GROUP + 1
SPAN = 9


def chemistry_kernel(species, chunk, order, counts, pair, warming, rates, table, state, out, warm_out,
                     held, low_gained, high_gained, progress, steps, staged, sems, *losses):
    rows, cols = warm_out.shape
    layers = state.shape[0] * LANES // cols * 8
    per_row = cols // TILE
    tiles = rows * per_row
    warm_row = species
    length = rates.shape[0] // 3
    reactions = length // chunk * chunk
    span = progress.shape[0] // GROUP
    depth = table.shape[1]
    half = table.shape[0] // 2
    blocks = layers // 8
    lines = staged.reshape(staged.shape[0] * staged.shape[1], LANES)
    line_span = staged.shape[1]
    gained = (low_gained, high_gained)

    for t in range(GROUP):
        progress[pl.ds(t * span + reactions, depth - reactions)] = jnp.zeros((depth - reactions, LANES), jnp.float32)
    for loss in losses:
        loss[...] = jnp.zeros_like(loss)

    def at(field):
        return pl.ds(field * PITCH, GROUP)

    def handle(g, c):
        ids = [order[0, g * GROUP + t] for t in range(GROUP)]
        numbers = [counts[t] for t in ids]
        places = [(t % per_row, pl.ds(pl.multiple_of(t // per_row * 8, 8), 8)) for t in ids]
        turn_count = functools.reduce(jnp.maximum, numbers)
        for t in range(GROUP):
            part, at_row = places[t]
            steps[t:t + 1, :] = jnp.full((1, LANES), numbers[t].astype(jnp.float32))
            for f in range(blocks):
                held[pl.ds(f * 8 * PITCH + t, 8, stride=PITCH)] = state[f * per_row + part, at_row, :]

        def advance(s, c):
            heat = jnp.tanh(held[at(warm_row)])

            def react(k, c):
                for j in range(chunk):
                    r = k * chunk + j
                    first = pl.ds(pair[0, r], GROUP)
                    second = pl.ds(pair[0, pair.shape[1] // 2 + r], GROUP)
                    a, e, weight = [jnp.broadcast_to(rates[pl.ds(n * length + r, 1), :], (GROUP, LANES)) for n in range(3)]
                    rate = jnp.exp2(a + e * heat)
                    ca, cb = held[first], held[second]
                    qa, qb = rate * ca, rate * cb
                    progress[pl.ds(r, GROUP, stride=span)] = qa * (weight * cb)
                    n = 2 * (j % (len(losses) // 2))
                    losses[n][first] += qb
                    losses[n + 1][second] += qa
                return c

            lax.fori_loop(0, reactions // chunk, react, 0)
            for n, fill in enumerate(gained):
                for q in range(4 * n, 4 * n + 4):
                    p = jnp.concatenate([progress[pl.ds((2 * q + t) * span, depth)] for t in range(2)], 1)
                    both = jnp.dot(table[...], p.astype(jnp.bfloat16), preferred_element_type=jnp.float32)
                    total = both[:half] + both[half:]
                    for t in range(2):
                        for f in range(half // 8):
                            fill[pl.ds(f * 8 * SPAN + 2 * (q - 4 * n) + t, 8, stride=SPAN)] = (
                                total[f * 8:(f + 1) * 8, t * TILE:(t + 1) * TILE])
                number = steps[8 * n:8 * n + 8, :]
                pace = number * (1.0 / chemistry_span)
                active = s.astype(jnp.float32) < number
                change = jnp.zeros((8, LANES), jnp.float32)
                for j in range(species):
                    place = pl.ds(j * PITCH + 8 * n, 8)
                    x = held[place]
                    destroyed = functools.reduce(jnp.add, [loss[place] for loss in losses])
                    for loss in losses:
                        loss[place] = jnp.zeros((8, LANES), jnp.float32)
                    updated = (pace * x + fill[pl.ds(j * SPAN, 8)]) / (pace + destroyed)
                    change = change + warming[j] * (updated - x)
                    held[place] = jnp.where(active, updated, x)
                place = pl.ds(warm_row * PITCH + 8 * n, 8)
                w = held[place]
                held[place] = jnp.where(active, w + change, w)
            return c

        lax.fori_loop(0, turn_count, advance, 0)
        for t in range(GROUP):
            line = (ids[t] % per_row) * ((warm_row + 1) * line_span) + ids[t] // per_row
            for f in range(0, warm_row + 1, 8):
                n = min(8, warm_row + 1 - f)
                lines[pl.ds(line + f * line_span, n, stride=line_span)] = held[pl.ds(f * PITCH + t, n, stride=PITCH)]
        return c

    lax.fori_loop(0, tiles // GROUP, handle, 0)
    wide = out.reshape(species, rows, cols)
    copies = []
    for n in range(per_row):
        lanes = pl.ds(n * TILE, TILE)
        first = n * (warm_row + 1)
        copies.append(pltpu.make_async_copy(
            staged.at[pl.ds(first, species), pl.ds(0, rows)], wide.at[:, :, lanes], sems.at[0, n]))
        copies.append(pltpu.make_async_copy(
            staged.at[first + species, pl.ds(0, rows)], warm_out.at[:, lanes], sems.at[1, n]))
    for copy in copies:
        copy.start()
    for copy in copies:
        copy.wait()


LOSSES = 4


def chemistry(state, order, counts, pair, warming, rates, table, species, rows, cols):
    layers = state.shape[0] * LANES // cols * 8
    smem = pl.BlockSpec(memory_space=pltpu.SMEM)
    vmem = pl.BlockSpec(memory_space=pltpu.VMEM)
    block = pltpu.VMEM((layers * PITCH, LANES), jnp.float32)
    part = pltpu.VMEM((layers * SPAN, LANES), jnp.float32)
    return pl.pallas_call(
        functools.partial(chemistry_kernel, species, rates.shape[0] // 3 // TRIPS),
        in_specs=[smem, smem, smem, smem, vmem, vmem, vmem],
        out_specs=[pl.BlockSpec(memory_space=pl.ANY)] * 2,
        out_shape=[jax.ShapeDtypeStruct((species * rows, cols), jnp.float32),
                   jax.ShapeDtypeStruct((rows, cols), jnp.float32)],
        scratch_shapes=[block, part, part,
                        pltpu.VMEM((GROUP * (table.shape[1] + 1), LANES), jnp.float32),
                        pltpu.VMEM((GROUP, LANES), jnp.float32),
                        pltpu.VMEM((cols // TILE * (species + 1), rows + 8, TILE), jnp.float32),
                        pltpu.SemaphoreType.DMA((2, cols // TILE))]
        + [block] * LOSSES,
        compiler_params=pltpu.CompilerParams(vmem_limit_bytes=ROOM),
        name="chemistry",
    )(order, counts, pair, warming, rates, table, state)


def body(component_density, scaled_thermal_state, leading_direction_flow, trailing_direction_flow,
         spreading_coefficient, colliding_pair, natural_exponent_scaler, arrhenius_energy,
         stoichiometric_output, formation_warming, explicit_increments):
    species, rows, cols = component_density.shape
    clipped, rates, table, pair, order = advect(
        component_density, scaled_thermal_state, leading_direction_flow, trailing_direction_flow, spreading_coefficient,
        colliding_pair.T, natural_exponent_scaler, arrhenius_energy, stoichiometric_output.T,
        explicit_increments[None])
    reacted, warm = chemistry(clipped, order, explicit_increments, pair, formation_warming, rates, table,
                              species, rows, cols)
    return reacted.reshape(species, rows, cols), warm


def solution(mesh):
    return jax.shard_map(
        body,
        mesh=mesh,
        in_specs=(
            P(None, "gx", "grp"),
            P("gx", "grp"),
            P("gx", "grp"),
            P("gx", "grp"),
            P(),
            P(),
            P(),
            P(),
            P(),
            P(),
            P(("grp", "gx")),
        ),
        out_specs=(P(None, "gx", "grp"), P("gx", "grp")),
        check_vma=False,
    )
```

```python
import functools
import math

import jax
import jax.numpy as jnp
import numpy as np
from jax import lax
from jax.experimental import pallas as pl
from jax.experimental.pallas import tpu as pltpu
from jax.sharding import PartitionSpec as P

TILE = 128
FIRST_SCALE = 60.0
SECOND_SCALE = 180.0
transport_step = 0.4
chemistry_span = 0.5
sixth_first = (0.75, -0.15, 1.0 / 60.0)
sixth_second = (1.5, -0.15, 1.0 / 90.0)
sixth_center = -49.0 / 18.0


def up(n, m):
    return -(-n // m) * m


def spread_weights(reactions):
    golden = (math.sqrt(5.0) - 1.0) / 2.0
    return np.exp2((np.arange(reactions) * golden) % 1.0).astype(np.float32)


REACH = 3
SLOT = 4
LANES = 128
NEVER = -16384.0
TRIPS = 3


def halves(value):
    high = value.astype(jnp.bfloat16)
    return high, (value - high.astype(jnp.float32)).astype(jnp.bfloat16)


def prepare_tables(pair, scaler, energy, produced, weight, counts, rates, table, offsets, order, lines):
    reactions = pair.shape[1]
    length = rates.shape[0] // 3
    species = produced.shape[0]
    half = table.shape[0] // 2
    scale = 1.0 / math.log(2.0)
    wide = lines.shape[1]
    lines[...] = jnp.zeros_like(lines)
    lines[0:1, :] = jnp.full((1, wide), NEVER)
    lines[0, 0:reactions] = scaler[...] * scale
    lines[1, 0:reactions] = energy[...] * scale
    lines[2:3, 0:reactions] = weight[...]
    for n in range(3):
        for r in range(0, length, LANES):
            count = min(LANES, length - r)
            row = jnp.broadcast_to(lines[n:n + 1, r:r + LANES], (LANES, LANES))
            rates[n * length + r:n * length + r + count, :] = row.T[:count]
    table[...] = jnp.zeros_like(table)
    high, low = halves(produced[...] / weight[...])
    table[0:species, 0:reactions] = high
    table[half:half + species, 0:reactions] = low
    offsets[...] = jnp.zeros_like(offsets)
    for n in range(2):
        offsets[:, n * wide:n * wide + reactions] = pair[n:n + 1, :] * PITCH
    tiles = counts.shape[1]
    lines[3:4, 0:tiles] = counts[...].astype(jnp.float32) * tiles
    key = lines[3:4, 0:LANES] + lax.broadcasted_iota(jnp.int32, (1, LANES), 1).astype(jnp.float32)
    down = lax.broadcasted_iota(jnp.int32, (LANES, LANES), 0).astype(jnp.float32)
    along = lax.broadcasted_iota(jnp.int32, (LANES, LANES), 1)
    across = jnp.broadcast_to(key, (LANES, LANES))
    before = jnp.where((across < across.T) & (along < tiles), 1.0, 0.0)
    rank = jnp.sum(before, axis=1, keepdims=True)
    here = jnp.where((rank == along.astype(jnp.float32)) & (down < tiles), down, 0.0)
    order[...] = jnp.sum(here, axis=0, keepdims=True).astype(jnp.int32)


def advect_kernel(fields, sizes, sources, targets, scratch):
    (out, rates, table, offsets, order, stored, density, warm, leading, trailing, diffusion, band, pair, scaler, energy, produced, weight, counts, loaded,
     lines, spread, start, one, two, east, north, pieces, across, packed, landed, flows, send, recv) = scratch
    inputs = [pltpu.make_async_copy(src, dst, loaded.at[n]) for n, (src, dst) in enumerate(
        zip(sources, (density, warm, leading, trailing, diffusion, band, pair, scaler, energy, produced, weight, counts)))]
    for copy in inputs:
        copy.start()
    n_grp, n_gx = sizes
    g, x = lax.axis_index("grp"), lax.axis_index("gx")
    rows, cols = warm.shape
    parts = cols // LANES
    tiles = start.shape[0] // parts
    species = fields - 1
    last = fields // 8
    up, down = (g, lax.rem(x + n_gx - 1, n_gx)), (g, lax.rem(x + 1, n_gx))
    left, right = (lax.rem(g + n_grp - 1, n_grp), x), (lax.rem(g + 1, n_grp), x)
    barrier = pltpu.get_barrier_semaphore()
    for place in (up, down, left, right):
        pl.semaphore_signal(barrier, inc=1, device_id=place, device_id_type=pl.DeviceIdType.MESH)

    lane = lax.broadcasted_iota(jnp.int32, (8, LANES), 1)
    slot = lane % SLOT
    home = LANES - SLOT * rows

    def at(row):
        return pl.ds(row * 8 if isinstance(row, int) else pl.multiple_of(row * 8, 8), 8)

    def spread_out(read, t, sub):
        for q in range(rows // 8):
            for h in range(parts):
                start[t * parts + h, pl.ds((REACH + q * 8) * 8 + sub, 8, stride=8), :] = read(q, h)

    def of_density(f):
        return lambda q, h: density[pl.ds(pl.multiple_of(f * rows + q * 8, 8), 8), h * LANES:(h + 1) * LANES]

    def of_plane(ref):
        return lambda q, h: ref[q * 8:(q + 1) * 8, h * LANES:(h + 1) * LANES]

    def result(t):
        both = pl.ds(t * parts, parts)
        return pltpu.make_async_copy(out.at[both], targets[0].at[both], stored.at[t])

    def copies(s, t):
        held = (start, one, two)[s]
        both = pl.ds(t * parts, parts)
        plan = [
            (held.at[both, pl.ds(REACH * 8, REACH * 8)], held.at[both, pl.ds((REACH + rows) * 8, REACH * 8)], up),
            (held.at[both, pl.ds(rows * 8, REACH * 8)], held.at[both, pl.ds(0, REACH * 8)], down),
            (packed.at[s, t, 0], landed.at[s, t, 1], left),
            (packed.at[s, t, 1], landed.at[s, t, 0], right),
        ]
        return [pltpu.make_async_remote_copy(
            src_ref=src, dst_ref=dst, send_sem=send.at[s, t, n], recv_sem=recv.at[s, t, n],
            device_id=place, device_id_type=pl.DeviceIdType.MESH) for n, (src, dst, place) in enumerate(plan)]

    def pack(s, t):
        held = (start, one, two)[s]
        def merge(low, count, part, join):
            if count == 1:
                return held[t * parts + part, at(REACH + low), :]
            here = count // 2
            return join(merge(low, here, part, join), here, merge(low + here, count - here, part, join), count - here)

        def from_left(a, n, b, m):
            return jnp.where(lane < SLOT * n, a, pltpu.roll(b, SLOT * n, 1))

        def from_right(a, n, b, m):
            return jnp.where(lane >= LANES - SLOT * m, b, pltpu.roll(a, LANES - SLOT * m, 1))

        first = merge(0, rows, 0, from_left)
        final = merge(0, rows, parts - 1, from_right)
        packed[s, t, 0] = first
        packed[s, t, 1] = final
        for copy in copies(s, t):
            copy.start()

    for copy in inputs:
        copy.wait()
    for f in range(tiles * 8):
        spread[f:f + 1, :] = jnp.full((1, LANES), diffusion[f] if f < fields else 0.0)
    for f in range(last * 8, species):
        spread_out(of_density(f), last, f % 8)
    for n, ref in enumerate((warm, leading, trailing)):
        spread_out(of_plane(ref), last, (species + n) % 8)
    pl.semaphore_wait(barrier, 4)
    pack(0, last)

    def prepare(t, c):
        for sub in range(8):
            spread_out(of_density(t * 8 + sub), t, sub)
        pack(0, t)
        return c

    lax.fori_loop(0, last, prepare, 0)

    pull, push = transport_step * sixth_first[0], -transport_step / FIRST_SCALE
    for i in range(rows):
        for h in range(parts):
            lanes = slice(h * LANES, (h + 1) * LANES)
            east[h, at(REACH + i), :] = jnp.broadcast_to(pull * leading[i:i + 1, lanes], (8, LANES))
            north[h, at(i), :] = jnp.broadcast_to(push * trailing[i:i + 1, lanes], (8, LANES))

    def arrive(s, t):
        for copy in copies(s, t):
            copy.wait_recv()

    prepare_tables(pair, scaler, energy, produced, weight, counts, rates, table, offsets, order, lines)
    tables = [pltpu.make_async_copy(src, dst, stored.at[tiles + n]) for n, (src, dst) in enumerate(
        zip((rates, table, offsets, order), targets[1:]))]
    for copy in tables:
        copy.start()
    arrive(0, last)
    u_sub, v_sub = fields % 8, (fields + 1) % 8
    for r in (*range(REACH), *range(REACH + rows, 2 * REACH + rows)):
        for h in range(parts):
            east[h, at(r), :] = jnp.broadcast_to(
                pull * start[last * parts + h, pl.ds(r * 8 + u_sub, 1), :], (8, LANES))
    for side in range(2):
        flow = jnp.broadcast_to(landed[0, last, side, pl.ds(v_sub, 1), :], (8, LANES))
        for k in range(1, REACH + 1):
            inside = slot >= SLOT - k if side == 0 else slot < k
            weight = (1.0 if side == 0 else -1.0) * transport_step * sixth_first[k - 1]
            flows[side * REACH + k - 1] = jnp.where(inside, weight * flow, 0.0)

    def split(held, t):
        scale = spread[at(t), :] * (transport_step / SECOND_SCALE)
        for i in range(rows):
            fs = [held[t * parts + h, at(REACH + i), :] for h in range(parts)]
            f_high, f_low = halves(jnp.concatenate([scale * f for f in fs], 1))
            g_high, g_low = halves(jnp.concatenate([north[h, at(i), :] * f for h, f in enumerate(fs)], 1))
            for m, piece in enumerate((f_high, f_low, g_high, g_low)):
                pieces[at(i), m * cols:(m + 1) * cols] = piece

    def stage(s):
        held, fresh = (start, one, two)[s], (one, two, None)[s]

        def tile(n, c):
            t = lax.rem(n + last, tiles)

            @pl.when(n > 0 if s == 0 else n >= 0)
            def _():
                arrive(s, t)

            d = spread[at(t), :] * transport_step
            across[...] = jnp.dot(pieces[...], band[...], preferred_element_type=jnp.float32)
            split(held, lax.rem(t + 1, tiles))

            borders = []
            for side in range(2):
                halo = landed[s, t, side]
                total = None
                for k in range(1, REACH + 1):
                    inside = slot >= SLOT - k if side == 0 else slot < k
                    part = (jnp.where(inside, sixth_second[k - 1] * d, 0.0) + flows[side * REACH + k - 1]) * halo
                    if k < REACH:
                        part = pltpu.roll(part, (k - REACH) % LANES if side == 0 else REACH - k, 1)
                    total = part if total is None else total + part
                borders.append(total)
            ids = t * 8 + lax.broadcasted_iota(jnp.int32, (8, LANES), 0)
            reach = sixth_second[0] * d

            for b in range(rows // 8):
                for h in range(parts):
                    lanes = slice(h * LANES, (h + 1) * LANES)
                    f = [held[t * parts + h, at(b * 8 + m), :] for m in range(8 + 2 * REACH)]
                    gs = [east[h, at(b * 8 + m), :] * f[m] for m in range(8 + 2 * REACH)]
                    for r in range(8):
                        i = b * 8 + r
                        m = r + REACH
                        lap = (sixth_center / sixth_second[0]) * f[m] + (f[m + 1] + f[m - 1])
                        grad = gs[m + 1] - gs[m - 1]
                        for k in range(2, REACH + 1):
                            lap = lap + (sixth_second[k - 1] / sixth_second[0]) * (f[m + k] + f[m - k])
                            grad = grad + (sixth_first[k - 1] / sixth_first[0]) * (gs[m + k] - gs[m - k])
                        change = across[at(i), lanes] + (reach * lap - grad)
                        if h == 0:
                            change = change + jnp.where(
                                lane < REACH, pltpu.roll(borders[0], (LANES - home - SLOT * i - 1) % LANES, 1), 0.0)
                        if h == parts - 1:
                            change = change + jnp.where(
                                lane >= LANES - REACH,
                                pltpu.roll(borders[1], (2 * LANES - REACH - SLOT * i) % LANES, 1), 0.0)
                        if s == 0:
                            fresh[t * parts + h, at(REACH + i), :] = f[m] + change
                        elif s == 1:
                            fresh[t * parts + h, at(REACH + i), :] = (
                                0.75 * start[t * parts + h, at(REACH + i), :] + 0.25 * (f[m] + change))
                        else:
                            value = start[t * parts + h, at(REACH + i), :] * (1.0 / 3.0) + (2.0 / 3.0) * (f[m] + change)
                            out[t * parts + h, at(i), :] = jnp.where(ids < species, jnp.maximum(value, 0.0), value)
            if s < 2:
                pack(s + 1, t)
            else:
                result(t).start()
            return c

        split(held, last)
        lax.fori_loop(0, tiles, tile, 0)

    for s in range(3):
        stage(s)

    for copy in tables:
        copy.wait()

    def finish(t, c):
        result(t).wait()
        for s in range(3):
            for copy in copies(s, t):
                copy.wait_send()
        return c

    lax.fori_loop(0, tiles, finish, 0)


def band_matrix(width):
    here = np.arange(width)
    lag = here[:, None] - here[None, :]
    second = np.where(lag == 0, round(sixth_center * SECOND_SCALE), 0)
    first = np.zeros((width, width))
    for k in range(1, REACH + 1):
        ahead, behind = lag == k, lag == -k
        second = np.where(ahead | behind, round(sixth_second[k - 1] * SECOND_SCALE), second)
        weight = round(sixth_first[k - 1] * FIRST_SCALE)
        first = np.where(ahead, weight, np.where(behind, -weight, first))
    return jnp.asarray(np.concatenate([second, second, first, first], 0), jnp.bfloat16)


def advect(density, warm, leading, trailing, diffusion, pair, scaler, energy, produced, counts):
    species, rows, cols = density.shape
    fields = species + 1
    tiles = (fields + 2) // 8
    if (fields + 2) % 8 or rows * SLOT > LANES or cols % LANES or rows % 8:
        raise ValueError("unsupported sizes")
    parts = cols // LANES
    sizes = (lax.axis_size("grp"), lax.axis_size("gx"))
    wide = pltpu.VMEM((tiles * parts, (rows + 2 * REACH) * 8, LANES), jnp.float32)
    band = band_matrix(cols)
    reactions = pair.shape[1]
    if counts.shape[1] > LANES or species > 64:
        raise ValueError("unsupported sizes")
    length = up(up(reactions, TRIPS), 8)
    weight = spread_weights(reactions)[None]
    args = (density.reshape(species * rows, cols), warm, leading, trailing, diffusion, band, pair, scaler, energy, produced,
            weight, counts)
    count = len(args)
    places = [pltpu.SMEM if n == 4 else pltpu.VMEM for n in range(count)]

    results = [jax.ShapeDtypeStruct((tiles * parts, rows * 8, LANES), jnp.float32),
               jax.ShapeDtypeStruct((3 * length, LANES), jnp.float32),
               jax.ShapeDtypeStruct((2 * up(species, 8), up(length, 16)), jnp.bfloat16),
               jax.ShapeDtypeStruct((1, 2 * up(length, LANES)), jnp.int32),
               jax.ShapeDtypeStruct((1, LANES), jnp.int32)]

    def kernel(*refs):
        advect_kernel(fields, sizes, refs[:count], refs[count:count + len(results)], refs[count + len(results):])

    return pl.pallas_call(
        kernel,
        in_specs=[pl.BlockSpec(memory_space=pltpu.HBM)] * count,
        out_specs=[pl.BlockSpec(memory_space=pltpu.HBM)] * len(results),
        out_shape=results,
        scratch_shapes=[pltpu.VMEM(result.shape, result.dtype) for result in results]
        + [pltpu.SemaphoreType.DMA((tiles + len(results) - 1,))]
        + [place(arg.shape, arg.dtype) for place, arg in zip(places, args)]
        + [pltpu.SemaphoreType.DMA((count,)),
           pltpu.VMEM((8, up(length, LANES)), jnp.float32),
           pltpu.VMEM((tiles * 8, LANES), jnp.float32), wide, wide, wide,
           pltpu.VMEM((parts, (rows + 2 * REACH) * 8, LANES), jnp.float32),
           pltpu.VMEM((parts, rows * 8, LANES), jnp.float32),
           pltpu.VMEM((rows * 8, 4 * cols), jnp.bfloat16),
           pltpu.VMEM((rows * 8, cols), jnp.float32),
           pltpu.VMEM((3, tiles, 2, 8, LANES), jnp.float32),
           pltpu.VMEM((3, tiles, 2, 8, LANES), jnp.float32),
           pltpu.VMEM((2 * REACH, 8, LANES), jnp.float32),
           pltpu.SemaphoreType.DMA((3, tiles, 4)),
           pltpu.SemaphoreType.DMA((3, tiles, 4))],
        compiler_params=pltpu.CompilerParams(collective_id=0, has_side_effects=True),
        name="advect",
    )(*args)


GROUP = 16
PITCH = GROUP + 1
SPAN = 9


def chemistry_kernel(species, chunk, order, counts, pair, warming, rates, table, state, out, warm_out,
                     held, low_gained, high_gained, progress, steps, staged, sems, *losses):
    rows, cols = warm_out.shape
    layers = state.shape[0] * LANES // cols * 8
    per_row = cols // TILE
    tiles = rows * per_row
    warm_row = species
    length = rates.shape[0] // 3
    reactions = length // chunk * chunk
    span = progress.shape[0] // GROUP
    depth = table.shape[1]
    half = table.shape[0] // 2
    blocks = layers // 8
    lines = staged.reshape(staged.shape[0] * staged.shape[1], LANES)
    line_span = staged.shape[1]
    gained = (low_gained, high_gained)

    for t in range(GROUP):
        progress[pl.ds(t * span + reactions, depth - reactions)] = jnp.zeros((depth - reactions, LANES), jnp.float32)
    for loss in losses:
        loss[...] = jnp.zeros_like(loss)

    def at(field):
        return pl.ds(field * PITCH, GROUP)

    def handle(g, c):
        ids = [order[0, g * GROUP + t] for t in range(GROUP)]
        numbers = [counts[t] for t in ids]
        places = [(t % per_row, pl.ds(pl.multiple_of(t // per_row * 8, 8), 8)) for t in ids]
        turn_count = functools.reduce(jnp.maximum, numbers)
        for t in range(GROUP):
            part, at_row = places[t]
            steps[t:t + 1, :] = jnp.full((1, LANES), numbers[t].astype(jnp.float32))
            for f in range(blocks):
                held[pl.ds(f * 8 * PITCH + t, 8, stride=PITCH)] = state[f * per_row + part, at_row, :]

        def advance(s, c):
            heat = jnp.tanh(held[at(warm_row)])

            def react(k, c):
                for j in range(chunk):
                    r = k * chunk + j
                    first = pl.ds(pair[0, r], GROUP)
                    second = pl.ds(pair[0, pair.shape[1] // 2 + r], GROUP)
                    a, e, weight = [jnp.broadcast_to(rates[pl.ds(n * length + r, 1), :], (GROUP, LANES)) for n in range(3)]
                    rate = jnp.exp2(a + e * heat)
                    ca, cb = held[first], held[second]
                    qa, qb = rate * ca, rate * cb
                    progress[pl.ds(r, GROUP, stride=span)] = qa * (weight * cb)
                    n = 2 * (j % (len(losses) // 2))
                    losses[n][first] += qb
                    losses[n + 1][second] += qa
                return c

            lax.fori_loop(0, reactions // chunk, react, 0)
            for n, fill in enumerate(gained):
                for q in range(4 * n, 4 * n + 4):
                    p = jnp.concatenate([progress[pl.ds((2 * q + t) * span, depth)] for t in range(2)], 1)
                    both = jnp.dot(table[...], p.astype(jnp.bfloat16), preferred_element_type=jnp.float32)
                    total = both[:half] + both[half:]
                    for t in range(2):
                        for f in range(half // 8):
                            fill[pl.ds(f * 8 * SPAN + 2 * (q - 4 * n) + t, 8, stride=SPAN)] = (
                                total[f * 8:(f + 1) * 8, t * TILE:(t + 1) * TILE])
                number = steps[8 * n:8 * n + 8, :]
                pace = number * (1.0 / chemistry_span)
                active = s.astype(jnp.float32) < number
                change = jnp.zeros((8, LANES), jnp.float32)
                for j in range(species):
                    place = pl.ds(j * PITCH + 8 * n, 8)
                    x = held[place]
                    destroyed = functools.reduce(jnp.add, [loss[place] for loss in losses])
                    for loss in losses:
                        loss[place] = jnp.zeros((8, LANES), jnp.float32)
                    updated = (pace * x + fill[pl.ds(j * SPAN, 8)]) / (pace + destroyed)
                    change = change + warming[j] * (updated - x)
                    held[place] = jnp.where(active, updated, x)
                place = pl.ds(warm_row * PITCH + 8 * n, 8)
                w = held[place]
                held[place] = jnp.where(active, w + change, w)
            return c

        lax.fori_loop(0, turn_count, advance, 0)
        for t in range(GROUP):
            line = (ids[t] % per_row) * ((warm_row + 1) * line_span) + ids[t] // per_row
            for f in range(0, warm_row + 1, 8):
                n = min(8, warm_row + 1 - f)
                lines[pl.ds(line + f * line_span, n, stride=line_span)] = held[pl.ds(f * PITCH + t, n, stride=PITCH)]
        return c

    lax.fori_loop(0, tiles // GROUP, handle, 0)
    wide = out.reshape(species, rows, cols)
    copies = []
    for n in range(per_row):
        lanes = pl.ds(n * TILE, TILE)
        first = n * (warm_row + 1)
        copies.append(pltpu.make_async_copy(
            staged.at[pl.ds(first, species), pl.ds(0, rows)], wide.at[:, :, lanes], sems.at[0, n]))
        copies.append(pltpu.make_async_copy(
            staged.at[first + species, pl.ds(0, rows)], warm_out.at[:, lanes], sems.at[1, n]))
    for copy in copies:
        copy.start()
    for copy in copies:
        copy.wait()


LOSSES = 4


def chemistry(state, order, counts, pair, warming, rates, table, species, rows, cols):
    layers = state.shape[0] * LANES // cols * 8
    smem = pl.BlockSpec(memory_space=pltpu.SMEM)
    vmem = pl.BlockSpec(memory_space=pltpu.VMEM)
    block = pltpu.VMEM((layers * PITCH, LANES), jnp.float32)
    part = pltpu.VMEM((layers * SPAN, LANES), jnp.float32)
    return pl.pallas_call(
        functools.partial(chemistry_kernel, species, rates.shape[0] // 3 // TRIPS),
        in_specs=[smem, smem, smem, smem, vmem, vmem, vmem],
        out_specs=[pl.BlockSpec(memory_space=pl.ANY)] * 2,
        out_shape=[jax.ShapeDtypeStruct((species * rows, cols), jnp.float32),
                   jax.ShapeDtypeStruct((rows, cols), jnp.float32)],
        scratch_shapes=[block, part, part,
                        pltpu.VMEM((GROUP * (table.shape[1] + 1), LANES), jnp.float32),
                        pltpu.VMEM((GROUP, LANES), jnp.float32),
                        pltpu.VMEM((cols // TILE * (species + 1), rows + 8, TILE), jnp.float32),
                        pltpu.SemaphoreType.DMA((2, cols // TILE))]
        + [block] * LOSSES,
        name="chemistry",
    )(order, counts, pair, warming, rates, table, state)


def body(component_density, scaled_thermal_state, leading_direction_flow, trailing_direction_flow,
         spreading_coefficient, colliding_pair, natural_exponent_scaler, arrhenius_energy,
         stoichiometric_output, formation_warming, explicit_increments):
    species, rows, cols = component_density.shape
    clipped, rates, table, pair, order = advect(
        component_density, scaled_thermal_state, leading_direction_flow, trailing_direction_flow, spreading_coefficient,
        colliding_pair.T, natural_exponent_scaler, arrhenius_energy, stoichiometric_output.T,
        explicit_increments[None])
    reacted, warm = chemistry(clipped, order, explicit_increments, pair, formation_warming, rates, table,
                              species, rows, cols)
    return reacted.reshape(species, rows, cols), warm


def solution(mesh):
    return jax.shard_map(
        body,
        mesh=mesh,
        in_specs=(
            P(None, "gx", "grp"),
            P("gx", "grp"),
            P("gx", "grp"),
            P("gx", "grp"),
            P(),
            P(),
            P(),
            P(),
            P(),
            P(),
            P(("grp", "gx")),
        ),
        out_specs=(P(None, "gx", "grp"), P("gx", "grp")),
        check_vma=False,
    )
```

```python
import functools
import math

import jax
import jax.numpy as jnp
import numpy as np
from jax import lax
from jax.experimental import pallas as pl
from jax.experimental.pallas import tpu as pltpu
from jax.sharding import PartitionSpec as P

TILE = 128
FIRST_SCALE = 60.0
SECOND_SCALE = 180.0
transport_step = 0.4
chemistry_span = 0.5
sixth_first = (0.75, -0.15, 1.0 / 60.0)
sixth_second = (1.5, -0.15, 1.0 / 90.0)
sixth_center = -49.0 / 18.0


def up(n, m):
    return -(-n // m) * m


def spread_weights(reactions):
    golden = (math.sqrt(5.0) - 1.0) / 2.0
    return np.exp2((np.arange(reactions) * golden) % 1.0).astype(np.float32)


REACH = 3
SLOT = 4
LANES = 128
NEVER = -16384.0
TRIPS = 3
BAND = 4


def halves(value):
    high = value.astype(jnp.bfloat16)
    return high, (value - high.astype(jnp.float32)).astype(jnp.bfloat16)


def prepare_tables(pair, scaler, energy, produced, weight, counts, rates, table, offsets, order, lines):
    reactions = pair.shape[1]
    length = rates.shape[0] // 3
    species = produced.shape[0]
    half = table.shape[0] // 2
    scale = 1.0 / math.log(2.0)
    wide = lines.shape[1]
    lines[...] = jnp.zeros_like(lines)
    lines[0:1, :] = jnp.full((1, wide), NEVER)
    lines[0, 0:reactions] = scaler[...] * scale
    lines[1, 0:reactions] = energy[...] * scale
    lines[2:3, 0:reactions] = weight[...]
    for n in range(3):
        for r in range(0, length, LANES):
            count = min(LANES, length - r)
            row = jnp.broadcast_to(lines[n:n + 1, r:r + LANES], (LANES, LANES))
            rates[n * length + r:n * length + r + count, :] = row.T[:count]
    table[...] = jnp.zeros_like(table)
    high, low = halves(produced[...] / weight[...])
    table[0:species, 0:reactions] = high
    table[half:half + species, 0:reactions] = low
    offsets[...] = jnp.zeros_like(offsets)
    for n in range(2):
        offsets[:, n * wide:n * wide + reactions] = pair[n:n + 1, :] * PITCH
    tiles = counts.shape[1]
    lines[3:4, 0:tiles] = counts[...].astype(jnp.float32) * tiles
    key = lines[3:4, 0:LANES] + lax.broadcasted_iota(jnp.int32, (1, LANES), 1).astype(jnp.float32)
    down = lax.broadcasted_iota(jnp.int32, (LANES, LANES), 0).astype(jnp.float32)
    along = lax.broadcasted_iota(jnp.int32, (LANES, LANES), 1)
    across = jnp.broadcast_to(key, (LANES, LANES))
    before = jnp.where((across < across.T) & (along < tiles), 1.0, 0.0)
    rank = jnp.sum(before, axis=1, keepdims=True)
    here = jnp.where((rank == along.astype(jnp.float32)) & (down < tiles), down, 0.0)
    order[...] = jnp.sum(here, axis=0, keepdims=True).astype(jnp.int32)


def advect_kernel(fields, sizes, sources, targets, scratch):
    (out, rates, table, offsets, order, stored, density, warm, leading, trailing, diffusion, band, pair, scaler, energy, produced, weight, counts, loaded,
     lines, spread, start, one, two, east, north, pieces, across, coming, packed, landed, flows, send, recv) = scratch
    n_grp, n_gx = sizes
    g, x = lax.axis_index("grp"), lax.axis_index("gx")
    rows, cols = warm.shape
    parts = cols // LANES
    tiles = start.shape[0] // parts
    species = fields - 1
    last = fields // 8
    up, down = (g, lax.rem(x + n_gx - 1, n_gx)), (g, lax.rem(x + 1, n_gx))
    left, right = (lax.rem(g + n_grp - 1, n_grp), x), (lax.rem(g + 1, n_grp), x)
    places = (warm, leading, trailing, diffusion, band, pair, scaler, energy, produced, weight, counts)
    inputs = [pltpu.make_async_copy(src, dst, loaded.at[n]) for n, (src, dst) in enumerate(zip(sources[1:], places))]

    def layers_in(t, count):
        span = pl.ds(t * 8 * rows if isinstance(t, int) else pl.multiple_of(t * 8 * rows, 8), count * rows)
        return pltpu.make_async_copy(sources[0].at[span], density.at[span], loaded.at[len(places) + t])

    early, late = inputs[:BAND] + inputs[BAND + 1:], inputs[BAND]
    for copy in early:
        copy.start()
    layers_in(last, species - last * 8).start()

    def begin(t, c):
        layers_in(t, 8).start()
        return c

    lax.fori_loop(0, last, begin, 0)
    late.start()
    barrier = pltpu.get_barrier_semaphore()
    for place in (up, down, left, right):
        pl.semaphore_signal(barrier, inc=1, device_id=place, device_id_type=pl.DeviceIdType.MESH)

    lane = lax.broadcasted_iota(jnp.int32, (8, LANES), 1)
    slot = lane % SLOT
    home = LANES - SLOT * rows

    def at(row):
        return pl.ds(row * 8 if isinstance(row, int) else pl.multiple_of(row * 8, 8), 8)

    def spread_out(read, t, sub):
        for q in range(rows // 8):
            for h in range(parts):
                start[t * parts + h, pl.ds((REACH + q * 8) * 8 + sub, 8, stride=8), :] = read(q, h)

    def of_density(f):
        return lambda q, h: density[pl.ds(pl.multiple_of(f * rows + q * 8, 8), 8), h * LANES:(h + 1) * LANES]

    def of_plane(ref):
        return lambda q, h: ref[q * 8:(q + 1) * 8, h * LANES:(h + 1) * LANES]

    def result(t):
        both = pl.ds(t * parts, parts)
        return pltpu.make_async_copy(out.at[both], targets[0].at[both], stored.at[t])

    def copies(s, t):
        held = (start, one, two)[s]
        both = pl.ds(t * parts, parts)
        plan = [
            (held.at[both, pl.ds(REACH * 8, REACH * 8)], held.at[both, pl.ds((REACH + rows) * 8, REACH * 8)], up),
            (held.at[both, pl.ds(rows * 8, REACH * 8)], held.at[both, pl.ds(0, REACH * 8)], down),
            (packed.at[s, t, 0], landed.at[s, t, 1], left),
            (packed.at[s, t, 1], landed.at[s, t, 0], right),
        ]
        return [pltpu.make_async_remote_copy(
            src_ref=src, dst_ref=dst, send_sem=send.at[s, t, n], recv_sem=recv.at[s, t, n],
            device_id=place, device_id_type=pl.DeviceIdType.MESH) for n, (src, dst, place) in enumerate(plan)]

    def join_left(a, n, b, m):
        return jnp.where(lane < SLOT * n, a, pltpu.roll(b, SLOT * n, 1))

    def join_right(a, n, b, m):
        return jnp.where(lane >= LANES - SLOT * m, b, pltpu.roll(a, LANES - SLOT * m, 1))

    def gather(stack, value, join):
        stack.append((1, value))
        while len(stack) > 1 and stack[-1][0] == stack[-2][0]:
            m, b = stack.pop()
            n, a = stack.pop()
            stack.append((n + m, join(a, n, b, m)))

    def gathered(stack, join):
        while len(stack) > 1:
            m, b = stack.pop()
            n, a = stack.pop()
            stack.append((n + m, join(a, n, b, m)))
        return stack[0][1]

    def depart(s, t, firsts, finals):
        packed[s, t, 0] = gathered(firsts, join_left)
        packed[s, t, 1] = gathered(finals, join_right)
        for copy in copies(s, t):
            copy.start()

    def pack(t):
        firsts, finals = [], []
        for i in range(rows):
            gather(firsts, start[t * parts, at(REACH + i), :], join_left)
            gather(finals, start[t * parts + parts - 1, at(REACH + i), :], join_right)
        depart(0, t, firsts, finals)

    for copy in early:
        copy.wait()
    for f in range(tiles * 8):
        spread[f:f + 1, :] = jnp.full((1, LANES), diffusion[f] if f < fields else 0.0)
    prepare_tables(pair, scaler, energy, produced, weight, counts, rates, table, offsets, order, lines)
    tables = [pltpu.make_async_copy(src, dst, stored.at[tiles + n]) for n, (src, dst) in enumerate(
        zip((rates, table, offsets, order), targets[1:]))]
    for copy in tables:
        copy.start()
    pull, push = transport_step * sixth_first[0], -transport_step / FIRST_SCALE
    for i in range(rows):
        for h in range(parts):
            lanes = slice(h * LANES, (h + 1) * LANES)
            east[h, at(REACH + i), :] = jnp.broadcast_to(pull * leading[i:i + 1, lanes], (8, LANES))
            north[h, at(i), :] = jnp.broadcast_to(push * trailing[i:i + 1, lanes], (8, LANES))

    layers_in(last, species - last * 8).wait()
    for f in range(last * 8, species):
        spread_out(of_density(f), last, f % 8)
    for n, ref in enumerate((warm, leading, trailing)):
        spread_out(of_plane(ref), last, (species + n) % 8)
    pl.semaphore_wait(barrier, 4)

    def prepare(t, c):
        pack(lax.rem(t + last, tiles))
        layers_in(t, 8).wait()
        for sub in range(8):
            spread_out(of_density(t * 8 + sub), t, sub)
        return c

    lax.fori_loop(0, last, prepare, 0)
    pack(last - 1)
    def arrive(s, t):
        for copy in copies(s, t):
            copy.wait_recv()

    late.wait()
    arrive(0, last)
    u_sub, v_sub = fields % 8, (fields + 1) % 8
    for r in (*range(REACH), *range(REACH + rows, 2 * REACH + rows)):
        for h in range(parts):
            east[h, at(r), :] = jnp.broadcast_to(
                pull * start[last * parts + h, pl.ds(r * 8 + u_sub, 1), :], (8, LANES))
    for side in range(2):
        flow = jnp.broadcast_to(landed[0, last, side, pl.ds(v_sub, 1), :], (8, LANES))
        for k in range(1, REACH + 1):
            inside = slot >= SLOT - k if side == 0 else slot < k
            weight = (1.0 if side == 0 else -1.0) * transport_step * sixth_first[k - 1]
            flows[side * REACH + k - 1] = jnp.where(inside, weight * flow, 0.0)

    def split(held, t):
        scale = spread[at(t), :] * (transport_step / SECOND_SCALE)
        for i in range(rows):
            fs = [held[t * parts + h, at(REACH + i), :] for h in range(parts)]
            f_high, f_low = halves(jnp.concatenate([scale * f for f in fs], 1))
            g_high, g_low = halves(jnp.concatenate([north[h, at(i), :] * f for h, f in enumerate(fs)], 1))
            for m, piece in enumerate((f_high, f_low, g_high, g_low)):
                pieces[at(i), m * cols:(m + 1) * cols] = piece

    def stage(s):
        held, fresh = (start, one, two)[s], (one, two, None)[s]

        def tile(n, c):
            t = lax.rem(n + last, tiles)

            @pl.when(n > 0 if s == 0 else n >= 0)
            def _():
                arrive(s, t)

            d = spread[at(t), :] * transport_step
            coming[...] = jnp.dot(pieces[...], band[...], preferred_element_type=jnp.float32)
            split(held, lax.rem(t + 2, tiles))
            firsts, finals = [], []

            borders = []
            for side in range(2):
                halo = landed[s, t, side]
                total = None
                for k in range(1, REACH + 1):
                    inside = slot >= SLOT - k if side == 0 else slot < k
                    part = (jnp.where(inside, sixth_second[k - 1] * d, 0.0) + flows[side * REACH + k - 1]) * halo
                    if k < REACH:
                        part = pltpu.roll(part, (k - REACH) % LANES if side == 0 else REACH - k, 1)
                    total = part if total is None else total + part
                borders.append(total)
            ids = t * 8 + lax.broadcasted_iota(jnp.int32, (8, LANES), 0)
            reach = sixth_second[0] * d

            for b in range(rows // 8):
                for h in range(parts):
                    lanes = slice(h * LANES, (h + 1) * LANES)
                    f = [held[t * parts + h, at(b * 8 + m), :] for m in range(8 + 2 * REACH)]
                    gs = [east[h, at(b * 8 + m), :] * f[m] for m in range(8 + 2 * REACH)]
                    for r in range(8):
                        i = b * 8 + r
                        m = r + REACH
                        lap = (sixth_center / sixth_second[0]) * f[m] + (f[m + 1] + f[m - 1])
                        grad = gs[m + 1] - gs[m - 1]
                        for k in range(2, REACH + 1):
                            lap = lap + (sixth_second[k - 1] / sixth_second[0]) * (f[m + k] + f[m - k])
                            grad = grad + (sixth_first[k - 1] / sixth_first[0]) * (gs[m + k] - gs[m - k])
                        change = across[at(i), lanes] + (reach * lap - grad)
                        if h == 0:
                            change = change + jnp.where(
                                lane < REACH, pltpu.roll(borders[0], (LANES - home - SLOT * i - 1) % LANES, 1), 0.0)
                        if h == parts - 1:
                            change = change + jnp.where(
                                lane >= LANES - REACH,
                                pltpu.roll(borders[1], (2 * LANES - REACH - SLOT * i) % LANES, 1), 0.0)
                        if s < 2:
                            value = f[m] + change
                            if s == 1:
                                value = 0.75 * start[t * parts + h, at(REACH + i), :] + 0.25 * value
                            fresh[t * parts + h, at(REACH + i), :] = value
                            if h == 0:
                                gather(firsts, value, join_left)
                            if h == parts - 1:
                                gather(finals, value, join_right)
                        else:
                            value = start[t * parts + h, at(REACH + i), :] * (1.0 / 3.0) + (2.0 / 3.0) * (f[m] + change)
                            out[t * parts + h, at(i), :] = jnp.where(ids < species, jnp.maximum(value, 0.0), value)
            across[...] = coming[...]
            if s < 2:
                depart(s + 1, t, firsts, finals)
            else:
                result(t).start()
            return c

        split(held, last)
        across[...] = jnp.dot(pieces[...], band[...], preferred_element_type=jnp.float32)
        split(held, lax.rem(last + 1, tiles))
        lax.fori_loop(0, tiles, tile, 0)

    for s in range(3):
        stage(s)

    for copy in tables:
        copy.wait()

    def finish(t, c):
        result(t).wait()
        for s in range(3):
            for copy in copies(s, t):
                copy.wait_send()
        return c

    lax.fori_loop(0, tiles, finish, 0)


def band_matrix(width):
    here = np.arange(width)
    lag = here[:, None] - here[None, :]
    second = np.where(lag == 0, round(sixth_center * SECOND_SCALE), 0)
    first = np.zeros((width, width))
    for k in range(1, REACH + 1):
        ahead, behind = lag == k, lag == -k
        second = np.where(ahead | behind, round(sixth_second[k - 1] * SECOND_SCALE), second)
        weight = round(sixth_first[k - 1] * FIRST_SCALE)
        first = np.where(ahead, weight, np.where(behind, -weight, first))
    return jnp.asarray(np.concatenate([second, second, first, first], 0), jnp.bfloat16)


def advect(density, warm, leading, trailing, diffusion, pair, scaler, energy, produced, counts):
    species, rows, cols = density.shape
    fields = species + 1
    tiles = (fields + 2) // 8
    if (fields + 2) % 8 or rows * SLOT > LANES or cols % LANES or rows % 8:
        raise ValueError("unsupported sizes")
    parts = cols // LANES
    sizes = (lax.axis_size("grp"), lax.axis_size("gx"))
    wide = pltpu.VMEM((tiles * parts, (rows + 2 * REACH) * 8, LANES), jnp.float32)
    band = band_matrix(cols)
    reactions = pair.shape[1]
    if counts.shape[1] > LANES or species > 64:
        raise ValueError("unsupported sizes")
    length = up(up(reactions, TRIPS), 8)
    weight = spread_weights(reactions)[None]
    args = (density.reshape(species * rows, cols), warm, leading, trailing, diffusion, band, pair, scaler, energy, produced,
            weight, counts)
    count = len(args)
    places = [pltpu.SMEM if n == 4 else pltpu.VMEM for n in range(count)]

    results = [jax.ShapeDtypeStruct((tiles * parts, rows * 8, LANES), jnp.float32),
               jax.ShapeDtypeStruct((3 * length, LANES), jnp.float32),
               jax.ShapeDtypeStruct((2 * up(species, 8), up(length, 16)), jnp.bfloat16),
               jax.ShapeDtypeStruct((1, 2 * up(length, LANES)), jnp.int32),
               jax.ShapeDtypeStruct((1, LANES), jnp.int32)]

    def kernel(*refs):
        advect_kernel(fields, sizes, refs[:count], refs[count:count + len(results)], refs[count + len(results):])

    return pl.pallas_call(
        kernel,
        in_specs=[pl.BlockSpec(memory_space=pltpu.HBM)] * count,
        out_specs=[pl.BlockSpec(memory_space=pltpu.HBM)] * len(results),
        out_shape=results,
        scratch_shapes=[pltpu.VMEM(result.shape, result.dtype) for result in results]
        + [pltpu.SemaphoreType.DMA((tiles + len(results) - 1,))]
        + [place(arg.shape, arg.dtype) for place, arg in zip(places, args)]
        + [pltpu.SemaphoreType.DMA((count - 1 + tiles,)),
           pltpu.VMEM((8, up(length, LANES)), jnp.float32),
           pltpu.VMEM((tiles * 8, LANES), jnp.float32), wide, wide, wide,
           pltpu.VMEM((parts, (rows + 2 * REACH) * 8, LANES), jnp.float32),
           pltpu.VMEM((parts, rows * 8, LANES), jnp.float32),
           pltpu.VMEM((rows * 8, 4 * cols), jnp.bfloat16),
           pltpu.VMEM((rows * 8, cols), jnp.float32),
           pltpu.VMEM((rows * 8, cols), jnp.float32),
           pltpu.VMEM((3, tiles, 2, 8, LANES), jnp.float32),
           pltpu.VMEM((3, tiles, 2, 8, LANES), jnp.float32),
           pltpu.VMEM((2 * REACH, 8, LANES), jnp.float32),
           pltpu.SemaphoreType.DMA((3, tiles, 4)),
           pltpu.SemaphoreType.DMA((3, tiles, 4))],
        compiler_params=pltpu.CompilerParams(collective_id=0, has_side_effects=True),
        name="advect",
    )(*args)


GROUP = 16
PITCH = GROUP + 1
SPAN = 9


def chemistry_kernel(species, chunk, order, counts, pair, warming, rates, table, state, out, warm_out,
                     held, low_gained, high_gained, progress, steps, staged, sems, *losses):
    rows, cols = warm_out.shape
    layers = state.shape[0] * LANES // cols * 8
    per_row = cols // TILE
    tiles = rows * per_row
    warm_row = species
    length = rates.shape[0] // 3
    reactions = length // chunk * chunk
    span = progress.shape[0] // GROUP
    depth = table.shape[1]
    half = table.shape[0] // 2
    blocks = layers // 8
    lines = staged.reshape(staged.shape[0] * staged.shape[1], LANES)
    line_span = staged.shape[1]
    gained = (low_gained, high_gained)

    for t in range(GROUP):
        progress[pl.ds(t * span + reactions, depth - reactions)] = jnp.zeros((depth - reactions, LANES), jnp.float32)
    for loss in losses:
        loss[...] = jnp.zeros_like(loss)

    def at(field):
        return pl.ds(field * PITCH, GROUP)

    def handle(g, c):
        ids = [order[0, g * GROUP + t] for t in range(GROUP)]
        numbers = [counts[t] for t in ids]
        places = [(t % per_row, pl.ds(pl.multiple_of(t // per_row * 8, 8), 8)) for t in ids]
        turn_count = functools.reduce(jnp.maximum, numbers)
        for t in range(GROUP):
            part, at_row = places[t]
            steps[t:t + 1, :] = jnp.full((1, LANES), numbers[t].astype(jnp.float32))
            for f in range(blocks):
                held[pl.ds(f * 8 * PITCH + t, 8, stride=PITCH)] = state[f * per_row + part, at_row, :]

        def advance(s, c):
            heat = jnp.tanh(held[at(warm_row)])

            def react(k, c):
                for j in range(chunk):
                    r = k * chunk + j
                    first = pl.ds(pair[0, r], GROUP)
                    second = pl.ds(pair[0, pair.shape[1] // 2 + r], GROUP)
                    a, e, weight = [jnp.broadcast_to(rates[pl.ds(n * length + r, 1), :], (GROUP, LANES)) for n in range(3)]
                    rate = jnp.exp2(a + e * heat)
                    ca, cb = held[first], held[second]
                    qa, qb = rate * ca, rate * cb
                    progress[pl.ds(r, GROUP, stride=span)] = qa * (weight * cb)
                    n = 2 * (j % (len(losses) // 2))
                    losses[n][first] += qb
                    losses[n + 1][second] += qa
                return c

            lax.fori_loop(0, reactions // chunk, react, 0)
            for n, fill in enumerate(gained):
                for q in range(4 * n, 4 * n + 4):
                    p = jnp.concatenate([progress[pl.ds((2 * q + t) * span, depth)] for t in range(2)], 1)
                    both = jnp.dot(table[...], p.astype(jnp.bfloat16), preferred_element_type=jnp.float32)
                    total = both[:half] + both[half:]
                    for t in range(2):
                        for f in range(half // 8):
                            fill[pl.ds(f * 8 * SPAN + 2 * (q - 4 * n) + t, 8, stride=SPAN)] = (
                                total[f * 8:(f + 1) * 8, t * TILE:(t + 1) * TILE])
                number = steps[8 * n:8 * n + 8, :]
                pace = number * (1.0 / chemistry_span)
                active = s.astype(jnp.float32) < number
                change = jnp.zeros((8, LANES), jnp.float32)
                for j in range(species):
                    place = pl.ds(j * PITCH + 8 * n, 8)
                    x = held[place]
                    destroyed = functools.reduce(jnp.add, [loss[place] for loss in losses])
                    for loss in losses:
                        loss[place] = jnp.zeros((8, LANES), jnp.float32)
                    updated = (pace * x + fill[pl.ds(j * SPAN, 8)]) / (pace + destroyed)
                    change = change + warming[j] * (updated - x)
                    held[place] = jnp.where(active, updated, x)
                place = pl.ds(warm_row * PITCH + 8 * n, 8)
                w = held[place]
                held[place] = jnp.where(active, w + change, w)
            return c

        lax.fori_loop(0, turn_count, advance, 0)
        for t in range(GROUP):
            line = (ids[t] % per_row) * ((warm_row + 1) * line_span) + ids[t] // per_row
            for f in range(0, warm_row + 1, 8):
                n = min(8, warm_row + 1 - f)
                lines[pl.ds(line + f * line_span, n, stride=line_span)] = held[pl.ds(f * PITCH + t, n, stride=PITCH)]
        return c

    lax.fori_loop(0, tiles // GROUP, handle, 0)
    wide = out.reshape(species, rows, cols)
    copies = []
    for n in range(per_row):
        lanes = pl.ds(n * TILE, TILE)
        first = n * (warm_row + 1)
        copies.append(pltpu.make_async_copy(
            staged.at[pl.ds(first, species), pl.ds(0, rows)], wide.at[:, :, lanes], sems.at[0, n]))
        copies.append(pltpu.make_async_copy(
            staged.at[first + species, pl.ds(0, rows)], warm_out.at[:, lanes], sems.at[1, n]))
    for copy in copies:
        copy.start()
    for copy in copies:
        copy.wait()


LOSSES = 4


def chemistry(state, order, counts, pair, warming, rates, table, species, rows, cols):
    layers = state.shape[0] * LANES // cols * 8
    smem = pl.BlockSpec(memory_space=pltpu.SMEM)
    vmem = pl.BlockSpec(memory_space=pltpu.VMEM)
    block = pltpu.VMEM((layers * PITCH, LANES), jnp.float32)
    part = pltpu.VMEM((layers * SPAN, LANES), jnp.float32)
    return pl.pallas_call(
        functools.partial(chemistry_kernel, species, rates.shape[0] // 3 // TRIPS),
        in_specs=[smem, smem, smem, smem, vmem, vmem, vmem],
        out_specs=[pl.BlockSpec(memory_space=pl.ANY)] * 2,
        out_shape=[jax.ShapeDtypeStruct((species * rows, cols), jnp.float32),
                   jax.ShapeDtypeStruct((rows, cols), jnp.float32)],
        scratch_shapes=[block, part, part,
                        pltpu.VMEM((GROUP * (table.shape[1] + 1), LANES), jnp.float32),
                        pltpu.VMEM((GROUP, LANES), jnp.float32),
                        pltpu.VMEM((cols // TILE * (species + 1), rows + 8, TILE), jnp.float32),
                        pltpu.SemaphoreType.DMA((2, cols // TILE))]
        + [block] * LOSSES,
        name="chemistry",
    )(order, counts, pair, warming, rates, table, state)


def body(component_density, scaled_thermal_state, leading_direction_flow, trailing_direction_flow,
         spreading_coefficient, colliding_pair, natural_exponent_scaler, arrhenius_energy,
         stoichiometric_output, formation_warming, explicit_increments):
    species, rows, cols = component_density.shape
    clipped, rates, table, pair, order = advect(
        component_density, scaled_thermal_state, leading_direction_flow, trailing_direction_flow, spreading_coefficient,
        colliding_pair.T, natural_exponent_scaler, arrhenius_energy, stoichiometric_output.T,
        explicit_increments[None])
    reacted, warm = chemistry(clipped, order, explicit_increments, pair, formation_warming, rates, table,
                              species, rows, cols)
    return reacted.reshape(species, rows, cols), warm


def solution(mesh):
    return jax.shard_map(
        body,
        mesh=mesh,
        in_specs=(
            P(None, "gx", "grp"),
            P("gx", "grp"),
            P("gx", "grp"),
            P("gx", "grp"),
            P(),
            P(),
            P(),
            P(),
            P(),
            P(),
            P(("grp", "gx")),
        ),
        out_specs=(P(None, "gx", "grp"), P("gx", "grp")),
        check_vma=False,
    )
```

```python
import functools
import math

import jax
import jax.numpy as jnp
import numpy as np
from jax import lax
from jax.experimental import pallas as pl
from jax.experimental.pallas import tpu as pltpu
from jax.sharding import PartitionSpec as P

TILE = 128
FIRST_SCALE = 60.0
SECOND_SCALE = 180.0
transport_step = 0.4
chemistry_span = 0.5
sixth_first = (0.75, -0.15, 1.0 / 60.0)
sixth_second = (1.5, -0.15, 1.0 / 90.0)
sixth_center = -49.0 / 18.0


def up(n, m):
    return -(-n // m) * m


def spread_weights(reactions):
    golden = (math.sqrt(5.0) - 1.0) / 2.0
    return np.exp2((np.arange(reactions) * golden) % 1.0).astype(np.float32)


REACH = 3
SLOT = 4
LANES = 128
NEVER = -16384.0
TRIPS = 3
BAND = 4


def halves(value):
    high = value.astype(jnp.bfloat16)
    return high, (value - high.astype(jnp.float32)).astype(jnp.bfloat16)


def prepare_tables(pair, scaler, energy, produced, weight, counts, rates, table, offsets, order, lines):
    reactions = pair.shape[1]
    length = rates.shape[0] // 3
    species = produced.shape[0]
    half = table.shape[0] // 2
    scale = 1.0 / math.log(2.0)
    wide = lines.shape[1]
    lines[...] = jnp.zeros_like(lines)
    lines[0:1, :] = jnp.full((1, wide), NEVER)
    lines[0, 0:reactions] = scaler[...] * scale
    lines[1, 0:reactions] = energy[...] * scale
    lines[2:3, 0:reactions] = weight[...]
    for n in range(3):
        for r in range(0, length, LANES):
            count = min(LANES, length - r)
            row = jnp.broadcast_to(lines[n:n + 1, r:r + LANES], (LANES, LANES))
            rates[n * length + r:n * length + r + count, :] = row.T[:count]
    table[...] = jnp.zeros_like(table)
    high, low = halves(produced[...] / weight[...])
    table[0:species, 0:reactions] = high
    table[half:half + species, 0:reactions] = low
    offsets[...] = jnp.zeros_like(offsets)
    for n in range(2):
        offsets[:, n * wide:n * wide + reactions] = pair[n:n + 1, :] * PITCH
    tiles = counts.shape[1]
    lines[3:4, 0:tiles] = counts[...].astype(jnp.float32) * tiles
    key = lines[3:4, 0:LANES] + lax.broadcasted_iota(jnp.int32, (1, LANES), 1).astype(jnp.float32)
    down = lax.broadcasted_iota(jnp.int32, (LANES, LANES), 0).astype(jnp.float32)
    along = lax.broadcasted_iota(jnp.int32, (LANES, LANES), 1)
    across = jnp.broadcast_to(key, (LANES, LANES))
    before = jnp.where((across < across.T) & (along < tiles), 1.0, 0.0)
    rank = jnp.sum(before, axis=1, keepdims=True)
    here = jnp.where((rank == along.astype(jnp.float32)) & (down < tiles), down, 0.0)
    order[...] = jnp.sum(here, axis=0, keepdims=True).astype(jnp.int32)


def advect_kernel(fields, sizes, sources, targets, scratch):
    (out, rates, table, offsets, order, stored, density, warm, leading, trailing, diffusion, band, pair, scaler, energy, produced, weight, counts, loaded,
     lines, spread, start, one, two, east, north, pieces, across, coming, packed, landed, flows, send, recv) = scratch
    n_grp, n_gx = sizes
    g, x = lax.axis_index("grp"), lax.axis_index("gx")
    rows, cols = warm.shape
    parts = cols // LANES
    tiles = start.shape[0] // parts
    species = fields - 1
    last = fields // 8
    up, down = (g, lax.rem(x + n_gx - 1, n_gx)), (g, lax.rem(x + 1, n_gx))
    left, right = (lax.rem(g + n_grp - 1, n_grp), x), (lax.rem(g + 1, n_grp), x)
    places = (warm, leading, trailing, diffusion, band, pair, scaler, energy, produced, weight, counts)
    inputs = [pltpu.make_async_copy(src, dst, loaded.at[n]) for n, (src, dst) in enumerate(zip(sources[1:], places))]

    def layers_in(t, count):
        span = pl.ds(t * 8 * rows if isinstance(t, int) else pl.multiple_of(t * 8 * rows, 8), count * rows)
        return pltpu.make_async_copy(sources[0].at[span], density.at[span], loaded.at[len(places) + t])

    early, late = inputs[:BAND] + inputs[BAND + 1:], inputs[BAND]
    for copy in early:
        copy.start()
    layers_in(last, species - last * 8).start()

    def begin(t, c):
        layers_in(t, 8).start()
        return c

    lax.fori_loop(0, last, begin, 0)
    late.start()
    barrier = pltpu.get_barrier_semaphore()
    for place in (up, down, left, right):
        pl.semaphore_signal(barrier, inc=1, device_id=place, device_id_type=pl.DeviceIdType.MESH)

    lane = lax.broadcasted_iota(jnp.int32, (8, LANES), 1)
    slot = lane % SLOT
    home = LANES - SLOT * rows

    def at(row):
        return pl.ds(row * 8 if isinstance(row, int) else pl.multiple_of(row * 8, 8), 8)

    def spread_out(read, t, sub):
        for q in range(rows // 8):
            for h in range(parts):
                start[t * parts + h, pl.ds((REACH + q * 8) * 8 + sub, 8, stride=8), :] = read(q, h)

    def of_density(f):
        return lambda q, h: density[pl.ds(pl.multiple_of(f * rows + q * 8, 8), 8), h * LANES:(h + 1) * LANES]

    def of_plane(ref):
        return lambda q, h: ref[q * 8:(q + 1) * 8, h * LANES:(h + 1) * LANES]

    def result(t):
        both = pl.ds(t * parts, parts)
        return pltpu.make_async_copy(out.at[both], targets[0].at[both], stored.at[t])

    def copies(s, t):
        held = (start, one, two)[s]
        both = pl.ds(t * parts, parts)
        plan = [
            (held.at[both, pl.ds(REACH * 8, REACH * 8)], held.at[both, pl.ds((REACH + rows) * 8, REACH * 8)], up),
            (held.at[both, pl.ds(rows * 8, REACH * 8)], held.at[both, pl.ds(0, REACH * 8)], down),
            (packed.at[s, t, 0], landed.at[s, t, 1], left),
            (packed.at[s, t, 1], landed.at[s, t, 0], right),
        ]
        return [pltpu.make_async_remote_copy(
            src_ref=src, dst_ref=dst, send_sem=send.at[s, t, n], recv_sem=recv.at[s, t, n],
            device_id=place, device_id_type=pl.DeviceIdType.MESH) for n, (src, dst, place) in enumerate(plan)]

    def join_left(a, n, b, m):
        return jnp.where(lane < SLOT * n, a, pltpu.roll(b, SLOT * n, 1))

    def join_right(a, n, b, m):
        return jnp.where(lane >= LANES - SLOT * m, b, pltpu.roll(a, LANES - SLOT * m, 1))

    def gather(stack, value, join):
        stack.append((1, value))
        while len(stack) > 1 and stack[-1][0] == stack[-2][0]:
            m, b = stack.pop()
            n, a = stack.pop()
            stack.append((n + m, join(a, n, b, m)))

    def gathered(stack, join):
        while len(stack) > 1:
            m, b = stack.pop()
            n, a = stack.pop()
            stack.append((n + m, join(a, n, b, m)))
        return stack[0][1]

    def depart(s, t, firsts, finals):
        packed[s, t, 0] = gathered(firsts, join_left)
        packed[s, t, 1] = gathered(finals, join_right)
        for copy in copies(s, t):
            copy.start()

    def pack(t):
        firsts, finals = [], []
        for i in range(rows):
            gather(firsts, start[t * parts, at(REACH + i), :], join_left)
            gather(finals, start[t * parts + parts - 1, at(REACH + i), :], join_right)
        depart(0, t, firsts, finals)

    for copy in early:
        copy.wait()
    for f in range(tiles * 8):
        spread[f:f + 1, :] = jnp.full((1, LANES), diffusion[f] if f < fields else 0.0)
    prepare_tables(pair, scaler, energy, produced, weight, counts, rates, table, offsets, order, lines)
    tables = [pltpu.make_async_copy(src, dst, stored.at[tiles + n]) for n, (src, dst) in enumerate(
        zip((rates, table, offsets, order), targets[1:]))]
    for copy in tables:
        copy.start()
    pull, push = transport_step * sixth_first[0], -transport_step / FIRST_SCALE
    for i in range(rows):
        for h in range(parts):
            lanes = slice(h * LANES, (h + 1) * LANES)
            east[h, at(REACH + i), :] = jnp.broadcast_to(pull * leading[i:i + 1, lanes], (8, LANES))
            north[h, at(i), :] = jnp.broadcast_to(push * trailing[i:i + 1, lanes], (8, LANES))

    layers_in(last, species - last * 8).wait()
    for f in range(last * 8, species):
        spread_out(of_density(f), last, f % 8)
    for n, ref in enumerate((warm, leading, trailing)):
        spread_out(of_plane(ref), last, (species + n) % 8)
    pl.semaphore_wait(barrier, 4)

    def prepare(t, c):
        pack(lax.rem(t + last, tiles))
        layers_in(t, 8).wait()
        for sub in range(8):
            spread_out(of_density(t * 8 + sub), t, sub)
        return c

    lax.fori_loop(0, last, prepare, 0)
    pack(last - 1)
    def arrive(s, t):
        for copy in copies(s, t):
            copy.wait_recv()

    late.wait()
    arrive(0, last)
    u_sub, v_sub = fields % 8, (fields + 1) % 8
    for r in (*range(REACH), *range(REACH + rows, 2 * REACH + rows)):
        for h in range(parts):
            east[h, at(r), :] = jnp.broadcast_to(
                pull * start[last * parts + h, pl.ds(r * 8 + u_sub, 1), :], (8, LANES))
    for side in range(2):
        flow = jnp.broadcast_to(landed[0, last, side, pl.ds(v_sub, 1), :], (8, LANES))
        for k in range(1, REACH + 1):
            inside = slot >= SLOT - k if side == 0 else slot < k
            weight = (1.0 if side == 0 else -1.0) * transport_step * sixth_first[k - 1]
            flows[side * REACH + k - 1] = jnp.where(inside, weight * flow, 0.0)

    def split(held, t):
        scale = spread[at(t), :] * (transport_step / SECOND_SCALE)
        for i in range(rows):
            fs = [held[t * parts + h, at(REACH + i), :] for h in range(parts)]
            f_high, f_low = halves(jnp.concatenate([scale * f for f in fs], 1))
            g_high, g_low = halves(jnp.concatenate([north[h, at(i), :] * f for h, f in enumerate(fs)], 1))
            for m, piece in enumerate((f_high, f_low, g_high, g_low)):
                pieces[at(i), m * cols:(m + 1) * cols] = piece

    def stage(s):
        held, fresh = (start, one, two)[s], (one, two, None)[s]

        def tile(n, c):
            t = lax.rem(n + last, tiles)

            @pl.when(n > 0 if s == 0 else n >= 0)
            def _():
                arrive(s, t)

            d = spread[at(t), :] * transport_step
            coming[...] = jnp.dot(pieces[...], band[...], preferred_element_type=jnp.float32)
            split(held, lax.rem(t + 2, tiles))
            firsts, finals = [], []

            borders = []
            for side in range(2):
                halo = landed[s, t, side]
                total = None
                for k in range(1, REACH + 1):
                    inside = slot >= SLOT - k if side == 0 else slot < k
                    part = (jnp.where(inside, sixth_second[k - 1] * d, 0.0) + flows[side * REACH + k - 1]) * halo
                    if k < REACH:
                        part = pltpu.roll(part, (k - REACH) % LANES if side == 0 else REACH - k, 1)
                    total = part if total is None else total + part
                borders.append(total)
            ids = t * 8 + lax.broadcasted_iota(jnp.int32, (8, LANES), 0)
            reach = sixth_second[0] * d

            for b in range(rows // 8):
                for h in range(parts):
                    lanes = slice(h * LANES, (h + 1) * LANES)
                    f = [held[t * parts + h, at(b * 8 + m), :] for m in range(8 + 2 * REACH)]
                    gs = [east[h, at(b * 8 + m), :] * f[m] for m in range(8 + 2 * REACH)]
                    for r in range(8):
                        i = b * 8 + r
                        m = r + REACH
                        lap = (sixth_center / sixth_second[0]) * f[m] + (f[m + 1] + f[m - 1])
                        grad = gs[m + 1] - gs[m - 1]
                        for k in range(2, REACH + 1):
                            lap = lap + (sixth_second[k - 1] / sixth_second[0]) * (f[m + k] + f[m - k])
                            grad = grad + (sixth_first[k - 1] / sixth_first[0]) * (gs[m + k] - gs[m - k])
                        change = across[at(i), lanes] + (reach * lap - grad)
                        if h == 0:
                            change = change + jnp.where(
                                lane < REACH, pltpu.roll(borders[0], (LANES - home - SLOT * i - 1) % LANES, 1), 0.0)
                        if h == parts - 1:
                            change = change + jnp.where(
                                lane >= LANES - REACH,
                                pltpu.roll(borders[1], (2 * LANES - REACH - SLOT * i) % LANES, 1), 0.0)
                        if s < 2:
                            value = f[m] + change
                            if s == 1:
                                value = 0.75 * start[t * parts + h, at(REACH + i), :] + 0.25 * value
                            fresh[t * parts + h, at(REACH + i), :] = value
                            if h == 0:
                                gather(firsts, value, join_left)
                            if h == parts - 1:
                                gather(finals, value, join_right)
                        else:
                            value = start[t * parts + h, at(REACH + i), :] * (1.0 / 3.0) + (2.0 / 3.0) * (f[m] + change)
                            out[t * parts + h, at(i), :] = jnp.where(ids < species, jnp.maximum(value, 0.0), value)
            across[...] = coming[...]
            if s < 2:
                depart(s + 1, t, firsts, finals)
            else:
                result(t).start()
            return c

        split(held, last)
        across[...] = jnp.dot(pieces[...], band[...], preferred_element_type=jnp.float32)
        split(held, lax.rem(last + 1, tiles))
        lax.fori_loop(0, tiles, tile, 0)

    for s in range(3):
        stage(s)

    for copy in tables:
        copy.wait()

    def finish(t, c):
        result(t).wait()
        for s in range(3):
            for copy in copies(s, t):
                copy.wait_send()
        return c

    lax.fori_loop(0, tiles, finish, 0)


def band_matrix(width):
    here = np.arange(width)
    lag = here[:, None] - here[None, :]
    second = np.where(lag == 0, round(sixth_center * SECOND_SCALE), 0)
    first = np.zeros((width, width))
    for k in range(1, REACH + 1):
        ahead, behind = lag == k, lag == -k
        second = np.where(ahead | behind, round(sixth_second[k - 1] * SECOND_SCALE), second)
        weight = round(sixth_first[k - 1] * FIRST_SCALE)
        first = np.where(ahead, weight, np.where(behind, -weight, first))
    return jnp.asarray(np.concatenate([second, second, first, first], 0), jnp.bfloat16)


def advect(density, warm, leading, trailing, diffusion, pair, scaler, energy, produced, counts):
    species, rows, cols = density.shape
    fields = species + 1
    tiles = (fields + 2) // 8
    if (fields + 2) % 8 or rows * SLOT > LANES or cols % LANES or rows % 8:
        raise ValueError("unsupported sizes")
    parts = cols // LANES
    sizes = (lax.axis_size("grp"), lax.axis_size("gx"))
    wide = pltpu.VMEM((tiles * parts, (rows + 2 * REACH) * 8, LANES), jnp.float32)
    band = band_matrix(cols)
    reactions = pair.shape[1]
    if counts.shape[1] > LANES or species > 64:
        raise ValueError("unsupported sizes")
    length = up(up(reactions, TRIPS), 8)
    weight = spread_weights(reactions)[None]
    args = (density.reshape(species * rows, cols), warm, leading, trailing, diffusion, band, pair, scaler, energy, produced,
            weight, counts)
    count = len(args)
    places = [pltpu.SMEM if n == 4 else pltpu.VMEM for n in range(count)]

    results = [jax.ShapeDtypeStruct((tiles * parts, rows * 8, LANES), jnp.float32),
               jax.ShapeDtypeStruct((3 * length, LANES), jnp.float32),
               jax.ShapeDtypeStruct((2 * up(species, 8), up(length, 16)), jnp.bfloat16),
               jax.ShapeDtypeStruct((1, 2 * up(length, LANES)), jnp.int32),
               jax.ShapeDtypeStruct((1, LANES), jnp.int32)]

    def kernel(*refs):
        advect_kernel(fields, sizes, refs[:count], refs[count:count + len(results)], refs[count + len(results):])

    return pl.pallas_call(
        kernel,
        in_specs=[pl.BlockSpec(memory_space=pltpu.HBM)] * count,
        out_specs=[pl.BlockSpec(memory_space=pltpu.HBM)] * len(results),
        out_shape=results,
        scratch_shapes=[pltpu.VMEM(result.shape, result.dtype) for result in results]
        + [pltpu.SemaphoreType.DMA((tiles + len(results) - 1,))]
        + [place(arg.shape, arg.dtype) for place, arg in zip(places, args)]
        + [pltpu.SemaphoreType.DMA((count - 1 + tiles,)),
           pltpu.VMEM((8, up(length, LANES)), jnp.float32),
           pltpu.VMEM((tiles * 8, LANES), jnp.float32), wide, wide, wide,
           pltpu.VMEM((parts, (rows + 2 * REACH) * 8, LANES), jnp.float32),
           pltpu.VMEM((parts, rows * 8, LANES), jnp.float32),
           pltpu.VMEM((rows * 8, 4 * cols), jnp.bfloat16),
           pltpu.VMEM((rows * 8, cols), jnp.float32),
           pltpu.VMEM((rows * 8, cols), jnp.float32),
           pltpu.VMEM((3, tiles, 2, 8, LANES), jnp.float32),
           pltpu.VMEM((3, tiles, 2, 8, LANES), jnp.float32),
           pltpu.VMEM((2 * REACH, 8, LANES), jnp.float32),
           pltpu.SemaphoreType.DMA((3, tiles, 4)),
           pltpu.SemaphoreType.DMA((3, tiles, 4))],
        compiler_params=pltpu.CompilerParams(collective_id=0, has_side_effects=True),
        name="advect",
    )(*args)


GROUP = 16
PITCH = GROUP + 1
SPAN = 9


def chemistry_kernel(species, chunk, order, counts, pair, warming, rates_in, table_in, state_in, out, warm_out,
                     rates, table, state, loaded, held, low_gained, high_gained, progress, steps, staged, sems, *losses):
    rows, cols = warm_out.shape
    layers = state.shape[0] * LANES // cols * 8
    per_row = cols // TILE
    tiles = rows * per_row
    warm_row = species
    length = rates.shape[0] // 3
    reactions = length // chunk * chunk
    span = progress.shape[0] // GROUP
    depth = table.shape[1]
    half = table.shape[0] // 2
    blocks = layers // 8
    lines = staged.reshape(staged.shape[0] * staged.shape[1], LANES)
    line_span = staged.shape[1]
    gained = (low_gained, high_gained)

    inputs = [pltpu.make_async_copy(src, dst, loaded.at[n]) for n, (src, dst) in enumerate(
        zip((state_in, rates_in, table_in), (state, rates, table)))]
    for copy in inputs:
        copy.start()
    plain = state.reshape(state.shape[0] * state.shape[1], LANES)
    part_rows = state.shape[1]
    for t in range(GROUP):
        progress[pl.ds(t * span + reactions, depth - reactions)] = jnp.zeros((depth - reactions, LANES), jnp.float32)
    for loss in losses:
        loss[...] = jnp.zeros_like(loss)
    for copy in inputs:
        copy.wait()

    def at(field):
        return pl.ds(field * PITCH, GROUP)

    def handle(g, c):
        ids = [order[0, g * GROUP + t] for t in range(GROUP)]
        numbers = [counts[t] for t in ids]
        bases = [pl.multiple_of((t % per_row) * part_rows + t // per_row * 8, 8) for t in ids]
        turn_count = functools.reduce(jnp.maximum, numbers)
        for t in range(GROUP):
            steps[t:t + 1, :] = jnp.full((1, LANES), numbers[t].astype(jnp.float32))
            for f in range(blocks):
                held[pl.ds(f * 8 * PITCH + t, 8, stride=PITCH)] = (
                    plain[pl.ds(pl.multiple_of(bases[t] + f * per_row * part_rows, 8), 8), :])

        def advance(s, c):
            heat = jnp.tanh(held[at(warm_row)])

            def react(k, c):
                for j in range(chunk):
                    r = k * chunk + j
                    first = pl.ds(pair[0, r], GROUP)
                    second = pl.ds(pair[0, pair.shape[1] // 2 + r], GROUP)
                    a, e, weight = [jnp.broadcast_to(rates[pl.ds(n * length + r, 1), :], (GROUP, LANES)) for n in range(3)]
                    rate = jnp.exp2(a + e * heat)
                    ca, cb = held[first], held[second]
                    qa, qb = rate * ca, rate * cb
                    progress[pl.ds(r, GROUP, stride=span)] = qa * (weight * cb)
                    n = 2 * (j % (len(losses) // 2))
                    losses[n][first] += qb
                    losses[n + 1][second] += qa
                return c

            lax.fori_loop(0, reactions // chunk, react, 0)
            for n, fill in enumerate(gained):
                for q in range(4 * n, 4 * n + 4):
                    p = jnp.concatenate([progress[pl.ds((2 * q + t) * span, depth)] for t in range(2)], 1)
                    both = jnp.dot(table[...], p.astype(jnp.bfloat16), preferred_element_type=jnp.float32)
                    total = both[:half] + both[half:]
                    for t in range(2):
                        for f in range(half // 8):
                            fill[pl.ds(f * 8 * SPAN + 2 * (q - 4 * n) + t, 8, stride=SPAN)] = (
                                total[f * 8:(f + 1) * 8, t * TILE:(t + 1) * TILE])
                number = steps[8 * n:8 * n + 8, :]
                pace = number * (1.0 / chemistry_span)
                active = s.astype(jnp.float32) < number
                change = jnp.zeros((8, LANES), jnp.float32)
                for j in range(species):
                    place = pl.ds(j * PITCH + 8 * n, 8)
                    x = held[place]
                    destroyed = functools.reduce(jnp.add, [loss[place] for loss in losses])
                    for loss in losses:
                        loss[place] = jnp.zeros((8, LANES), jnp.float32)
                    updated = (pace * x + fill[pl.ds(j * SPAN, 8)]) / (pace + destroyed)
                    change = change + warming[j] * (updated - x)
                    held[place] = jnp.where(active, updated, x)
                place = pl.ds(warm_row * PITCH + 8 * n, 8)
                w = held[place]
                held[place] = jnp.where(active, w + change, w)
            return c

        lax.fori_loop(0, turn_count, advance, 0)
        for t in range(GROUP):
            line = (ids[t] % per_row) * ((warm_row + 1) * line_span) + ids[t] // per_row
            for f in range(0, warm_row + 1, 8):
                n = min(8, warm_row + 1 - f)
                lines[pl.ds(line + f * line_span, n, stride=line_span)] = held[pl.ds(f * PITCH + t, n, stride=PITCH)]
        return c

    lax.fori_loop(0, tiles // GROUP, handle, 0)
    wide = out.reshape(species, rows, cols)
    copies = []
    for n in range(per_row):
        lanes = pl.ds(n * TILE, TILE)
        first = n * (warm_row + 1)
        copies.append(pltpu.make_async_copy(
            staged.at[pl.ds(first, species), pl.ds(0, rows)], wide.at[:, :, lanes], sems.at[0, n]))
        copies.append(pltpu.make_async_copy(
            staged.at[first + species, pl.ds(0, rows)], warm_out.at[:, lanes], sems.at[1, n]))
    for copy in copies:
        copy.start()
    for copy in copies:
        copy.wait()


LOSSES = 4


def chemistry(state, order, counts, pair, warming, rates, table, species, rows, cols):
    layers = state.shape[0] * LANES // cols * 8
    smem = pl.BlockSpec(memory_space=pltpu.SMEM)
    block = pltpu.VMEM((layers * PITCH, LANES), jnp.float32)
    part = pltpu.VMEM((layers * SPAN, LANES), jnp.float32)
    return pl.pallas_call(
        functools.partial(chemistry_kernel, species, rates.shape[0] // 3 // TRIPS),
        in_specs=[smem] * 4 + [pl.BlockSpec(memory_space=pltpu.HBM)] * 3,
        out_specs=[pl.BlockSpec(memory_space=pl.ANY)] * 2,
        out_shape=[jax.ShapeDtypeStruct((species * rows, cols), jnp.float32),
                   jax.ShapeDtypeStruct((rows, cols), jnp.float32)],
        scratch_shapes=[pltpu.VMEM(ref.shape, ref.dtype) for ref in (rates, table, state)]
        + [pltpu.SemaphoreType.DMA((3,)), block, part, part,
                        pltpu.VMEM((GROUP * (table.shape[1] + 1), LANES), jnp.float32),
                        pltpu.VMEM((GROUP, LANES), jnp.float32),
                        pltpu.VMEM((cols // TILE * (species + 1), rows + 8, TILE), jnp.float32),
                        pltpu.SemaphoreType.DMA((2, cols // TILE))]
        + [block] * LOSSES,
        compiler_params=pltpu.CompilerParams(),
        name="chemistry",
    )(order, counts, pair, warming, rates, table, state)


def body(component_density, scaled_thermal_state, leading_direction_flow, trailing_direction_flow,
         spreading_coefficient, colliding_pair, natural_exponent_scaler, arrhenius_energy,
         stoichiometric_output, formation_warming, explicit_increments):
    species, rows, cols = component_density.shape
    clipped, rates, table, pair, order = advect(
        component_density, scaled_thermal_state, leading_direction_flow, trailing_direction_flow, spreading_coefficient,
        colliding_pair.T, natural_exponent_scaler, arrhenius_energy, stoichiometric_output.T,
        explicit_increments[None])
    reacted, warm = chemistry(clipped, order, explicit_increments, pair, formation_warming, rates, table,
                              species, rows, cols)
    return reacted.reshape(species, rows, cols), warm


def solution(mesh):
    return jax.shard_map(
        body,
        mesh=mesh,
        in_specs=(
            P(None, "gx", "grp"),
            P("gx", "grp"),
            P("gx", "grp"),
            P("gx", "grp"),
            P(),
            P(),
            P(),
            P(),
            P(),
            P(),
            P(("grp", "gx")),
        ),
        out_specs=(P(None, "gx", "grp"), P("gx", "grp")),
        check_vma=False,
    )
```

```python
import functools
import math

import jax
import jax.numpy as jnp
import numpy as np
from jax import lax
from jax.experimental import pallas as pl
from jax.experimental.pallas import tpu as pltpu
from jax.sharding import PartitionSpec as P

TILE = 128
FIRST_SCALE = 60.0
SECOND_SCALE = 180.0
transport_step = 0.4
chemistry_span = 0.5
sixth_first = (0.75, -0.15, 1.0 / 60.0)
sixth_second = (1.5, -0.15, 1.0 / 90.0)
sixth_center = -49.0 / 18.0


def up(n, m):
    return -(-n // m) * m


def spread_weights(reactions):
    golden = (math.sqrt(5.0) - 1.0) / 2.0
    return np.exp2((np.arange(reactions) * golden) % 1.0).astype(np.float32)


REACH = 3
SLOT = 4
LANES = 128
NEVER = -16384.0
TRIPS = 2
BAND = 4


def halves(value):
    high = value.astype(jnp.bfloat16)
    return high, (value - high.astype(jnp.float32)).astype(jnp.bfloat16)


def prepare_tables(pair, scaler, energy, produced, weight, counts, rates, table, offsets, order, lines):
    reactions = pair.shape[1]
    length = rates.shape[0] // 3
    species = produced.shape[0]
    half = table.shape[0] // 2
    scale = 1.0 / math.log(2.0)
    wide = lines.shape[1]
    lines[...] = jnp.zeros_like(lines)
    lines[0:1, :] = jnp.full((1, wide), NEVER)
    lines[0, 0:reactions] = scaler[...] * scale
    lines[1, 0:reactions] = energy[...] * scale
    lines[2:3, 0:reactions] = weight[...]
    for n in range(3):
        for r in range(0, length, LANES):
            count = min(LANES, length - r)
            row = jnp.broadcast_to(lines[n:n + 1, r:r + LANES], (LANES, LANES))
            rates[n * length + r:n * length + r + count, :] = row.T[:count]
    table[...] = jnp.zeros_like(table)
    high, low = halves(produced[...] / weight[...])
    table[0:species, 0:reactions] = high
    table[half:half + species, 0:reactions] = low
    offsets[...] = jnp.zeros_like(offsets)
    for n in range(2):
        offsets[:, n * wide:n * wide + reactions] = pair[n:n + 1, :] * PITCH
    tiles = counts.shape[1]
    lines[3:4, 0:tiles] = counts[...].astype(jnp.float32) * tiles
    key = lines[3:4, 0:LANES] + lax.broadcasted_iota(jnp.int32, (1, LANES), 1).astype(jnp.float32)
    down = lax.broadcasted_iota(jnp.int32, (LANES, LANES), 0).astype(jnp.float32)
    along = lax.broadcasted_iota(jnp.int32, (LANES, LANES), 1)
    across = jnp.broadcast_to(key, (LANES, LANES))
    before = jnp.where((across < across.T) & (along < tiles), 1.0, 0.0)
    rank = jnp.sum(before, axis=1, keepdims=True)
    here = jnp.where((rank == along.astype(jnp.float32)) & (down < tiles), down, 0.0)
    order[...] = jnp.sum(here, axis=0, keepdims=True).astype(jnp.int32)


def advect_kernel(fields, sizes, sources, targets, scratch):
    (out, rates, table, offsets, order, stored, density, warm, leading, trailing, diffusion, band, pair, scaler, energy, produced, weight, counts, loaded,
     lines, spread, start, one, two, east, north, pieces, across, coming, packed, landed, flows, send, recv) = scratch
    n_grp, n_gx = sizes
    g, x = lax.axis_index("grp"), lax.axis_index("gx")
    rows, cols = warm.shape
    parts = cols // LANES
    tiles = start.shape[0] // parts
    species = fields - 1
    last = fields // 8
    up, down = (g, lax.rem(x + n_gx - 1, n_gx)), (g, lax.rem(x + 1, n_gx))
    left, right = (lax.rem(g + n_grp - 1, n_grp), x), (lax.rem(g + 1, n_grp), x)
    places = (warm, leading, trailing, diffusion, band, pair, scaler, energy, produced, weight, counts)
    inputs = [pltpu.make_async_copy(src, dst, loaded.at[n]) for n, (src, dst) in enumerate(zip(sources[1:], places))]

    def layers_in(t, count):
        span = pl.ds(t * 8 * rows if isinstance(t, int) else pl.multiple_of(t * 8 * rows, 8), count * rows)
        return pltpu.make_async_copy(sources[0].at[span], density.at[span], loaded.at[len(places) + t])

    early, late = inputs[:BAND] + inputs[BAND + 1:], inputs[BAND]
    for copy in early:
        copy.start()
    layers_in(last, species - last * 8).start()

    def begin(t, c):
        layers_in(t, 8).start()
        return c

    lax.fori_loop(0, last, begin, 0)
    late.start()
    barrier = pltpu.get_barrier_semaphore()
    for place in (up, down, left, right):
        pl.semaphore_signal(barrier, inc=1, device_id=place, device_id_type=pl.DeviceIdType.MESH)

    lane = lax.broadcasted_iota(jnp.int32, (8, LANES), 1)
    slot = lane % SLOT
    home = LANES - SLOT * rows

    def at(row):
        return pl.ds(row * 8 if isinstance(row, int) else pl.multiple_of(row * 8, 8), 8)

    def spread_out(read, t, sub):
        for q in range(rows // 8):
            for h in range(parts):
                start[t * parts + h, pl.ds((REACH + q * 8) * 8 + sub, 8, stride=8), :] = read(q, h)

    def of_density(f):
        return lambda q, h: density[pl.ds(pl.multiple_of(f * rows + q * 8, 8), 8), h * LANES:(h + 1) * LANES]

    def of_plane(ref):
        return lambda q, h: ref[q * 8:(q + 1) * 8, h * LANES:(h + 1) * LANES]

    def result(t):
        both = pl.ds(t * parts, parts)
        return pltpu.make_async_copy(out.at[both], targets[0].at[both], stored.at[t])

    def copies(s, t):
        held = (start, one, two)[s]
        both = pl.ds(t * parts, parts)
        plan = [
            (held.at[both, pl.ds(REACH * 8, REACH * 8)], held.at[both, pl.ds((REACH + rows) * 8, REACH * 8)], up),
            (held.at[both, pl.ds(rows * 8, REACH * 8)], held.at[both, pl.ds(0, REACH * 8)], down),
            (packed.at[s, t, 0], landed.at[s, t, 1], left),
            (packed.at[s, t, 1], landed.at[s, t, 0], right),
        ]
        return [pltpu.make_async_remote_copy(
            src_ref=src, dst_ref=dst, send_sem=send.at[s, t, n], recv_sem=recv.at[s, t, n],
            device_id=place, device_id_type=pl.DeviceIdType.MESH) for n, (src, dst, place) in enumerate(plan)]

    def join_left(a, n, b, m):
        return jnp.where(lane < SLOT * n, a, pltpu.roll(b, SLOT * n, 1))

    def join_right(a, n, b, m):
        return jnp.where(lane >= LANES - SLOT * m, b, pltpu.roll(a, LANES - SLOT * m, 1))

    def gather(stack, value, join):
        stack.append((1, value))
        while len(stack) > 1 and stack[-1][0] == stack[-2][0]:
            m, b = stack.pop()
            n, a = stack.pop()
            stack.append((n + m, join(a, n, b, m)))

    def gathered(stack, join):
        while len(stack) > 1:
            m, b = stack.pop()
            n, a = stack.pop()
            stack.append((n + m, join(a, n, b, m)))
        return stack[0][1]

    def depart(s, t, firsts, finals):
        packed[s, t, 0] = gathered(firsts, join_left)
        packed[s, t, 1] = gathered(finals, join_right)
        for copy in copies(s, t):
            copy.start()

    def pack(t):
        firsts, finals = [], []
        for i in range(rows):
            gather(firsts, start[t * parts, at(REACH + i), :], join_left)
            gather(finals, start[t * parts + parts - 1, at(REACH + i), :], join_right)
        depart(0, t, firsts, finals)

    for copy in early:
        copy.wait()
    for f in range(tiles * 8):
        spread[f:f + 1, :] = jnp.full((1, LANES), diffusion[f] if f < fields else 0.0)
    prepare_tables(pair, scaler, energy, produced, weight, counts, rates, table, offsets, order, lines)
    tables = [pltpu.make_async_copy(src, dst, stored.at[tiles + n]) for n, (src, dst) in enumerate(
        zip((rates, table, offsets, order), targets[1:]))]
    for copy in tables:
        copy.start()
    pull, push = transport_step * sixth_first[0], -transport_step / FIRST_SCALE
    for i in range(rows):
        for h in range(parts):
            lanes = slice(h * LANES, (h + 1) * LANES)
            east[h, at(REACH + i), :] = jnp.broadcast_to(pull * leading[i:i + 1, lanes], (8, LANES))
            north[h, at(i), :] = jnp.broadcast_to(push * trailing[i:i + 1, lanes], (8, LANES))

    layers_in(last, species - last * 8).wait()
    for f in range(last * 8, species):
        spread_out(of_density(f), last, f % 8)
    for n, ref in enumerate((warm, leading, trailing)):
        spread_out(of_plane(ref), last, (species + n) % 8)
    pl.semaphore_wait(barrier, 4)

    def prepare(t, c):
        pack(lax.rem(t + last, tiles))
        layers_in(t, 8).wait()
        for sub in range(8):
            spread_out(of_density(t * 8 + sub), t, sub)
        return c

    lax.fori_loop(0, last, prepare, 0, unroll=2)
    pack(last - 1)
    def arrive(s, t):
        for copy in copies(s, t):
            copy.wait_recv()

    late.wait()
    arrive(0, last)
    u_sub, v_sub = fields % 8, (fields + 1) % 8
    for r in (*range(REACH), *range(REACH + rows, 2 * REACH + rows)):
        for h in range(parts):
            east[h, at(r), :] = jnp.broadcast_to(
                pull * start[last * parts + h, pl.ds(r * 8 + u_sub, 1), :], (8, LANES))
    for side in range(2):
        flow = jnp.broadcast_to(landed[0, last, side, pl.ds(v_sub, 1), :], (8, LANES))
        for k in range(1, REACH + 1):
            inside = slot >= SLOT - k if side == 0 else slot < k
            weight = (1.0 if side == 0 else -1.0) * transport_step * sixth_first[k - 1]
            flows[side * REACH + k - 1] = jnp.where(inside, weight * flow, 0.0)

    def split(held, t):
        scale = spread[at(t), :] * (transport_step / SECOND_SCALE)
        for i in range(rows):
            fs = [held[t * parts + h, at(REACH + i), :] for h in range(parts)]
            f_high, f_low = halves(jnp.concatenate([scale * f for f in fs], 1))
            g_high, g_low = halves(jnp.concatenate([north[h, at(i), :] * f for h, f in enumerate(fs)], 1))
            for m, piece in enumerate((f_high, f_low, g_high, g_low)):
                pieces[at(i), m * cols:(m + 1) * cols] = piece

    def stage(s):
        held, fresh = (start, one, two)[s], (one, two, None)[s]

        def tile(n, c):
            t = lax.rem(n + last, tiles)

            @pl.when(n > 0 if s == 0 else n >= 0)
            def _():
                arrive(s, t)

            d = spread[at(t), :] * transport_step
            coming[...] = jnp.dot(pieces[...], band[...], preferred_element_type=jnp.float32)
            split(held, lax.rem(t + 2, tiles))
            firsts, finals = [], []

            borders = []
            for side in range(2):
                halo = landed[s, t, side]
                total = None
                for k in range(1, REACH + 1):
                    inside = slot >= SLOT - k if side == 0 else slot < k
                    part = (jnp.where(inside, sixth_second[k - 1] * d, 0.0) + flows[side * REACH + k - 1]) * halo
                    if k < REACH:
                        part = pltpu.roll(part, (k - REACH) % LANES if side == 0 else REACH - k, 1)
                    total = part if total is None else total + part
                borders.append(total)
            ids = t * 8 + lax.broadcasted_iota(jnp.int32, (8, LANES), 0)
            reach = sixth_second[0] * d

            for b in range(rows // 8):
                for h in range(parts):
                    lanes = slice(h * LANES, (h + 1) * LANES)
                    f = [held[t * parts + h, at(b * 8 + m), :] for m in range(8 + 2 * REACH)]
                    gs = [east[h, at(b * 8 + m), :] * f[m] for m in range(8 + 2 * REACH)]
                    for r in range(8):
                        i = b * 8 + r
                        m = r + REACH
                        lap = (sixth_center / sixth_second[0]) * f[m] + (f[m + 1] + f[m - 1])
                        grad = gs[m + 1] - gs[m - 1]
                        for k in range(2, REACH + 1):
                            lap = lap + (sixth_second[k - 1] / sixth_second[0]) * (f[m + k] + f[m - k])
                            grad = grad + (sixth_first[k - 1] / sixth_first[0]) * (gs[m + k] - gs[m - k])
                        change = across[at(i), lanes] + (reach * lap - grad)
                        if h == 0:
                            change = change + jnp.where(
                                lane < REACH, pltpu.roll(borders[0], (LANES - home - SLOT * i - 1) % LANES, 1), 0.0)
                        if h == parts - 1:
                            change = change + jnp.where(
                                lane >= LANES - REACH,
                                pltpu.roll(borders[1], (2 * LANES - REACH - SLOT * i) % LANES, 1), 0.0)
                        if s < 2:
                            value = f[m] + change
                            if s == 1:
                                value = 0.75 * start[t * parts + h, at(REACH + i), :] + 0.25 * value
                            fresh[t * parts + h, at(REACH + i), :] = value
                            if h == 0:
                                gather(firsts, value, join_left)
                            if h == parts - 1:
                                gather(finals, value, join_right)
                        else:
                            value = start[t * parts + h, at(REACH + i), :] * (1.0 / 3.0) + (2.0 / 3.0) * (f[m] + change)
                            out[t * parts + h, at(i), :] = jnp.where(ids < species, jnp.maximum(value, 0.0), value)
            across[...] = coming[...]
            if s < 2:
                depart(s + 1, t, firsts, finals)
            else:
                result(t).start()
            return c

        split(held, last)
        across[...] = jnp.dot(pieces[...], band[...], preferred_element_type=jnp.float32)
        split(held, lax.rem(last + 1, tiles))
        lax.fori_loop(0, tiles, tile, 0)

    for s in range(3):
        stage(s)

    for copy in tables:
        copy.wait()

    def finish(t, c):
        result(t).wait()
        for s in range(3):
            for copy in copies(s, t):
                copy.wait_send()
        return c

    lax.fori_loop(0, tiles, finish, 0)


def band_matrix(width):
    here = np.arange(width)
    lag = here[:, None] - here[None, :]
    second = np.where(lag == 0, round(sixth_center * SECOND_SCALE), 0)
    first = np.zeros((width, width))
    for k in range(1, REACH + 1):
        ahead, behind = lag == k, lag == -k
        second = np.where(ahead | behind, round(sixth_second[k - 1] * SECOND_SCALE), second)
        weight = round(sixth_first[k - 1] * FIRST_SCALE)
        first = np.where(ahead, weight, np.where(behind, -weight, first))
    return jnp.asarray(np.concatenate([second, second, first, first], 0), jnp.bfloat16)


def advect(density, warm, leading, trailing, diffusion, pair, scaler, energy, produced, counts):
    species, rows, cols = density.shape
    fields = species + 1
    tiles = (fields + 2) // 8
    if (fields + 2) % 8 or rows * SLOT > LANES or cols % LANES or rows % 8:
        raise ValueError("unsupported sizes")
    parts = cols // LANES
    sizes = (lax.axis_size("grp"), lax.axis_size("gx"))
    wide = pltpu.VMEM((tiles * parts, (rows + 2 * REACH) * 8, LANES), jnp.float32)
    band = band_matrix(cols)
    reactions = pair.shape[1]
    if counts.shape[1] > LANES or species > 64:
        raise ValueError("unsupported sizes")
    length = up(up(reactions, TRIPS), 8)
    weight = spread_weights(reactions)[None]
    args = (density.reshape(species * rows, cols), warm, leading, trailing, diffusion, band, pair, scaler, energy, produced,
            weight, counts)
    count = len(args)
    places = [pltpu.SMEM if n == 4 else pltpu.VMEM for n in range(count)]

    results = [jax.ShapeDtypeStruct((tiles * parts, rows * 8, LANES), jnp.float32),
               jax.ShapeDtypeStruct((3 * length, LANES), jnp.float32),
               jax.ShapeDtypeStruct((2 * up(species, 8), up(length, 16)), jnp.bfloat16),
               jax.ShapeDtypeStruct((1, 2 * up(length, LANES)), jnp.int32),
               jax.ShapeDtypeStruct((1, LANES), jnp.int32)]

    def kernel(*refs):
        advect_kernel(fields, sizes, refs[:count], refs[count:count + len(results)], refs[count + len(results):])

    return pl.pallas_call(
        kernel,
        in_specs=[pl.BlockSpec(memory_space=pltpu.HBM)] * count,
        out_specs=[pl.BlockSpec(memory_space=pltpu.HBM)] * len(results),
        out_shape=results,
        scratch_shapes=[pltpu.VMEM(result.shape, result.dtype) for result in results]
        + [pltpu.SemaphoreType.DMA((tiles + len(results) - 1,))]
        + [place(arg.shape, arg.dtype) for place, arg in zip(places, args)]
        + [pltpu.SemaphoreType.DMA((count - 1 + tiles,)),
           pltpu.VMEM((8, up(length, LANES)), jnp.float32),
           pltpu.VMEM((tiles * 8, LANES), jnp.float32), wide, wide, wide,
           pltpu.VMEM((parts, (rows + 2 * REACH) * 8, LANES), jnp.float32),
           pltpu.VMEM((parts, rows * 8, LANES), jnp.float32),
           pltpu.VMEM((rows * 8, 4 * cols), jnp.bfloat16),
           pltpu.VMEM((rows * 8, cols), jnp.float32),
           pltpu.VMEM((rows * 8, cols), jnp.float32),
           pltpu.VMEM((3, tiles, 2, 8, LANES), jnp.float32),
           pltpu.VMEM((3, tiles, 2, 8, LANES), jnp.float32),
           pltpu.VMEM((2 * REACH, 8, LANES), jnp.float32),
           pltpu.SemaphoreType.DMA((3, tiles, 4)),
           pltpu.SemaphoreType.DMA((3, tiles, 4))],
        compiler_params=pltpu.CompilerParams(collective_id=0, has_side_effects=True),
        name="advect",
    )(*args)


GROUP = 16
PITCH = GROUP + 1
SPAN = 9


def chemistry_kernel(species, chunk, order, counts, pair, warming, rates, table, state, out, warm_out,
                     held, low_gained, high_gained, progress, steps, staged, sems, *losses):
    rows, cols = warm_out.shape
    layers = state.shape[0] * LANES // cols * 8
    per_row = cols // TILE
    tiles = rows * per_row
    warm_row = species
    length = rates.shape[0] // 3
    reactions = length // chunk * chunk
    span = progress.shape[0] // GROUP
    depth = table.shape[1]
    half = table.shape[0] // 2
    blocks = layers // 8
    lines = staged.reshape(staged.shape[0] * staged.shape[1], LANES)
    line_span = staged.shape[1]
    gained = (low_gained, high_gained)

    for t in range(GROUP):
        progress[pl.ds(t * span + reactions, depth - reactions)] = jnp.zeros((depth - reactions, LANES), jnp.float32)
    for loss in losses:
        loss[...] = jnp.zeros_like(loss)

    def at(field):
        return pl.ds(field * PITCH, GROUP)

    def handle(g, c):
        ids = [order[0, g * GROUP + t] for t in range(GROUP)]
        numbers = [counts[t] for t in ids]
        places = [(t % per_row, pl.ds(pl.multiple_of(t // per_row * 8, 8), 8)) for t in ids]
        turn_count = functools.reduce(jnp.maximum, numbers)
        for t in range(GROUP):
            part, at_row = places[t]
            steps[t:t + 1, :] = jnp.full((1, LANES), numbers[t].astype(jnp.float32))
            for f in range(blocks):
                held[pl.ds(f * 8 * PITCH + t, 8, stride=PITCH)] = state[f * per_row + part, at_row, :]

        def advance(s, c):
            heat = jnp.tanh(held[at(warm_row)])

            def react(k, c):
                for j in range(chunk):
                    r = k * chunk + j
                    first = pl.ds(pair[0, r], GROUP)
                    second = pl.ds(pair[0, pair.shape[1] // 2 + r], GROUP)
                    a, e, weight = [jnp.broadcast_to(rates[pl.ds(n * length + r, 1), :], (GROUP, LANES)) for n in range(3)]
                    rate = jnp.exp2(a + e * heat)
                    ca, cb = held[first], held[second]
                    qa, qb = rate * ca, rate * cb
                    progress[pl.ds(r, GROUP, stride=span)] = qa * (weight * cb)
                    n = 2 * (j % (len(losses) // 2))
                    losses[n][first] += qb
                    losses[n + 1][second] += qa
                return c

            lax.fori_loop(0, reactions // chunk, react, 0)
            for n, fill in enumerate(gained):
                for q in range(4 * n, 4 * n + 4):
                    p = jnp.concatenate([progress[pl.ds((2 * q + t) * span, depth)] for t in range(2)], 1)
                    both = jnp.dot(table[...], p.astype(jnp.bfloat16), preferred_element_type=jnp.float32)
                    total = both[:half] + both[half:]
                    for t in range(2):
                        for f in range(half // 8):
                            fill[pl.ds(f * 8 * SPAN + 2 * (q - 4 * n) + t, 8, stride=SPAN)] = (
                                total[f * 8:(f + 1) * 8, t * TILE:(t + 1) * TILE])
                number = steps[8 * n:8 * n + 8, :]
                pace = number * (1.0 / chemistry_span)
                active = s.astype(jnp.float32) < number
                change = jnp.zeros((8, LANES), jnp.float32)
                for j in range(species):
                    place = pl.ds(j * PITCH + 8 * n, 8)
                    x = held[place]
                    destroyed = functools.reduce(jnp.add, [loss[place] for loss in losses])
                    for loss in losses:
                        loss[place] = jnp.zeros((8, LANES), jnp.float32)
                    updated = (pace * x + fill[pl.ds(j * SPAN, 8)]) / (pace + destroyed)
                    change = change + warming[j] * (updated - x)
                    held[place] = jnp.where(active, updated, x)
                place = pl.ds(warm_row * PITCH + 8 * n, 8)
                w = held[place]
                held[place] = jnp.where(active, w + change, w)
            return c

        lax.fori_loop(0, turn_count, advance, 0)
        for t in range(GROUP):
            line = (ids[t] % per_row) * ((warm_row + 1) * line_span) + ids[t] // per_row
            for f in range(0, warm_row + 1, 8):
                n = min(8, warm_row + 1 - f)
                lines[pl.ds(line + f * line_span, n, stride=line_span)] = held[pl.ds(f * PITCH + t, n, stride=PITCH)]
        return c

    lax.fori_loop(0, tiles // GROUP, handle, 0)
    wide = out.reshape(species, rows, cols)
    copies = []
    for n in range(per_row):
        lanes = pl.ds(n * TILE, TILE)
        first = n * (warm_row + 1)
        copies.append(pltpu.make_async_copy(
            staged.at[pl.ds(first, species), pl.ds(0, rows)], wide.at[:, :, lanes], sems.at[0, n]))
        copies.append(pltpu.make_async_copy(
            staged.at[first + species, pl.ds(0, rows)], warm_out.at[:, lanes], sems.at[1, n]))
    for copy in copies:
        copy.start()
    for copy in copies:
        copy.wait()


LOSSES = 4


def chemistry(state, order, counts, pair, warming, rates, table, species, rows, cols):
    layers = state.shape[0] * LANES // cols * 8
    smem = pl.BlockSpec(memory_space=pltpu.SMEM)
    vmem = pl.BlockSpec(memory_space=pltpu.VMEM)
    block = pltpu.VMEM((layers * PITCH, LANES), jnp.float32)
    part = pltpu.VMEM((layers * SPAN, LANES), jnp.float32)
    return pl.pallas_call(
        functools.partial(chemistry_kernel, species, rates.shape[0] // 3 // TRIPS),
        in_specs=[smem, smem, smem, smem, vmem, vmem, vmem],
        out_specs=[pl.BlockSpec(memory_space=pl.ANY)] * 2,
        out_shape=[jax.ShapeDtypeStruct((species * rows, cols), jnp.float32),
                   jax.ShapeDtypeStruct((rows, cols), jnp.float32)],
        scratch_shapes=[block, part, part,
                        pltpu.VMEM((GROUP * (table.shape[1] + 1), LANES), jnp.float32),
                        pltpu.VMEM((GROUP, LANES), jnp.float32),
                        pltpu.VMEM((cols // TILE * (species + 1), rows + 8, TILE), jnp.float32),
                        pltpu.SemaphoreType.DMA((2, cols // TILE))]
        + [block] * LOSSES,
        name="chemistry",
    )(order, counts, pair, warming, rates, table, state)


def body(component_density, scaled_thermal_state, leading_direction_flow, trailing_direction_flow,
         spreading_coefficient, colliding_pair, natural_exponent_scaler, arrhenius_energy,
         stoichiometric_output, formation_warming, explicit_increments):
    species, rows, cols = component_density.shape
    clipped, rates, table, pair, order = advect(
        component_density, scaled_thermal_state, leading_direction_flow, trailing_direction_flow, spreading_coefficient,
        colliding_pair.T, natural_exponent_scaler, arrhenius_energy, stoichiometric_output.T,
        explicit_increments[None])
    reacted, warm = chemistry(clipped, order, explicit_increments, pair, formation_warming, rates, table,
                              species, rows, cols)
    return reacted.reshape(species, rows, cols), warm


def solution(mesh):
    return jax.shard_map(
        body,
        mesh=mesh,
        in_specs=(
            P(None, "gx", "grp"),
            P("gx", "grp"),
            P("gx", "grp"),
            P("gx", "grp"),
            P(),
            P(),
            P(),
            P(),
            P(),
            P(),
            P(("grp", "gx")),
        ),
        out_specs=(P(None, "gx", "grp"), P("gx", "grp")),
        check_vma=False,
    )
```

```python
import functools
import math

import jax
import jax.numpy as jnp
import numpy as np
from jax import lax
from jax.experimental import pallas as pl
from jax.experimental.pallas import tpu as pltpu
from jax.sharding import PartitionSpec as P

TILE = 128
FIRST_SCALE = 60.0
SECOND_SCALE = 180.0
transport_step = 0.4
chemistry_span = 0.5
sixth_first = (0.75, -0.15, 1.0 / 60.0)
sixth_second = (1.5, -0.15, 1.0 / 90.0)
sixth_center = -49.0 / 18.0


def up(n, m):
    return -(-n // m) * m


def spread_weights(reactions):
    golden = (math.sqrt(5.0) - 1.0) / 2.0
    return np.exp2((np.arange(reactions) * golden) % 1.0).astype(np.float32)


REACH = 3
SLOT = 4
LANES = 128
NEVER = -16384.0
TRIPS = 3
BAND = 4


def halves(value):
    high = value.astype(jnp.bfloat16)
    return high, (value - high.astype(jnp.float32)).astype(jnp.bfloat16)


def prepare_tables(pair, scaler, energy, produced, weight, counts, rates, table, offsets, order, lines):
    reactions = pair.shape[1]
    length = rates.shape[0] // 3
    species = produced.shape[0]
    half = table.shape[0] // 2
    scale = 1.0 / math.log(2.0)
    wide = lines.shape[1]
    lines[...] = jnp.zeros_like(lines)
    lines[0:1, :] = jnp.full((1, wide), NEVER)
    lines[0, 0:reactions] = scaler[...] * scale
    lines[1, 0:reactions] = energy[...] * scale
    lines[2:3, 0:reactions] = weight[...]
    for n in range(3):
        for r in range(0, length, LANES):
            count = min(LANES, length - r)
            row = jnp.broadcast_to(lines[n:n + 1, r:r + LANES], (LANES, LANES))
            rates[n * length + r:n * length + r + count, :] = row.T[:count]
    table[...] = jnp.zeros_like(table)
    high, low = halves(produced[...] / weight[...])
    table[0:species, 0:reactions] = high
    table[half:half + species, 0:reactions] = low
    offsets[...] = jnp.zeros_like(offsets)
    for n in range(2):
        offsets[:, n * wide:n * wide + reactions] = pair[n:n + 1, :] * PITCH
    tiles = counts.shape[1]
    lines[3:4, 0:tiles] = counts[...].astype(jnp.float32) * tiles
    key = lines[3:4, 0:LANES] + lax.broadcasted_iota(jnp.int32, (1, LANES), 1).astype(jnp.float32)
    down = lax.broadcasted_iota(jnp.int32, (LANES, LANES), 0).astype(jnp.float32)
    along = lax.broadcasted_iota(jnp.int32, (LANES, LANES), 1)
    across = jnp.broadcast_to(key, (LANES, LANES))
    before = jnp.where((across < across.T) & (along < tiles), 1.0, 0.0)
    rank = jnp.sum(before, axis=1, keepdims=True)
    here = jnp.where((rank == along.astype(jnp.float32)) & (down < tiles), down, 0.0)
    order[...] = jnp.sum(here, axis=0, keepdims=True).astype(jnp.int32)


def advect_kernel(fields, sizes, sources, targets, scratch):
    (out, rates, table, offsets, order, stored, density, warm, leading, trailing, diffusion, band, pair, scaler, energy, produced, weight, counts, loaded,
     lines, spread, start, one, two, east, north, pieces, across, coming, packed, landed, flows, send, recv) = scratch
    n_grp, n_gx = sizes
    g, x = lax.axis_index("grp"), lax.axis_index("gx")
    rows, cols = warm.shape
    parts = cols // LANES
    tiles = start.shape[0] // parts
    species = fields - 1
    last = fields // 8
    up, down = (g, lax.rem(x + n_gx - 1, n_gx)), (g, lax.rem(x + 1, n_gx))
    left, right = (lax.rem(g + n_grp - 1, n_grp), x), (lax.rem(g + 1, n_grp), x)
    places = (warm, leading, trailing, diffusion, band, pair, scaler, energy, produced, weight, counts)
    inputs = [pltpu.make_async_copy(src, dst, loaded.at[n]) for n, (src, dst) in enumerate(zip(sources[1:], places))]

    def layers_in(t, count):
        span = pl.ds(t * 8 * rows if isinstance(t, int) else pl.multiple_of(t * 8 * rows, 8), count * rows)
        return pltpu.make_async_copy(sources[0].at[span], density.at[span], loaded.at[len(places) + t])

    early, late = inputs[:BAND] + inputs[BAND + 1:], inputs[BAND]
    for copy in early:
        copy.start()
    layers_in(last, species - last * 8).start()

    def begin(t, c):
        layers_in(t, 8).start()
        return c

    lax.fori_loop(0, last, begin, 0)
    late.start()
    barrier = pltpu.get_barrier_semaphore()
    for place in (up, down, left, right):
        pl.semaphore_signal(barrier, inc=1, device_id=place, device_id_type=pl.DeviceIdType.MESH)

    lane = lax.broadcasted_iota(jnp.int32, (8, LANES), 1)
    slot = lane % SLOT
    home = LANES - SLOT * rows

    def at(row):
        return pl.ds(row * 8 if isinstance(row, int) else pl.multiple_of(row * 8, 8), 8)

    def spread_out(read, t, sub):
        for q in range(rows // 8):
            for h in range(parts):
                start[t * parts + h, pl.ds((REACH + q * 8) * 8 + sub, 8, stride=8), :] = read(q, h)

    def of_density(f):
        return lambda q, h: density[pl.ds(pl.multiple_of(f * rows + q * 8, 8), 8), h * LANES:(h + 1) * LANES]

    def of_plane(ref):
        return lambda q, h: ref[q * 8:(q + 1) * 8, h * LANES:(h + 1) * LANES]

    def result(t):
        both = pl.ds(t * parts, parts)
        return pltpu.make_async_copy(out.at[both], targets[0].at[both], stored.at[t])

    def copies(s, t):
        held = (start, one, two)[s]
        both = pl.ds(t * parts, parts)
        plan = [
            (held.at[both, pl.ds(REACH * 8, REACH * 8)], held.at[both, pl.ds((REACH + rows) * 8, REACH * 8)], up),
            (held.at[both, pl.ds(rows * 8, REACH * 8)], held.at[both, pl.ds(0, REACH * 8)], down),
            (packed.at[s, t, 0], landed.at[s, t, 1], left),
            (packed.at[s, t, 1], landed.at[s, t, 0], right),
        ]
        return [pltpu.make_async_remote_copy(
            src_ref=src, dst_ref=dst, send_sem=send.at[s, t, n], recv_sem=recv.at[s, t, n],
            device_id=place, device_id_type=pl.DeviceIdType.MESH) for n, (src, dst, place) in enumerate(plan)]

    def join_left(a, n, b, m):
        return jnp.where(lane < SLOT * n, a, pltpu.roll(b, SLOT * n, 1))

    def join_right(a, n, b, m):
        return jnp.where(lane >= LANES - SLOT * m, b, pltpu.roll(a, LANES - SLOT * m, 1))

    def gather(stack, value, join):
        stack.append((1, value))
        while len(stack) > 1 and stack[-1][0] == stack[-2][0]:
            m, b = stack.pop()
            n, a = stack.pop()
            stack.append((n + m, join(a, n, b, m)))

    def gathered(stack, join):
        while len(stack) > 1:
            m, b = stack.pop()
            n, a = stack.pop()
            stack.append((n + m, join(a, n, b, m)))
        return stack[0][1]

    def depart(s, t, firsts, finals):
        packed[s, t, 0] = gathered(firsts, join_left)
        packed[s, t, 1] = gathered(finals, join_right)
        for copy in copies(s, t):
            copy.start()

    def pack(t):
        firsts, finals = [], []
        for i in range(rows):
            gather(firsts, start[t * parts, at(REACH + i), :], join_left)
            gather(finals, start[t * parts + parts - 1, at(REACH + i), :], join_right)
        depart(0, t, firsts, finals)

    for copy in early:
        copy.wait()
    for f in range(tiles * 8):
        spread[f:f + 1, :] = jnp.full((1, LANES), diffusion[f] if f < fields else 0.0)
    prepare_tables(pair, scaler, energy, produced, weight, counts, rates, table, offsets, order, lines)
    tables = [pltpu.make_async_copy(src, dst, stored.at[tiles + n]) for n, (src, dst) in enumerate(
        zip((rates, table, offsets, order), targets[1:]))]
    for copy in tables:
        copy.start()
    pull, push = transport_step * sixth_first[0], -transport_step / FIRST_SCALE
    for i in range(rows):
        for h in range(parts):
            lanes = slice(h * LANES, (h + 1) * LANES)
            east[h, at(REACH + i), :] = jnp.broadcast_to(pull * leading[i:i + 1, lanes], (8, LANES))
            north[h, at(i), :] = jnp.broadcast_to(push * trailing[i:i + 1, lanes], (8, LANES))

    layers_in(last, species - last * 8).wait()
    for f in range(last * 8, species):
        spread_out(of_density(f), last, f % 8)
    for n, ref in enumerate((warm, leading, trailing)):
        spread_out(of_plane(ref), last, (species + n) % 8)
    pl.semaphore_wait(barrier, 4)

    def prepare(t, c):
        pack(lax.rem(t + last, tiles))
        layers_in(t, 8).wait()
        for sub in range(8):
            spread_out(of_density(t * 8 + sub), t, sub)
        return c

    lax.fori_loop(0, last, prepare, 0, unroll=2)
    pack(last - 1)
    def arrive(s, t):
        for copy in copies(s, t):
            copy.wait_recv()

    late.wait()
    arrive(0, last)
    u_sub, v_sub = fields % 8, (fields + 1) % 8
    for r in (*range(REACH), *range(REACH + rows, 2 * REACH + rows)):
        for h in range(parts):
            east[h, at(r), :] = jnp.broadcast_to(
                pull * start[last * parts + h, pl.ds(r * 8 + u_sub, 1), :], (8, LANES))
    for side in range(2):
        flow = jnp.broadcast_to(landed[0, last, side, pl.ds(v_sub, 1), :], (8, LANES))
        for k in range(1, REACH + 1):
            inside = slot >= SLOT - k if side == 0 else slot < k
            weight = (1.0 if side == 0 else -1.0) * transport_step * sixth_first[k - 1]
            flows[side * REACH + k - 1] = jnp.where(inside, weight * flow, 0.0)

    def split(held, t):
        scale = spread[at(t), :] * (transport_step / SECOND_SCALE)
        for i in range(rows):
            fs = [held[t * parts + h, at(REACH + i), :] for h in range(parts)]
            f_high, f_low = halves(jnp.concatenate([scale * f for f in fs], 1))
            g_high, g_low = halves(jnp.concatenate([north[h, at(i), :] * f for h, f in enumerate(fs)], 1))
            for m, piece in enumerate((f_high, f_low, g_high, g_low)):
                pieces[at(i), m * cols:(m + 1) * cols] = piece

    def stage(s):
        held, fresh = (start, one, two)[s], (one, two, None)[s]

        def tile(n, c):
            t = lax.rem(n + last, tiles)

            @pl.when(n > 0 if s == 0 else n >= 0)
            def _():
                arrive(s, t)

            d = spread[at(t), :] * transport_step
            coming[...] = jnp.dot(pieces[...], band[...], preferred_element_type=jnp.float32)
            split(held, lax.rem(t + 2, tiles))
            firsts, finals = [], []

            borders = []
            for side in range(2):
                halo = landed[s, t, side]
                total = None
                for k in range(1, REACH + 1):
                    inside = slot >= SLOT - k if side == 0 else slot < k
                    part = (jnp.where(inside, sixth_second[k - 1] * d, 0.0) + flows[side * REACH + k - 1]) * halo
                    if k < REACH:
                        part = pltpu.roll(part, (k - REACH) % LANES if side == 0 else REACH - k, 1)
                    total = part if total is None else total + part
                borders.append(total)
            ids = t * 8 + lax.broadcasted_iota(jnp.int32, (8, LANES), 0)
            reach = sixth_second[0] * d

            for b in range(rows // 8):
                for h in range(parts):
                    lanes = slice(h * LANES, (h + 1) * LANES)
                    f = [held[t * parts + h, at(b * 8 + m), :] for m in range(8 + 2 * REACH)]
                    gs = [east[h, at(b * 8 + m), :] * f[m] for m in range(8 + 2 * REACH)]
                    for r in range(8):
                        i = b * 8 + r
                        m = r + REACH
                        lap = (sixth_center / sixth_second[0]) * f[m] + (f[m + 1] + f[m - 1])
                        grad = gs[m + 1] - gs[m - 1]
                        for k in range(2, REACH + 1):
                            lap = lap + (sixth_second[k - 1] / sixth_second[0]) * (f[m + k] + f[m - k])
                            grad = grad + (sixth_first[k - 1] / sixth_first[0]) * (gs[m + k] - gs[m - k])
                        change = across[at(i), lanes] + (reach * lap - grad)
                        if h == 0:
                            change = change + jnp.where(
                                lane < REACH, pltpu.roll(borders[0], (LANES - home - SLOT * i - 1) % LANES, 1), 0.0)
                        if h == parts - 1:
                            change = change + jnp.where(
                                lane >= LANES - REACH,
                                pltpu.roll(borders[1], (2 * LANES - REACH - SLOT * i) % LANES, 1), 0.0)
                        if s < 2:
                            value = f[m] + change
                            if s == 1:
                                value = 0.75 * start[t * parts + h, at(REACH + i), :] + 0.25 * value
                            fresh[t * parts + h, at(REACH + i), :] = value
                            if h == 0:
                                gather(firsts, value, join_left)
                            if h == parts - 1:
                                gather(finals, value, join_right)
                        else:
                            value = start[t * parts + h, at(REACH + i), :] * (1.0 / 3.0) + (2.0 / 3.0) * (f[m] + change)
                            out[t * parts + h, at(i), :] = jnp.where(ids < species, jnp.maximum(value, 0.0), value)
            across[...] = coming[...]
            if s < 2:
                depart(s + 1, t, firsts, finals)
            else:
                result(t).start()
            return c

        split(held, last)
        across[...] = jnp.dot(pieces[...], band[...], preferred_element_type=jnp.float32)
        split(held, lax.rem(last + 1, tiles))
        lax.fori_loop(0, tiles, tile, 0)

    for s in range(3):
        stage(s)

    for copy in tables:
        copy.wait()

    def finish(t, c):
        result(t).wait()
        for s in range(3):
            for copy in copies(s, t):
                copy.wait_send()
        return c

    lax.fori_loop(0, tiles, finish, 0)


def band_matrix(width):
    here = np.arange(width)
    lag = here[:, None] - here[None, :]
    second = np.where(lag == 0, round(sixth_center * SECOND_SCALE), 0)
    first = np.zeros((width, width))
    for k in range(1, REACH + 1):
        ahead, behind = lag == k, lag == -k
        second = np.where(ahead | behind, round(sixth_second[k - 1] * SECOND_SCALE), second)
        weight = round(sixth_first[k - 1] * FIRST_SCALE)
        first = np.where(ahead, weight, np.where(behind, -weight, first))
    return jnp.asarray(np.concatenate([second, second, first, first], 0), jnp.bfloat16)


def advect(density, warm, leading, trailing, diffusion, pair, scaler, energy, produced, counts):
    species, rows, cols = density.shape
    fields = species + 1
    tiles = (fields + 2) // 8
    if (fields + 2) % 8 or rows * SLOT > LANES or cols % LANES or rows % 8:
        raise ValueError("unsupported sizes")
    parts = cols // LANES
    sizes = (lax.axis_size("grp"), lax.axis_size("gx"))
    wide = pltpu.VMEM((tiles * parts, (rows + 2 * REACH) * 8, LANES), jnp.float32)
    band = band_matrix(cols)
    reactions = pair.shape[1]
    if counts.shape[1] > LANES or species > 64:
        raise ValueError("unsupported sizes")
    length = up(up(reactions, TRIPS), 8)
    weight = spread_weights(reactions)[None]
    args = (density.reshape(species * rows, cols), warm, leading, trailing, diffusion, band, pair, scaler, energy, produced,
            weight, counts)
    count = len(args)
    places = [pltpu.SMEM if n == 4 else pltpu.VMEM for n in range(count)]

    results = [jax.ShapeDtypeStruct((tiles * parts, rows * 8, LANES), jnp.float32),
               jax.ShapeDtypeStruct((3 * length, LANES), jnp.float32),
               jax.ShapeDtypeStruct((2 * up(species, 8), up(length, 16)), jnp.bfloat16),
               jax.ShapeDtypeStruct((1, 2 * up(length, LANES)), jnp.int32),
               jax.ShapeDtypeStruct((1, LANES), jnp.int32)]

    def kernel(*refs):
        advect_kernel(fields, sizes, refs[:count], refs[count:count + len(results)], refs[count + len(results):])

    return pl.pallas_call(
        kernel,
        in_specs=[pl.BlockSpec(memory_space=pltpu.HBM)] * count,
        out_specs=[pl.BlockSpec(memory_space=pltpu.HBM)] * len(results),
        out_shape=results,
        scratch_shapes=[pltpu.VMEM(result.shape, result.dtype) for result in results]
        + [pltpu.SemaphoreType.DMA((tiles + len(results) - 1,))]
        + [place(arg.shape, arg.dtype) for place, arg in zip(places, args)]
        + [pltpu.SemaphoreType.DMA((count - 1 + tiles,)),
           pltpu.VMEM((8, up(length, LANES)), jnp.float32),
           pltpu.VMEM((tiles * 8, LANES), jnp.float32), wide, wide, wide,
           pltpu.VMEM((parts, (rows + 2 * REACH) * 8, LANES), jnp.float32),
           pltpu.VMEM((parts, rows * 8, LANES), jnp.float32),
           pltpu.VMEM((rows * 8, 4 * cols), jnp.bfloat16),
           pltpu.VMEM((rows * 8, cols), jnp.float32),
           pltpu.VMEM((rows * 8, cols), jnp.float32),
           pltpu.VMEM((3, tiles, 2, 8, LANES), jnp.float32),
           pltpu.VMEM((3, tiles, 2, 8, LANES), jnp.float32),
           pltpu.VMEM((2 * REACH, 8, LANES), jnp.float32),
           pltpu.SemaphoreType.DMA((3, tiles, 4)),
           pltpu.SemaphoreType.DMA((3, tiles, 4))],
        compiler_params=pltpu.CompilerParams(collective_id=0, has_side_effects=True),
        name="advect",
    )(*args)


GROUP = 16
PITCH = GROUP + 1
SPAN = 9


def chemistry_kernel(species, chunk, order, counts, pair, warming, rates, table, state, out, warm_out,
                     held, low_gained, high_gained, progress, steps, staged, sems, *losses):
    rows, cols = warm_out.shape
    layers = state.shape[0] * LANES // cols * 8
    per_row = cols // TILE
    tiles = rows * per_row
    warm_row = species
    length = rates.shape[0] // 3
    reactions = length // chunk * chunk
    span = progress.shape[0] // GROUP
    depth = table.shape[1]
    half = table.shape[0] // 2
    blocks = layers // 8
    lines = staged.reshape(staged.shape[0] * staged.shape[1], LANES)
    line_span = staged.shape[1]
    gained = (low_gained, high_gained)

    for t in range(GROUP):
        progress[pl.ds(t * span + reactions, depth - reactions)] = jnp.zeros((depth - reactions, LANES), jnp.float32)
    for loss in losses:
        loss[...] = jnp.zeros_like(loss)

    def at(field):
        return pl.ds(field * PITCH, GROUP)

    def handle(g, c):
        ids = [order[0, g * GROUP + t] for t in range(GROUP)]
        numbers = [counts[t] for t in ids]
        places = [(t % per_row, pl.ds(pl.multiple_of(t // per_row * 8, 8), 8)) for t in ids]
        turn_count = functools.reduce(jnp.maximum, numbers)
        for t in range(GROUP):
            part, at_row = places[t]
            steps[t:t + 1, :] = jnp.full((1, LANES), numbers[t].astype(jnp.float32))
            for f in range(blocks):
                held[pl.ds(f * 8 * PITCH + t, 8, stride=PITCH)] = state[f * per_row + part, at_row, :]

        def advance(s, c):
            heat = jnp.tanh(held[at(warm_row)])

            def react(k, c):
                for j in range(chunk):
                    r = k * chunk + j
                    first = pl.ds(pair[0, r], GROUP)
                    second = pl.ds(pair[0, pair.shape[1] // 2 + r], GROUP)
                    a, e, weight = [jnp.broadcast_to(rates[pl.ds(n * length + r, 1), :], (GROUP, LANES)) for n in range(3)]
                    rate = jnp.exp2(a + e * heat)
                    ca, cb = held[first], held[second]
                    qa, qb = rate * ca, rate * cb
                    progress[pl.ds(r, GROUP, stride=span)] = qa * (weight * cb)
                    n = 2 * (j % (len(losses) // 2))
                    losses[n][first] += qb
                    losses[n + 1][second] += qa
                return c

            lax.fori_loop(0, reactions // chunk, react, 0)
            for n, fill in enumerate(gained):
                for q in range(4 * n, 4 * n + 4):
                    p = jnp.concatenate([progress[pl.ds((2 * q + t) * span, depth)] for t in range(2)], 1)
                    both = jnp.dot(table[...], p.astype(jnp.bfloat16), preferred_element_type=jnp.float32)
                    total = both[:half] + both[half:]
                    for t in range(2):
                        for f in range(half // 8):
                            fill[pl.ds(f * 8 * SPAN + 2 * (q - 4 * n) + t, 8, stride=SPAN)] = (
                                total[f * 8:(f + 1) * 8, t * TILE:(t + 1) * TILE])
                number = steps[8 * n:8 * n + 8, :]
                pace = number * (1.0 / chemistry_span)
                active = s.astype(jnp.float32) < number
                change = jnp.zeros((8, LANES), jnp.float32)
                for j in range(species):
                    place = pl.ds(j * PITCH + 8 * n, 8)
                    x = held[place]
                    destroyed = functools.reduce(jnp.add, [loss[place] for loss in losses])
                    for loss in losses:
                        loss[place] = jnp.zeros((8, LANES), jnp.float32)
                    updated = (pace * x + fill[pl.ds(j * SPAN, 8)]) / (pace + destroyed)
                    change = change + warming[j] * (updated - x)
                    held[place] = jnp.where(active, updated, x)
                place = pl.ds(warm_row * PITCH + 8 * n, 8)
                w = held[place]
                held[place] = jnp.where(active, w + change, w)
            return c

        lax.fori_loop(0, turn_count, advance, 0)
        for t in range(GROUP):
            line = (ids[t] % per_row) * ((warm_row + 1) * line_span) + ids[t] // per_row
            for f in range(0, warm_row + 1, 8):
                n = min(8, warm_row + 1 - f)
                lines[pl.ds(line + f * line_span, n, stride=line_span)] = held[pl.ds(f * PITCH + t, n, stride=PITCH)]
        return c

    lax.fori_loop(0, tiles // GROUP, handle, 0)
    wide = out.reshape(species, rows, cols)
    copies = []
    for n in range(per_row):
        lanes = pl.ds(n * TILE, TILE)
        first = n * (warm_row + 1)
        copies.append(pltpu.make_async_copy(
            staged.at[pl.ds(first, species), pl.ds(0, rows)], wide.at[:, :, lanes], sems.at[0, n]))
        copies.append(pltpu.make_async_copy(
            staged.at[first + species, pl.ds(0, rows)], warm_out.at[:, lanes], sems.at[1, n]))
    for copy in copies:
        copy.start()
    for copy in copies:
        copy.wait()


LOSSES = 4


def chemistry(state, order, counts, pair, warming, rates, table, species, rows, cols):
    layers = state.shape[0] * LANES // cols * 8
    smem = pl.BlockSpec(memory_space=pltpu.SMEM)
    vmem = pl.BlockSpec(memory_space=pltpu.VMEM)
    block = pltpu.VMEM((layers * PITCH, LANES), jnp.float32)
    part = pltpu.VMEM((layers * SPAN, LANES), jnp.float32)
    return pl.pallas_call(
        functools.partial(chemistry_kernel, species, rates.shape[0] // 3 // TRIPS),
        in_specs=[smem, smem, smem, smem, vmem, vmem, vmem],
        out_specs=[pl.BlockSpec(memory_space=pl.ANY)] * 2,
        out_shape=[jax.ShapeDtypeStruct((species * rows, cols), jnp.float32),
                   jax.ShapeDtypeStruct((rows, cols), jnp.float32)],
        scratch_shapes=[block, part, part,
                        pltpu.VMEM((GROUP * (table.shape[1] + 1), LANES), jnp.float32),
                        pltpu.VMEM((GROUP, LANES), jnp.float32),
                        pltpu.VMEM((cols // TILE * (species + 1), rows + 8, TILE), jnp.float32),
                        pltpu.SemaphoreType.DMA((2, cols // TILE))]
        + [block] * LOSSES,
        name="chemistry",
    )(order, counts, pair, warming, rates, table, state)


def body(component_density, scaled_thermal_state, leading_direction_flow, trailing_direction_flow,
         spreading_coefficient, colliding_pair, natural_exponent_scaler, arrhenius_energy,
         stoichiometric_output, formation_warming, explicit_increments):
    species, rows, cols = component_density.shape
    clipped, rates, table, pair, order = advect(
        component_density, scaled_thermal_state, leading_direction_flow, trailing_direction_flow, spreading_coefficient,
        colliding_pair.T, natural_exponent_scaler, arrhenius_energy, stoichiometric_output.T,
        explicit_increments[None])
    reacted, warm = chemistry(clipped, order, explicit_increments, pair, formation_warming, rates, table,
                              species, rows, cols)
    return reacted.reshape(species, rows, cols), warm


def solution(mesh):
    return jax.shard_map(
        body,
        mesh=mesh,
        in_specs=(
            P(None, "gx", "grp"),
            P("gx", "grp"),
            P("gx", "grp"),
            P("gx", "grp"),
            P(),
            P(),
            P(),
            P(),
            P(),
            P(),
            P(("grp", "gx")),
        ),
        out_specs=(P(None, "gx", "grp"), P("gx", "grp")),
        check_vma=False,
    )
```
